512 devices in a mesh: slab: 64 (over z, x, core), tile: 8 (over y).
Axes of the slice: x: 4, y: 8, z: 8, core: 2. Of those that a mesh axis runs over, the one named last changes fastest.
Arguments:
- features: bfloat16 [64, 8, 512, 128], P('slab', 'tile'), may hold values from -24 to 24
- counts: int32 [64, 8], P('slab', 'tile'), may hold values from 128 to 512, as said below
- rulebook: int32 [64, 8, 27, 512], P('slab', 'tile'), may hold values from 0 to 800, as said below
- face_rows: int32 [64, 8, 4, 64], P('slab', 'tile'), may hold values from 0 to 511, as said below
- conv_one: bfloat16 [27, 128, 128], replicated, may hold values from -0.109375 to 0.109375
- gain_one: float32 [128], replicated, may hold values from 0.5 to 1.5
- shift_one: float32 [128], replicated, may hold values from -0.5 to 0.5
- conv_two: bfloat16 [27, 128, 128], replicated, may hold values from -0.109375 to 0.109375
- gain_two: float32 [128], replicated, may hold values from 0.5 to 1.5
- shift_two: float32 [128], replicated, may hold values from -0.5 to 0.5
Outputs:
- output: bfloat16 [64, 8, 512, 128], P('slab', 'tile')
The draws below stay inside these ranges and needn't reach their ends.
Inputs may be any that keep to these rules, and one draw needn't show every extreme that they name: `counts`: each device's voxels fill its 8 x 8 grid columns with the same number each, between 2 and 8; some device of the highest slab index holds 512. `rulebook`: an entry names the extended-table row that holds the voxel's neighbour at offset k = 9 (dx + 1) + 3 (dy + 1) + (dz + 1) of the submanifold 3x3x3 stencil, or 800 where that cell is inactive or outside the grid; the voxel itself is at offset 13; rows at or past the device's count name 800 at every offset. `face_rows`: lists 0 to 3 hold the device's voxels on its lower and higher face along the first, then the lower and higher face along the second dimension; the j-th voxel of the i-th column along a face stands at position i * 8 + j; unused positions name row 0.
All inputs are finite; a program needn't handle non-finite values.
Results may differ from the reference program's by a relative error of at most 0.0033.
Values may be sent and summed in bfloat16 or wider, within the bound.
No kernel may reach another device: no remote copies, remote signals or barrier semaphores. Data moves between devices by JAX's collectives and lax.ppermute only.
A program may use at most 64 MiB of HBM per device.

```python
import math
import jax
import jax.numpy as jnp
from jax import lax

CHANNELS = 128
SIDE = 8
COLUMN = 8
DEPTH = 512
ROWS = 512
FACE = 64
TABLE = 800
N_SLAB = 64
N_TILE = 8


def voxel_layout(key):
    base_key = jax.random.fold_in(key, 11)
    coin_key, pick_key, depth_key = jax.random.split(base_key, 3)
    quarter = COLUMN // 4
    slab_ramp = quarter + (COLUMN - quarter) * jnp.arange(N_SLAB, dtype=jnp.int32) // max(N_SLAB - 1, 1)
    coin_flip = jax.random.randint(coin_key, (N_SLAB, N_TILE), 0, 2)
    per_column = jnp.where(coin_flip == 0, slab_ramp[:, None], quarter).astype(jnp.int32)
    chosen = jax.random.randint(pick_key, (), 0, N_TILE)
    per_column = per_column.at[N_SLAB - 1, chosen].set(COLUMN)
    column_total = N_SLAB * N_TILE * SIDE * SIDE
    depth_keys = jax.random.split(depth_key, column_total)
    shuffled = jax.vmap(lambda one_key: jax.random.permutation(one_key, DEPTH)[:COLUMN])(depth_keys)
    shuffled = shuffled.astype(jnp.int32).reshape(N_SLAB, N_TILE, SIDE, SIDE, COLUMN)
    rank_list = jnp.arange(COLUMN, dtype=jnp.int32)
    full_shape = (N_SLAB, N_TILE, SIDE, SIDE, COLUMN)
    own_count = jnp.broadcast_to(per_column[:, :, None, None, None], full_shape)
    filled = jnp.broadcast_to(rank_list, full_shape) < own_count
    depth_pos = jnp.sort(jnp.where(filled, shuffled, DEPTH + COLUMN), axis=-1)
    local_slab = jnp.broadcast_to(jnp.arange(SIDE, dtype=jnp.int32)[None, None, :, None, None], full_shape)
    local_tile = jnp.broadcast_to(jnp.arange(SIDE, dtype=jnp.int32)[None, None, None, :, None], full_shape)
    slab_index = jnp.broadcast_to(jnp.arange(N_SLAB, dtype=jnp.int32)[:, None, None, None, None], full_shape)
    tile_index = jnp.broadcast_to(jnp.arange(N_TILE, dtype=jnp.int32)[None, :, None, None, None], full_shape)
    slab_cell = slab_index * SIDE + local_slab
    tile_cell = tile_index * SIDE + local_tile
    rank_full = jnp.broadcast_to(rank_list, full_shape)
    occupancy = jnp.full((N_SLAB * SIDE, N_TILE * SIDE, DEPTH), -1, jnp.int32)
    occupancy = occupancy.at[slab_cell, tile_cell, depth_pos].set(rank_full, mode='drop')
    tap_values = []
    for shift_slab in range(-1, 2):
        for shift_tile in range(-1, 2):
            for shift_depth in range(-1, 2):
                near_slab = local_slab + shift_slab
                near_tile = local_tile + shift_tile
                near_depth = depth_pos + shift_depth
                cell_slab = slab_cell + shift_slab
                cell_tile = tile_cell + shift_tile
                inside = (cell_slab >= 0) & (cell_slab < N_SLAB * SIDE) & (cell_tile >= 0) & (cell_tile < N_TILE * SIDE)
                inside = inside & (near_depth >= 0) & (near_depth < DEPTH) & filled
                found_rank = occupancy[jnp.clip(cell_slab, 0, N_SLAB * SIDE - 1), jnp.clip(cell_tile, 0, N_TILE * SIDE - 1), jnp.clip(near_depth, 0, DEPTH - 1)]
                present = inside & (found_rank >= 0)
                in_slab = (near_slab >= 0) & (near_slab < SIDE)
                in_tile = (near_tile >= 0) & (near_tile < SIDE)
                own_index = (near_slab * SIDE + near_tile) * own_count + found_rank
                slab_index_low = ROWS + near_tile * COLUMN + found_rank
                slab_index_high = ROWS + FACE + near_tile * COLUMN + found_rank
                tile_index_low = ROWS + 2 * FACE + (near_slab + 1) * COLUMN + found_rank
                tile_index_high = ROWS + 3 * FACE + 2 * COLUMN + (near_slab + 1) * COLUMN + found_rank
                local_index = jnp.where(in_slab & in_tile, own_index, jnp.where(in_tile, jnp.where(near_slab < 0, slab_index_low, slab_index_high), jnp.where(near_tile < 0, tile_index_low, tile_index_high)))
                tap_values.append(jnp.where(present, local_index, TABLE).astype(jnp.int32))
    stacked = jnp.stack(tap_values, axis=2)
    big_shape = (N_SLAB, N_TILE, 27, SIDE, SIDE, COLUMN)
    row_target = jnp.where(filled, (local_slab * SIDE + local_tile) * own_count + rank_full, ROWS)
    row_target = jnp.broadcast_to(row_target[:, :, None], big_shape)
    slab_target = jnp.broadcast_to(slab_index[:, :, None], big_shape)
    tile_target = jnp.broadcast_to(tile_index[:, :, None], big_shape)
    tap_target = jnp.broadcast_to(jnp.arange(27, dtype=jnp.int32)[None, None, :, None, None, None], big_shape)
    rulebook = jnp.full((N_SLAB, N_TILE, 27, ROWS), TABLE, jnp.int32)
    rulebook = rulebook.at[slab_target, tile_target, tap_target, row_target].set(stacked, mode='drop')
    along_face = jnp.arange(SIDE, dtype=jnp.int32)[None, None, :, None]
    face_rank = rank_list[None, None, None, :]
    face_count = per_column[:, :, None, None]
    face_filled = face_rank < face_count
    slab_lower = (0 * SIDE + along_face) * face_count + face_rank
    slab_upper = ((SIDE - 1) * SIDE + along_face) * face_count + face_rank
    tile_lower = (along_face * SIDE + 0) * face_count + face_rank
    tile_upper = (along_face * SIDE + SIDE - 1) * face_count + face_rank
    face_lists = []
    for face_list in (slab_lower, slab_upper, tile_lower, tile_upper):
        face_lists.append(jnp.where(face_filled, face_list, 0).reshape(N_SLAB, N_TILE, FACE))
    face_rows = jnp.stack(face_lists, axis=2).astype(jnp.int32)
    counts = (per_column * SIDE * SIDE).astype(jnp.int32)
    return (counts, rulebook, face_rows)


def draw_counts(key, part):
    return voxel_layout(key)[0]


def draw_rulebook(key, part):
    return voxel_layout(key)[1]


def draw_face_rows(key, part):
    return voxel_layout(key)[2]


def draw_features(key, part):
    noise_key, row_key, chan_key = jax.random.split(jax.random.fold_in(key, 23), 3)
    array_shape = (N_SLAB, N_TILE, ROWS, CHANNELS)
    row_scale = jnp.exp(jax.random.uniform(row_key, (N_SLAB, N_TILE, ROWS, 1), jnp.float32, math.log(0.3), math.log(3.0)))
    chan_scale = jnp.exp(jax.random.uniform(chan_key, (CHANNELS,), jnp.float32, math.log(0.5), math.log(2.0)))
    base_noise = jnp.clip(jax.random.normal(noise_key, array_shape, jnp.float32), -4.0, 4.0)
    return (base_noise * row_scale * chan_scale).astype(jnp.bfloat16)


def gaussian(own_key, extent, spread, limit, held_as=jnp.bfloat16):
    return jnp.clip(spread * jax.random.normal(own_key, extent, jnp.float32), -limit, limit).astype(held_as)


def setup_inputs(seed: int = 0) -> dict:
    streams_of = jax.random.split(jax.random.key(seed), 11)
    return {
        "features": draw_features(jax.random.fold_in(streams_of[10], 71), 0),
        "counts": draw_counts(jax.random.fold_in(streams_of[10], 71), 0),
        "rulebook": draw_rulebook(jax.random.fold_in(streams_of[10], 71), 0),
        "face_rows": draw_face_rows(jax.random.fold_in(streams_of[10], 71), 0),
        "conv_one": gaussian(streams_of[4], (27, CHANNELS, CHANNELS), (27 * CHANNELS) ** -0.5, 0.109375),
        "gain_one": jnp.clip(1.0 + 0.1 * jax.random.normal(streams_of[5], (CHANNELS,), jnp.float32), 0.5, 1.5),
        "shift_one": jnp.clip(jax.random.uniform(streams_of[6], (CHANNELS,), jnp.float32, -0.5, 0.5), -0.5, 0.5),
        "conv_two": gaussian(streams_of[7], (27, CHANNELS, CHANNELS), (27 * CHANNELS) ** -0.5, 0.109375),
        "gain_two": jnp.clip(1.0 + 0.1 * jax.random.normal(streams_of[8], (CHANNELS,), jnp.float32), 0.5, 1.5),
        "shift_two": jnp.clip(jax.random.uniform(streams_of[9], (CHANNELS,), jnp.float32, -0.5, 0.5), -0.5, 0.5),
    }


EPSILON = 1e-05

def extend(voxel_rows, face_rows):
    picked = jax.vmap(jax.vmap(lambda row_list, positions: row_list[positions]))(voxel_rows, face_rows)
    blank = jnp.zeros_like(picked[:1, :, 0])
    slab_low = jnp.concatenate([blank, picked[:-1, :, 1]], axis=0)
    slab_high = jnp.concatenate([picked[1:, :, 0], blank], axis=0)
    lower_send = jnp.concatenate([slab_low[:, :, :COLUMN], picked[:, :, 2], slab_high[:, :, :COLUMN]], axis=2)
    upper_send = jnp.concatenate([slab_low[:, :, FACE - COLUMN:], picked[:, :, 3], slab_high[:, :, FACE - COLUMN:]], axis=2)
    edge_rows = jnp.zeros_like(lower_send[:, :1])
    tile_low = jnp.concatenate([edge_rows, upper_send[:, :-1]], axis=1)
    tile_high = jnp.concatenate([lower_send[:, 1:], edge_rows], axis=1)
    zero_row = jnp.zeros_like(voxel_rows[:, :, :1])
    return jnp.concatenate([voxel_rows, slab_low, slab_high, tile_low, tile_high, zero_row], axis=2)

def convolve_all(lookup, rulebook, weight):
    device_count = N_SLAB * N_TILE
    flat_weight = weight.astype(jnp.float32).reshape(27 * CHANNELS, CHANNELS)
    tables = lookup.reshape(device_count, TABLE + 1, CHANNELS)
    indices = rulebook.reshape(device_count, 27, ROWS)

    def one_device(pair):
        table_rows, tap_rows = pair
        gathered = table_rows[tap_rows.T].reshape(ROWS, 27 * CHANNELS).astype(jnp.float32)
        return jnp.dot(gathered, flat_weight, preferred_element_type=jnp.float32)
    result = lax.map(one_device, (tables, indices))
    return result.reshape(N_SLAB, N_TILE, ROWS, CHANNELS)

def normalize(conv_out, live_mask, voxel_total, gain, shift):
    average = lax.optimization_barrier(jnp.sum(conv_out * live_mask, axis=(0, 1, 2))) / voxel_total
    centred = (conv_out - average) * live_mask
    variance = lax.optimization_barrier(jnp.sum(centred * centred, axis=(0, 1, 2))) / voxel_total
    return (conv_out - average) / jnp.sqrt(variance + EPSILON) * gain + shift

def reference(features, counts, rulebook, face_rows, conv_one, gain_one, shift_one, conv_two, gain_two, shift_two):
    live_mask = (jnp.arange(ROWS, dtype=jnp.int32)[None, None, :] < counts[:, :, None]).astype(jnp.float32)[..., None]
    voxel_total = jnp.sum(counts).astype(jnp.float32)
    first = convolve_all(extend(features, face_rows), rulebook, conv_one)
    hidden = (live_mask * jnp.maximum(normalize(first, live_mask, voxel_total, gain_one, shift_one), 0.0)).astype(jnp.bfloat16)
    second = convolve_all(extend(hidden, face_rows), rulebook, conv_two)
    summed = normalize(second, live_mask, voxel_total, gain_two, shift_two) + features.astype(jnp.float32)
    return (live_mask * jnp.maximum(summed, 0.0)).astype(jnp.bfloat16)
```

```python
from functools import partial

import jax
import jax.numpy as jnp
from jax import lax
from jax.experimental import pallas as pl
from jax.experimental.pallas import tpu as pltpu
from jax.sharding import Mesh
from jax.sharding import PartitionSpec as P

ROWS = 512
CH = 128
TAPS = 27
FACE = 64
COLUMN = 8
HALO = 2 * FACE + 2 * (FACE + 2 * COLUMN)
SLAB = ("slab_0", "slab_1", "slab_2")
EPSILON = 1e-05


def dot(a, b, **kw):
    return jnp.dot(a, b, preferred_element_type=jnp.float32, **kw)


def pick_faces(rows, faces, **kw):
    width = faces.shape[1]
    parts = []
    for k in range(faces.shape[0]):
        index = jnp.broadcast_to(faces[k : k + 1, :], (ROWS, width))
        hot = jnp.where(index == lax.broadcasted_iota(jnp.int32, (ROWS, width), 0), 1.0, 0.0)
        parts.append(
            lax.dot_general(
                hot.astype(rows.dtype), rows, (((0,), (0,)), ((), ())),
                preferred_element_type=jnp.float32, **kw,
            )
        )
    return parts


def faces_kernel(rows_ref, faces_ref, out_ref):
    parts = pick_faces(rows_ref[...], faces_ref[...])
    for k in range(4):
        out_ref[k] = parts[k].astype(out_ref.dtype)


def convolve(table_ref, rb_ref, turn_ref, gathered_ref, weight_ref):
    turn_ref[...] = jnp.zeros_like(turn_ref)
    turn_ref[0:TAPS, :] = rb_ref[...]
    turned = turn_ref[...].T
    for k in range(TAPS):
        index = turned[:, k : k + 1]
        low = jnp.broadcast_to(jnp.bitwise_and(index, ROWS - 1), (ROWS, ROWS))
        hot = jnp.where(low == lax.broadcasted_iota(jnp.int32, (ROWS, ROWS), 1), 1.0, 0.0)
        both = dot(hot.astype(jnp.bfloat16), table_ref[...])
        upper = jnp.broadcast_to(index, (ROWS, CH)) >= ROWS
        picked = jnp.where(upper, both[:, CH:], both[:, :CH])
        gathered_ref[:, k * CH : (k + 1) * CH] = picked.astype(jnp.bfloat16)
    return dot(gathered_ref[...], weight_ref[...])


def live_rows(count_ref):
    return (lax.broadcasted_iota(jnp.int32, (ROWS, 1), 0) < count_ref[0, 0]).astype(jnp.float32)


def sums_of(conv_out, live, count_ref):
    kept = conv_out * live
    first = jnp.sum(kept, axis=0, keepdims=True)
    second = jnp.sum(kept * conv_out, axis=0, keepdims=True)
    count = jnp.full((1, CH), count_ref[0, 0].astype(jnp.float32), jnp.float32)
    return jnp.concatenate([first, second, count, jnp.zeros((5, CH), jnp.float32)], axis=0)


def fill_table(table_ref, local, slab_low, slab_high, tile_low, tile_high):
    side = FACE + 2 * COLUMN
    table_ref[:, :CH] = local
    table_ref[0:FACE, CH:] = slab_low[:FACE]
    table_ref[FACE : 2 * FACE, CH:] = slab_high[:FACE]
    at = 2 * FACE
    table_ref[at : at + side, CH:] = tile_low
    table_ref[at + side : at + 2 * side, CH:] = tile_high
    table_ref[HALO:, CH:] = jnp.zeros((ROWS - HALO, CH), jnp.bfloat16)


def conv_one_kernel(
    count_ref, rows_ref, a_ref, b_ref, ql_ref, qh_ref, rb_ref, faces_ref, weight_ref,
    out_ref, sums_ref, send_ref, table_ref, turn_ref, gathered_ref,
):
    fill_table(table_ref, rows_ref[...], a_ref[...], b_ref[...], ql_ref[...], qh_ref[...])
    out = convolve(table_ref, rb_ref, turn_ref, gathered_ref, weight_ref)
    out_ref[...] = out
    sums_ref[...] = sums_of(out, live_rows(count_ref), count_ref)
    parts = pick_faces(out, faces_ref[...], precision=lax.Precision.HIGHEST)
    for k in range(4):
        send_ref[k] = parts[k]


def scale_of(sums, gain, shift):
    total = sums[2:3]
    average = sums[0:1] / total
    variance = sums[1:2] / total - average * average
    scale = lax.rsqrt(variance + EPSILON) * gain
    return average, scale, shift


def affine(values, average, scale, shift):
    return (values - average) * scale + shift


def conv_two_kernel(
    count_ref, first_ref, a_ref, b_ref, ql_ref, qh_ref, rb_ref, weight_ref, stats_ref, gain_ref, shift_ref,
    out_ref, sums_ref, table_ref, turn_ref, gathered_ref,
):
    stats = jnp.sum(stats_ref[...], axis=0)
    norm = scale_of(stats, gain_ref[...], shift_ref[...])
    live = live_rows(count_ref)

    def act(values):
        return jnp.maximum(affine(values, *norm), 0.0)

    def half(ref):
        return act(ref[...]).astype(jnp.bfloat16)

    local = (live * act(first_ref[...])).astype(jnp.bfloat16)
    fill_table(table_ref, local, half(a_ref), half(b_ref), half(ql_ref), half(qh_ref))
    out = convolve(table_ref, rb_ref, turn_ref, gathered_ref, weight_ref)
    out_ref[...] = out
    sums_ref[...] = sums_of(out, live, count_ref)


def finish_kernel(count_ref, second_ref, rows_ref, stats_ref, gain_ref, shift_ref, out_ref):
    stats = jnp.sum(stats_ref[...], axis=0)
    norm = scale_of(stats, gain_ref[...], shift_ref[...])
    summed = affine(second_ref[...], *norm) + rows_ref[...].astype(jnp.float32)
    out_ref[...] = (live_rows(count_ref) * jnp.maximum(summed, 0.0)).astype(jnp.bfloat16)


def call(kernel, outs, scratch, *args):
    specs = [
        pl.BlockSpec(memory_space=pltpu.SMEM if i == 0 and a.shape == (1, 1) else pltpu.VMEM)
        for i, a in enumerate(args)
    ]
    return pl.pallas_call(
        kernel,
        out_shape=outs,
        in_specs=specs,
        out_specs=jax.tree.map(lambda _: pl.BlockSpec(memory_space=pltpu.VMEM), outs),
        scratch_shapes=scratch,
    )(*args)


def conv_scratch():
    return [
        pltpu.VMEM((ROWS, 2 * CH), jnp.bfloat16),
        pltpu.VMEM((32, ROWS), jnp.int32),
        pltpu.VMEM((ROWS, TAPS * CH), jnp.bfloat16),
    ]


def neighbours(low_face, high_face, axis):
    count = lax.axis_size(axis)
    forward = [(i, i + 1) for i in range(count - 1)]
    backward = [(j, i) for i, j in forward]
    return lax.ppermute(high_face, axis, forward), lax.ppermute(low_face, axis, backward)


def halo(faces):
    last = FACE - COLUMN
    a, b = neighbours(faces[0], faces[1], SLAB)
    low = jnp.concatenate([a[:COLUMN], faces[2], b[:COLUMN]], axis=0)
    high = jnp.concatenate([a[last:], faces[3], b[last:]], axis=0)
    tile_low, tile_high = neighbours(low, high, "tile")
    return a, b, tile_low, tile_high


def spread(sums, axes):
    size = lax.axis_size(axes)
    block = jnp.broadcast_to(sums[None], (size, *sums.shape))
    return lax.all_to_all(block, axes, 0, 0)


def reduce_all(sums):
    near = jnp.sum(spread(sums[:3], ("slab_1", "slab_2")), axis=0)
    return spread(near, ("slab_0", "tile"))


def per_device(
    features, counts, rulebook, face_rows, conv_one, gain_one, shift_one, conv_two, gain_two, shift_two
):
    f32 = jnp.float32
    rows, faces, taps = features[0, 0], face_rows[0, 0], rulebook[0, 0]
    face_shape = jax.ShapeDtypeStruct((4, FACE, CH), jnp.bfloat16)
    picked = call(faces_kernel, face_shape, [], rows, faces)
    received = halo([picked[i] for i in range(4)])
    big = jax.ShapeDtypeStruct((ROWS, CH), f32)
    small = jax.ShapeDtypeStruct((8, CH), f32)
    first, sums, send = call(
        conv_one_kernel, (big, small, jax.ShapeDtypeStruct((4, FACE, CH), f32)), conv_scratch(),
        counts, rows, *received, taps, faces, conv_one.reshape(TAPS * CH, CH),
    )
    received = halo([send[i] for i in range(4)])
    stats = reduce_all(sums)
    second, sums = call(
        conv_two_kernel, (big, small), conv_scratch(),
        counts, first, *received, taps, conv_two.reshape(TAPS * CH, CH), stats, gain_one[None], shift_one[None],
    )
    stats = reduce_all(sums)
    out = call(
        finish_kernel, jax.ShapeDtypeStruct((ROWS, CH), jnp.bfloat16), [],
        counts, second, rows, stats, gain_two[None], shift_two[None],
    )
    return out[None, None]


def solution(mesh):
    torus = Mesh(
        mesh.devices.reshape(8, 4, 2, mesh.shape["tile"]), ("slab_0", "slab_1", "slab_2", "tile")
    )
    split = P(SLAB, "tile", None, None)
    in_specs = (split, P(SLAB, "tile"), split, split, P(), P(), P(), P(), P(), P())
    return jax.shard_map(
        per_device, mesh=torus, in_specs=in_specs, out_specs=split, check_vma=False
    )
```

```python
from functools import partial

import jax
import jax.numpy as jnp
from jax import lax
from jax.experimental import pallas as pl
from jax.experimental.pallas import tpu as pltpu
from jax.sharding import Mesh
from jax.sharding import PartitionSpec as P

ROWS = 512
CH = 128
TAPS = 27
FACE = 64
COLUMN = 8
HALO = 2 * FACE + 2 * (FACE + 2 * COLUMN)
SLAB = ("slab_0", "slab_1", "slab_2")
EPSILON = 1e-05


def dot(a, b, **kw):
    return jnp.dot(a, b, preferred_element_type=jnp.float32, **kw)


def pick_faces(rows, faces, **kw):
    width = faces.shape[1]
    parts = []
    for k in range(faces.shape[0]):
        index = jnp.broadcast_to(faces[k : k + 1, :], (ROWS, width))
        hot = jnp.where(index == lax.broadcasted_iota(jnp.int32, (ROWS, width), 0), 1.0, 0.0)
        parts.append(
            lax.dot_general(
                hot.astype(rows.dtype), rows, (((0,), (0,)), ((), ())),
                preferred_element_type=jnp.float32, **kw,
            )
        )
    return parts


def faces_kernel(rows_ref, faces_ref, *out_refs):
    for part, out_ref in zip(pick_faces(rows_ref[...], faces_ref[...]), out_refs, strict=True):
        out_ref[...] = part.astype(out_ref.dtype)


def convolve(table_ref, rb_ref, turn_ref, gathered_ref, weight_ref):
    turn_ref[...] = jnp.zeros_like(turn_ref)
    for k in range(TAPS):
        turn_ref[k : k + 1, :] = rb_ref[k]
    turned = turn_ref[...].T
    for k in range(TAPS):
        index = turned[:, k : k + 1]
        low = jnp.broadcast_to(jnp.bitwise_and(index, ROWS - 1), (ROWS, ROWS))
        hot = jnp.where(low == lax.broadcasted_iota(jnp.int32, (ROWS, ROWS), 1), 1.0, 0.0)
        both = dot(hot.astype(jnp.bfloat16), table_ref[...])
        upper = jnp.broadcast_to(index, (ROWS, CH)) >= ROWS
        picked = jnp.where(upper, both[:, CH:], both[:, :CH])
        gathered_ref[:, k * CH : (k + 1) * CH] = picked.astype(jnp.bfloat16)
    return dot(gathered_ref[...], weight_ref[...])


def live_rows(count_ref):
    return (lax.broadcasted_iota(jnp.int32, (ROWS, 1), 0) < count_ref[0, 0]).astype(jnp.float32)


def sums_of(conv_out, live, count_ref):
    kept = conv_out * live
    first = jnp.sum(kept, axis=0, keepdims=True)
    second = jnp.sum(kept * conv_out, axis=0, keepdims=True)
    count = jnp.full((1, CH), count_ref[0, 0].astype(jnp.float32), jnp.float32)
    return jnp.concatenate([first, second, count], axis=1)


def write_sums(sums_ref, sums):
    for i in range(sums_ref.shape[0]):
        sums_ref[i] = sums


def total_of(stats_ref):
    total = stats_ref[0]
    for i in range(1, stats_ref.shape[0]):
        total = total + stats_ref[i]
    return total


def near_kernel(stats_ref, out_ref):
    write_sums(out_ref, total_of(stats_ref))


def fill_table(table_ref, local, slab_low, slab_high, tile_low, tile_high):
    side = FACE + 2 * COLUMN
    table_ref[:, :CH] = local
    table_ref[0:FACE, CH:] = slab_low[:FACE]
    table_ref[FACE : 2 * FACE, CH:] = slab_high[:FACE]
    at = 2 * FACE
    table_ref[at : at + side, CH:] = tile_low
    table_ref[at + side : at + 2 * side, CH:] = tile_high
    table_ref[HALO:, CH:] = jnp.zeros((ROWS - HALO, CH), jnp.bfloat16)


def conv_one_kernel(
    count_ref, rows_ref, a_ref, b_ref, ql_ref, qh_ref, rb_ref, faces_ref, weight_ref,
    out_ref, sums_ref, send_0, send_1, send_2, send_3, table_ref, turn_ref, gathered_ref,
):
    fill_table(table_ref, rows_ref[...], a_ref[...], b_ref[...], ql_ref[...], qh_ref[...])
    out = convolve(table_ref, rb_ref, turn_ref, gathered_ref, weight_ref)
    out_ref[...] = out
    write_sums(sums_ref, sums_of(out, live_rows(count_ref), count_ref))
    parts = pick_faces(out, faces_ref[...], precision=lax.Precision.HIGHEST)
    for part, send_ref in zip(parts, (send_0, send_1, send_2, send_3), strict=True):
        send_ref[...] = part


def scale_of(sums, gain, shift):
    total = sums[:, 2 * CH :]
    average = sums[:, :CH] / total
    variance = sums[:, CH : 2 * CH] / total - average * average
    scale = lax.rsqrt(variance + EPSILON) * gain
    return average, scale, shift


def affine(values, average, scale, shift):
    return (values - average) * scale + shift


def conv_two_kernel(
    count_ref, first_ref, a_ref, b_ref, ql_ref, qh_ref, rb_ref, weight_ref, stats_ref, gain_ref, shift_ref,
    out_ref, sums_ref, table_ref, turn_ref, gathered_ref,
):
    stats = total_of(stats_ref)
    norm = scale_of(stats, gain_ref[...], shift_ref[...])
    live = live_rows(count_ref)

    def act(values):
        return jnp.maximum(affine(values, *norm), 0.0)

    def half(ref):
        return act(ref[...]).astype(jnp.bfloat16)

    local = (live * act(first_ref[...])).astype(jnp.bfloat16)
    fill_table(table_ref, local, half(a_ref), half(b_ref), half(ql_ref), half(qh_ref))
    out = convolve(table_ref, rb_ref, turn_ref, gathered_ref, weight_ref)
    out_ref[...] = out
    write_sums(sums_ref, sums_of(out, live, count_ref))


def finish_kernel(count_ref, second_ref, rows_ref, stats_ref, gain_ref, shift_ref, out_ref):
    stats = total_of(stats_ref)
    norm = scale_of(stats, gain_ref[...], shift_ref[...])
    summed = affine(second_ref[...], *norm) + rows_ref[...].astype(jnp.float32)
    out_ref[...] = (live_rows(count_ref) * jnp.maximum(summed, 0.0)).astype(jnp.bfloat16)


def call(kernel, outs, scratch, limit, *args):
    specs = [
        pl.BlockSpec(memory_space=pltpu.SMEM if i == 0 and a.shape == (1, 1) else pltpu.VMEM)
        for i, a in enumerate(args)
    ]
    return pl.pallas_call(
        kernel,
        out_shape=outs,
        in_specs=specs,
        out_specs=jax.tree.map(lambda _: pl.BlockSpec(memory_space=pltpu.VMEM), outs),
        scratch_shapes=scratch,
        compiler_params=pltpu.CompilerParams(vmem_limit_bytes=limit << 20),
    )(*args)


def conv_scratch():
    return [
        pltpu.VMEM((ROWS, 2 * CH), jnp.bfloat16),
        pltpu.VMEM((32, ROWS), jnp.int32),
        pltpu.VMEM((ROWS, TAPS * CH), jnp.bfloat16),
    ]


def neighbours(low_face, high_face, axis):
    count = lax.axis_size(axis)
    forward = [(i, i + 1) for i in range(count - 1)]
    backward = [(j, i) for i, j in forward]
    return lax.ppermute(high_face, axis, forward), lax.ppermute(low_face, axis, backward)


def halo(faces):
    last = FACE - COLUMN
    a, b = neighbours(faces[0], faces[1], SLAB)
    low = jnp.concatenate([a[:COLUMN], faces[2], b[:COLUMN]], axis=0)
    high = jnp.concatenate([a[last:], faces[3], b[last:]], axis=0)
    tile_low, tile_high = neighbours(low, high, "tile")
    return a, b, tile_low, tile_high


def reduce_all(sums):
    near = lax.all_to_all(sums, ("slab_1", "slab_2"), 0, 0)
    block = call(near_kernel, jax.ShapeDtypeStruct((64, 1, 3 * CH), jnp.float32), [], 4, near)
    return lax.all_to_all(block, ("slab_0", "tile"), 0, 0)


def per_device(
    features, counts, rulebook, face_rows, conv_one, gain_one, shift_one, conv_two, gain_two, shift_two
):
    f32 = jnp.float32
    rows, faces = features[0, 0], face_rows[0, 0]
    taps = rulebook.reshape(TAPS, 1, ROWS)
    face_shape = (jax.ShapeDtypeStruct((FACE, CH), jnp.bfloat16),) * 4
    received = halo(call(faces_kernel, face_shape, [], 4, rows, faces))
    big = jax.ShapeDtypeStruct((ROWS, CH), f32)
    small = jax.ShapeDtypeStruct((8, 1, 3 * CH), f32)
    first, sums, *send = call(
        conv_one_kernel, (big, small, *(jax.ShapeDtypeStruct((FACE, CH), f32),) * 4), conv_scratch(), 24,
        counts, rows, *received, taps, faces, conv_one.reshape(TAPS * CH, CH),
    )
    received = halo(send)
    stats = reduce_all(sums)
    second, sums = call(
        conv_two_kernel, (big, small), conv_scratch(), 24,
        counts, first, *received, taps, conv_two.reshape(TAPS * CH, CH), stats, gain_one[None], shift_one[None],
    )
    stats = reduce_all(sums)
    out = call(
        finish_kernel, jax.ShapeDtypeStruct((ROWS, CH), jnp.bfloat16), [], 4,
        counts, second, rows, stats, gain_two[None], shift_two[None],
    )
    return out[None, None]


def solution(mesh):
    torus = Mesh(
        mesh.devices.reshape(8, 4, 2, mesh.shape["tile"]), ("slab_0", "slab_1", "slab_2", "tile")
    )
    split = P(SLAB, "tile", None, None)
    in_specs = (split, P(SLAB, "tile"), split, split, P(), P(), P(), P(), P(), P())
    return jax.shard_map(
        per_device, mesh=torus, in_specs=in_specs, out_specs=split, check_vma=False
    )
```

```python
from functools import partial

import jax
import jax.numpy as jnp
from jax import lax
from jax.experimental import pallas as pl
from jax.experimental.pallas import tpu as pltpu
from jax.sharding import Mesh
from jax.sharding import PartitionSpec as P

ROWS = 512
CH = 128
TAPS = 27
SIDES = 26
CENTRE = 13
SLOTS = 32
TABLE = 800
FACE = 64
COLUMN = 8
HALO = 2 * FACE + 2 * (FACE + 2 * COLUMN)
SLAB = ("slab_0", "slab_1", "slab_2")
EPSILON = 1e-05


def dot(a, b, **kw):
    return jnp.dot(a, b, preferred_element_type=jnp.float32, **kw)


def pick_faces(rows, faces, **kw):
    width = faces.shape[1]
    parts = []
    for k in range(faces.shape[0]):
        index = jnp.broadcast_to(faces[k : k + 1, :], (ROWS, width))
        hot = jnp.where(index == lax.broadcasted_iota(jnp.int32, (ROWS, width), 0), 1.0, 0.0)
        parts.append(
            lax.dot_general(
                hot.astype(rows.dtype), rows, (((0,), (0,)), ((), ())),
                preferred_element_type=jnp.float32, **kw,
            )
        )
    return parts


def faces_kernel(rows_ref, faces_ref, *out_refs):
    for part, out_ref in zip(pick_faces(rows_ref[...], faces_ref[...]), out_refs, strict=True):
        out_ref[...] = part.astype(out_ref.dtype)


def plan_kernel(rb_ref, rank_ref, rank_t_ref, digits_ref, chunks_ref, work_ref):
    work_ref[...] = jnp.full_like(work_ref, TABLE)
    for t in range(SIDES):
        work_ref[t : t + 1, :] = rb_ref[t + (t >= CENTRE)]
    entry = work_ref[...]
    present = entry != TABLE
    ones = jnp.where(present, 1.0, 0.0)
    before = lax.broadcasted_iota(jnp.int32, (ROWS, ROWS), 0) < lax.broadcasted_iota(jnp.int32, (ROWS, ROWS), 1)
    place = dot(ones.astype(jnp.bfloat16), jnp.where(before, 1.0, 0.0).astype(jnp.bfloat16))
    rank = jnp.where(present, place.astype(jnp.int32), -1)
    rank_ref[...] = rank
    padded = jnp.concatenate([rank, jnp.full((CH - rank.shape[0], ROWS), -1, jnp.int32)], axis=0)
    rank_t_ref[...] = padded.T
    digits_ref[...] = jnp.concatenate(
        [(entry // SLOTS).astype(jnp.float32), (entry % SLOTS).astype(jnp.float32),
         jnp.zeros((CH - 2 * entry.shape[0], ROWS), jnp.float32)], axis=0
    ).astype(jnp.bfloat16)
    most = jnp.max(jnp.sum(ones, axis=1, keepdims=True))
    chunks_ref[0, 0] = (most.astype(jnp.int32) + (SLOTS - 1)) // SLOTS


def convolve(out_ref, table_ref, live, plan, weight_ref, scratch):
    rank_ref, rank_t_ref, digits_ref, chunks_ref = plan
    to_slot_ref, to_row_ref, part_ref = scratch
    out_ref[...] = dot(table_ref[:, :CH], weight_ref[CENTRE]) * live
    part_ref[SIDES * SLOTS :, :] = jnp.zeros((part_ref.shape[0] - SIDES * SLOTS, 2 * CH), jnp.bfloat16)
    total = SIDES * SLOTS

    def chunk(c, carry):
        base = c * SLOTS
        slot = lax.broadcasted_iota(jnp.int32, (SLOTS, ROWS), 0) + base
        for t in range(SIDES):
            hot = jnp.broadcast_to(rank_ref[t : t + 1, :], (SLOTS, ROWS)) == slot
            to_slot_ref[t * SLOTS : (t + 1) * SLOTS, :] = jnp.where(hot, 1.0, 0.0).astype(jnp.bfloat16)
        found = lax.dot_general(
            to_slot_ref[...], digits_ref[...], (((1,), (1,)), ((), ())), preferred_element_type=jnp.float32
        )
        tap = lax.broadcasted_iota(jnp.int32, (total, CH), 0) // SLOTS
        lane = lax.broadcasted_iota(jnp.int32, (total, CH), 1)
        worth = jnp.where(lane == tap, float(SLOTS), jnp.where(lane == tap + 32, 1.0, 0.0))
        source = jnp.sum(found * worth, axis=1, keepdims=True).astype(jnp.int32)
        low = jnp.broadcast_to(jnp.bitwise_and(source, ROWS - 1), (total, ROWS))
        hot = jnp.where(low == lax.broadcasted_iota(jnp.int32, (total, ROWS), 1), 1.0, 0.0)
        both = dot(hot.astype(jnp.bfloat16), table_ref[...])
        upper = jnp.broadcast_to(source, (total, CH)) >= ROWS
        picked = jnp.where(upper, both[:, CH:], both[:, :CH]).astype(jnp.bfloat16)
        for t in range(SIDES):
            at = slice(t * SLOTS, (t + 1) * SLOTS)
            part = dot(picked[at], weight_ref[t + (t >= CENTRE)])
            high = part.astype(jnp.bfloat16)
            part_ref[at, :CH] = high
            part_ref[at, CH:] = (part - high.astype(jnp.float32)).astype(jnp.bfloat16)
        lanes = lax.broadcasted_iota(jnp.int32, (ROWS, CH), 1)
        wanted = jnp.bitwise_and(lanes, SLOTS - 1) + base
        for i in range(part_ref.shape[0] // CH):
            spread = jnp.take_along_axis(
                rank_t_ref[...], lanes // SLOTS + i * (CH // SLOTS), axis=1, mode="promise_in_bounds"
            )
            to_row_ref[:, i * CH : (i + 1) * CH] = jnp.where(spread == wanted, 1.0, 0.0).astype(jnp.bfloat16)
        added = dot(to_row_ref[...], part_ref[...])
        out_ref[...] += added[:, :CH] + added[:, CH:]
        return carry

    lax.fori_loop(0, chunks_ref[0, 0], chunk, 0)


def live_rows(count_ref):
    return (lax.broadcasted_iota(jnp.int32, (ROWS, 1), 0) < count_ref[0, 0]).astype(jnp.float32)


def sums_of(conv_out, live, count_ref):
    kept = conv_out * live
    first = jnp.sum(kept, axis=0, keepdims=True)
    second = jnp.sum(kept * conv_out, axis=0, keepdims=True)
    count = jnp.full((1, CH), count_ref[0, 0].astype(jnp.float32), jnp.float32)
    return jnp.concatenate([first, second, count], axis=1)


def write_sums(sums_ref, sums):
    for i in range(sums_ref.shape[0]):
        sums_ref[i] = sums


def total_of(stats_ref):
    total = stats_ref[0]
    for i in range(1, stats_ref.shape[0]):
        total = total + stats_ref[i]
    return total


def near_kernel(stats_ref, out_ref):
    write_sums(out_ref, total_of(stats_ref))


def fill_table(table_ref, local, slab_low, slab_high, tile_low, tile_high):
    side = FACE + 2 * COLUMN
    table_ref[:, :CH] = local
    table_ref[0:FACE, CH:] = slab_low[:FACE]
    table_ref[FACE : 2 * FACE, CH:] = slab_high[:FACE]
    at = 2 * FACE
    table_ref[at : at + side, CH:] = tile_low
    table_ref[at + side : at + 2 * side, CH:] = tile_high
    table_ref[HALO:, CH:] = jnp.zeros((ROWS - HALO, CH), jnp.bfloat16)


def conv_one_kernel(
    count_ref, chunks_ref, rows_ref, a_ref, b_ref, ql_ref, qh_ref, rank_ref, rank_t_ref, digits_ref, faces_ref, weight_ref,
    out_ref, sums_ref, send_0, send_1, send_2, send_3, table_ref, *scratch,
):
    fill_table(table_ref, rows_ref[...], a_ref[...], b_ref[...], ql_ref[...], qh_ref[...])
    live = live_rows(count_ref)
    convolve(out_ref, table_ref, live, (rank_ref, rank_t_ref, digits_ref, chunks_ref), weight_ref, scratch)
    out = out_ref[...]
    write_sums(sums_ref, sums_of(out, live, count_ref))
    parts = pick_faces(out, faces_ref[...], precision=lax.Precision.HIGHEST)
    for part, send_ref in zip(parts, (send_0, send_1, send_2, send_3), strict=True):
        send_ref[...] = part


def scale_of(sums, gain, shift):
    total = sums[:, 2 * CH :]
    average = sums[:, :CH] / total
    variance = sums[:, CH : 2 * CH] / total - average * average
    scale = lax.rsqrt(variance + EPSILON) * gain
    return average, scale, shift


def affine(values, average, scale, shift):
    return (values - average) * scale + shift


def conv_two_kernel(
    count_ref, chunks_ref, first_ref, a_ref, b_ref, ql_ref, qh_ref, rank_ref, rank_t_ref, digits_ref, weight_ref,
    stats_ref, gain_ref, shift_ref, out_ref, sums_ref, table_ref, *scratch,
):
    norm = scale_of(total_of(stats_ref), gain_ref[...], shift_ref[...])
    live = live_rows(count_ref)

    def act(values):
        return jnp.maximum(affine(values, *norm), 0.0)

    def half(ref):
        return act(ref[...]).astype(jnp.bfloat16)

    local = (live * act(first_ref[...])).astype(jnp.bfloat16)
    fill_table(table_ref, local, half(a_ref), half(b_ref), half(ql_ref), half(qh_ref))
    convolve(out_ref, table_ref, live, (rank_ref, rank_t_ref, digits_ref, chunks_ref), weight_ref, scratch)
    write_sums(sums_ref, sums_of(out_ref[...], live, count_ref))


def finish_kernel(count_ref, second_ref, rows_ref, stats_ref, gain_ref, shift_ref, out_ref):
    stats = total_of(stats_ref)
    norm = scale_of(stats, gain_ref[...], shift_ref[...])
    summed = affine(second_ref[...], *norm) + rows_ref[...].astype(jnp.float32)
    out_ref[...] = (live_rows(count_ref) * jnp.maximum(summed, 0.0)).astype(jnp.bfloat16)


def call(kernel, outs, scratch, limit, *args):
    def spec(shape):
        return pl.BlockSpec(memory_space=pltpu.SMEM if shape == (1, 1) else pltpu.VMEM)

    return pl.pallas_call(
        kernel,
        out_shape=outs,
        in_specs=[spec(a.shape) for a in args],
        out_specs=jax.tree.map(lambda o: spec(o.shape), outs),
        scratch_shapes=scratch,
        compiler_params=pltpu.CompilerParams(vmem_limit_bytes=limit << 20),
    )(*args)


def conv_scratch():
    padded = -(-SIDES * SLOTS // CH) * CH
    return [
        pltpu.VMEM((ROWS, 2 * CH), jnp.bfloat16),
        pltpu.VMEM((SIDES * SLOTS, ROWS), jnp.bfloat16),
        pltpu.VMEM((ROWS, padded), jnp.bfloat16),
        pltpu.VMEM((padded, 2 * CH), jnp.bfloat16),
    ]


def neighbours(low_face, high_face, axis):
    count = lax.axis_size(axis)
    forward = [(i, i + 1) for i in range(count - 1)]
    backward = [(j, i) for i, j in forward]
    return lax.ppermute(high_face, axis, forward), lax.ppermute(low_face, axis, backward)


def halo(faces):
    last = FACE - COLUMN
    a, b = neighbours(faces[0], faces[1], SLAB)
    low = jnp.concatenate([a[:COLUMN], faces[2], b[:COLUMN]], axis=0)
    high = jnp.concatenate([a[last:], faces[3], b[last:]], axis=0)
    tile_low, tile_high = neighbours(low, high, "tile")
    return a, b, tile_low, tile_high


def reduce_all(sums):
    near = lax.all_to_all(sums, ("slab_1", "slab_2"), 0, 0)
    block = call(near_kernel, jax.ShapeDtypeStruct((64, 1, 3 * CH), jnp.float32), [], 4, near)
    return lax.all_to_all(block, ("slab_0", "tile"), 0, 0)


def per_device(
    features, counts, rulebook, face_rows, conv_one, gain_one, shift_one, conv_two, gain_two, shift_two
):
    f32 = jnp.float32
    rows, faces = features[0, 0], face_rows[0, 0]
    taps = rulebook.reshape(TAPS, 1, ROWS)
    face_shape = (jax.ShapeDtypeStruct((FACE, CH), jnp.bfloat16),) * 4
    received = halo(call(faces_kernel, face_shape, [], 4, rows, faces))
    plan_shape = (
        jax.ShapeDtypeStruct((32, ROWS), jnp.int32),
        jax.ShapeDtypeStruct((ROWS, CH), jnp.int32),
        jax.ShapeDtypeStruct((CH, ROWS), jnp.bfloat16),
        jax.ShapeDtypeStruct((1, 1), jnp.int32),
    )
    *plan, chunks = call(plan_kernel, plan_shape, [pltpu.VMEM((32, ROWS), jnp.int32)], 8, taps)
    big = jax.ShapeDtypeStruct((ROWS, CH), f32)
    small = jax.ShapeDtypeStruct((8, 1, 3 * CH), f32)
    first, sums, *send = call(
        conv_one_kernel, (big, small, *(jax.ShapeDtypeStruct((FACE, CH), f32),) * 4), conv_scratch(), 24,
        counts, chunks, rows, *received, *plan, faces, conv_one,
    )
    received = halo(send)
    stats = reduce_all(sums)
    second, sums = call(
        conv_two_kernel, (big, small), conv_scratch(), 24,
        counts, chunks, first, *received, *plan, conv_two, stats, gain_one[None], shift_one[None],
    )
    stats = reduce_all(sums)
    out = call(
        finish_kernel, jax.ShapeDtypeStruct((ROWS, CH), jnp.bfloat16), [], 4,
        counts, second, rows, stats, gain_two[None], shift_two[None],
    )
    return out[None, None]


def solution(mesh):
    torus = Mesh(
        mesh.devices.reshape(8, 4, 2, mesh.shape["tile"]), ("slab_0", "slab_1", "slab_2", "tile")
    )
    split = P(SLAB, "tile", None, None)
    in_specs = (split, P(SLAB, "tile"), split, split, P(), P(), P(), P(), P(), P())
    return jax.shard_map(
        per_device, mesh=torus, in_specs=in_specs, out_specs=split, check_vma=False
    )
```

```python
import jax
import jax.numpy as jnp
from jax import lax
from jax.experimental import pallas as pl
from jax.experimental.pallas import tpu as pltpu
from jax.sharding import Mesh
from jax.sharding import PartitionSpec as P

ROWS = 512
CH = 128
TAPS = 27
SIDES = 26
CENTRE = 13
SLOTS = 32
TABLE = 800
FACE = 64
COLUMN = 8
HALO = 2 * FACE + 2 * (FACE + 2 * COLUMN)
SLAB = ("slab_0", "slab_1", "slab_2")
EPSILON = 1e-05


def dot(a, b, **kw):
    return jnp.dot(a, b, preferred_element_type=jnp.float32, **kw)


def pick_faces(rows, faces, **kw):
    width = faces.shape[1]
    parts = []
    for k in range(faces.shape[0]):
        index = jnp.broadcast_to(faces[k : k + 1, :], (ROWS, width))
        hot = jnp.where(index == lax.broadcasted_iota(jnp.int32, (ROWS, width), 0), 1.0, 0.0)
        parts.append(
            lax.dot_general(
                hot.astype(rows.dtype), rows, (((0,), (0,)), ((), ())),
                preferred_element_type=jnp.float32, **kw,
            )
        )
    return parts


def fetch(pairs, sems):
    copies = [pltpu.make_async_copy(src, dst, sems.at[i]) for i, (src, dst) in enumerate(pairs)]
    for copy in copies:
        copy.start()
    return copies


def faces_kernel(rows_hbm, faces_hbm, rows_ref, faces_ref, p0, p1, p2, p3, sems):
    for copy in fetch([(rows_hbm, rows_ref), (faces_hbm, faces_ref)], sems):
        copy.wait()
    for part, out_ref in zip(pick_faces(rows_ref[...], faces_ref[...]), (p0, p1, p2, p3), strict=True):
        out_ref[...] = part.astype(out_ref.dtype)


def plan_kernel(*refs):
    rb_hbm, *params_hbm = refs[:7]
    rank_ref, rank_t_ref, digits_ref, chunks_ref, *params = refs[7:17]
    rb_ref, work_ref, sems = refs[17:]
    first, *others = fetch([(rb_hbm, rb_ref), *zip(params_hbm, params, strict=True)], sems)
    first.wait()
    work_ref[...] = jnp.full_like(work_ref, TABLE)
    for t in range(SIDES):
        work_ref[t : t + 1, :] = rb_ref[t + (t >= CENTRE)]
    entry = work_ref[...]
    present = entry != TABLE
    ones = jnp.where(present, 1.0, 0.0)
    before = lax.broadcasted_iota(jnp.int32, (ROWS, ROWS), 0) < lax.broadcasted_iota(jnp.int32, (ROWS, ROWS), 1)
    place = dot(ones.astype(jnp.bfloat16), jnp.where(before, 1.0, 0.0).astype(jnp.bfloat16))
    rank = jnp.where(present, place.astype(jnp.int32), -1)
    rank_ref[...] = rank
    padded = jnp.concatenate([rank, jnp.full((CH - rank.shape[0], ROWS), -1, jnp.int32)], axis=0)
    rank_t_ref[...] = padded.T
    digits_ref[...] = jnp.concatenate(
        [(entry // SLOTS).astype(jnp.float32), (entry % SLOTS).astype(jnp.float32),
         jnp.zeros((CH - 2 * entry.shape[0], ROWS), jnp.float32)], axis=0
    ).astype(jnp.bfloat16)
    most = jnp.max(jnp.sum(ones, axis=1, keepdims=True))
    chunks_ref[0, 0] = (most.astype(jnp.int32) + (SLOTS - 1)) // SLOTS
    for copy in others:
        copy.wait()


def convolve(out_ref, table_ref, live, plan, weight_ref, scratch):
    rank_ref, rank_t_ref, digits_ref, chunks_ref = plan
    to_slot_ref, to_row_ref, part_ref = scratch
    out_ref[...] = dot(table_ref[:, :CH], weight_ref[CENTRE]) * live
    part_ref[SIDES * SLOTS :, :] = jnp.zeros((part_ref.shape[0] - SIDES * SLOTS, 2 * CH), jnp.bfloat16)
    total = SIDES * SLOTS

    def chunk(c, carry):
        base = c * SLOTS
        slot = lax.broadcasted_iota(jnp.int32, (SLOTS, ROWS), 0) + base
        for t in range(SIDES):
            hot = jnp.broadcast_to(rank_ref[t : t + 1, :], (SLOTS, ROWS)) == slot
            to_slot_ref[t * SLOTS : (t + 1) * SLOTS, :] = jnp.where(hot, 1.0, 0.0).astype(jnp.bfloat16)
        found = lax.dot_general(
            to_slot_ref[...], digits_ref[...], (((1,), (1,)), ((), ())), preferred_element_type=jnp.float32
        )
        tap = lax.broadcasted_iota(jnp.int32, (total, CH), 0) // SLOTS
        lane = lax.broadcasted_iota(jnp.int32, (total, CH), 1)
        worth = jnp.where(lane == tap, float(SLOTS), jnp.where(lane == tap + 32, 1.0, 0.0))
        source = jnp.sum(found * worth, axis=1, keepdims=True).astype(jnp.int32)
        low = jnp.broadcast_to(jnp.bitwise_and(source, ROWS - 1), (total, ROWS))
        hot = jnp.where(low == lax.broadcasted_iota(jnp.int32, (total, ROWS), 1), 1.0, 0.0)
        both = dot(hot.astype(jnp.bfloat16), table_ref[...])
        upper = jnp.broadcast_to(source, (total, CH)) >= ROWS
        picked = jnp.where(upper, both[:, CH:], both[:, :CH]).astype(jnp.bfloat16)
        for t in range(SIDES):
            at = slice(t * SLOTS, (t + 1) * SLOTS)
            part = dot(picked[at], weight_ref[t + (t >= CENTRE)])
            high = part.astype(jnp.bfloat16)
            part_ref[at, :CH] = high
            part_ref[at, CH:] = (part - high.astype(jnp.float32)).astype(jnp.bfloat16)
        lanes = lax.broadcasted_iota(jnp.int32, (ROWS, CH), 1)
        wanted = jnp.bitwise_and(lanes, SLOTS - 1) + base
        for i in range(part_ref.shape[0] // CH):
            spread = jnp.take_along_axis(
                rank_t_ref[...], lanes // SLOTS + i * (CH // SLOTS), axis=1, mode="promise_in_bounds"
            )
            to_row_ref[:, i * CH : (i + 1) * CH] = jnp.where(spread == wanted, 1.0, 0.0).astype(jnp.bfloat16)
        added = dot(to_row_ref[...], part_ref[...])
        out_ref[...] += added[:, :CH] + added[:, CH:]
        return carry

    lax.fori_loop(0, chunks_ref[0, 0], chunk, 0)


def live_rows(count_ref):
    return (lax.broadcasted_iota(jnp.int32, (ROWS, 1), 0) < count_ref[0, 0]).astype(jnp.float32)


def sums_of(conv_out, live, count_ref):
    kept = conv_out * live
    first = jnp.sum(kept, axis=0, keepdims=True)
    second = jnp.sum(kept * conv_out, axis=0, keepdims=True)
    count = jnp.full((1, CH), count_ref[0, 0].astype(jnp.float32), jnp.float32)
    return jnp.concatenate([first, second, count], axis=1)


def write_sums(sums_ref, sums):
    for i in range(sums_ref.shape[0]):
        sums_ref[i] = sums


def total_of(stats_ref):
    total = stats_ref[0]
    for i in range(1, stats_ref.shape[0]):
        total = total + stats_ref[i]
    return total


def near_kernel(stats_ref, out_ref):
    write_sums(out_ref, total_of(stats_ref))


def fill_table(table_ref, local, slab_low, slab_high, tile_low, tile_high):
    side = FACE + 2 * COLUMN
    table_ref[:, :CH] = local
    table_ref[0:FACE, CH:] = slab_low[:FACE]
    table_ref[FACE : 2 * FACE, CH:] = slab_high[:FACE]
    at = 2 * FACE
    table_ref[at : at + side, CH:] = tile_low
    table_ref[at + side : at + 2 * side, CH:] = tile_high
    table_ref[HALO:, CH:] = jnp.zeros((ROWS - HALO, CH), jnp.bfloat16)


def conv_one_kernel(
    count_ref, chunks_ref, rows_ref, a_ref, b_ref, ql_ref, qh_ref, rank_ref, rank_t_ref, digits_ref, faces_ref, weight_ref,
    out_ref, sums_ref, send_0, send_1, send_2, send_3, table_ref, *scratch,
):
    fill_table(table_ref, rows_ref[...], a_ref[...], b_ref[...], ql_ref[...], qh_ref[...])
    live = live_rows(count_ref)
    convolve(out_ref, table_ref, live, (rank_ref, rank_t_ref, digits_ref, chunks_ref), weight_ref, scratch)
    out = out_ref[...]
    write_sums(sums_ref, sums_of(out, live, count_ref))
    parts = pick_faces(out, faces_ref[...], precision=lax.Precision.HIGHEST)
    for part, send_ref in zip(parts, (send_0, send_1, send_2, send_3), strict=True):
        send_ref[...] = part


def scale_of(sums, gain, shift):
    total = sums[:, 2 * CH :]
    average = sums[:, :CH] / total
    variance = sums[:, CH : 2 * CH] / total - average * average
    scale = lax.rsqrt(variance + EPSILON) * gain
    return average, scale, shift


def affine(values, average, scale, shift):
    return (values - average) * scale + shift


def conv_two_kernel(
    count_ref, chunks_ref, first_ref, a_ref, b_ref, ql_ref, qh_ref, rank_ref, rank_t_ref, digits_ref, weight_ref,
    stats_ref, gain_ref, shift_ref, out_ref, sums_ref, table_ref, *scratch,
):
    norm = scale_of(total_of(stats_ref), gain_ref[...], shift_ref[...])
    live = live_rows(count_ref)

    def act(values):
        return jnp.maximum(affine(values, *norm), 0.0)

    def half(ref):
        return act(ref[...]).astype(jnp.bfloat16)

    local = (live * act(first_ref[...])).astype(jnp.bfloat16)
    fill_table(table_ref, local, half(a_ref), half(b_ref), half(ql_ref), half(qh_ref))
    convolve(out_ref, table_ref, live, (rank_ref, rank_t_ref, digits_ref, chunks_ref), weight_ref, scratch)
    write_sums(sums_ref, sums_of(out_ref[...], live, count_ref))


def finish_kernel(count_ref, second_ref, rows_ref, stats_ref, gain_ref, shift_ref, out_ref):
    stats = total_of(stats_ref)
    norm = scale_of(stats, gain_ref[...], shift_ref[...])
    summed = affine(second_ref[...], *norm) + rows_ref[...].astype(jnp.float32)
    out_ref[...] = (live_rows(count_ref) * jnp.maximum(summed, 0.0)).astype(jnp.bfloat16)


def call(kernel, outs, scratch, limit, *args, hbm=False):
    def spec(shape):
        if hbm:
            return pl.BlockSpec(memory_space=pltpu.HBM)
        return out_spec(shape)

    def out_spec(shape):
        return pl.BlockSpec(memory_space=pltpu.SMEM if shape == (1, 1) else pltpu.VMEM)

    if hbm:
        args = [pltpu.with_memory_space_constraint(a, pltpu.HBM) for a in args]
    return pl.pallas_call(
        kernel,
        out_shape=outs,
        in_specs=[spec(a.shape) for a in args],
        out_specs=jax.tree.map(lambda o: out_spec(o.shape), outs),
        scratch_shapes=scratch,
        compiler_params=pltpu.CompilerParams(vmem_limit_bytes=limit << 20),
    )(*args)


def conv_scratch():
    padded = -(-SIDES * SLOTS // CH) * CH
    return [
        pltpu.VMEM((ROWS, 2 * CH), jnp.bfloat16),
        pltpu.VMEM((SIDES * SLOTS, ROWS), jnp.bfloat16),
        pltpu.VMEM((ROWS, padded), jnp.bfloat16),
        pltpu.VMEM((padded, 2 * CH), jnp.bfloat16),
    ]


def slab_neighbours(low_face, high_face):
    count = lax.axis_size(SLAB)
    even = lax.axis_index("slab_2") == 0
    partner = [(i, i ^ 1) for i in range(count)]
    across = [(i, i + 1) for i in range(1, count - 1, 2)] + [(i + 1, i) for i in range(1, count - 1, 2)]
    near = lax.ppermute(jnp.where(even, high_face, low_face), SLAB, partner)
    far = lax.ppermute(jnp.where(even, low_face, high_face), SLAB, across)
    return jnp.where(even, far, near), jnp.where(even, near, far)


def tile_neighbours(low_face, high_face):
    count = lax.axis_size("tile")
    forward = [(i, i + 1) for i in range(count - 1)]
    backward = [(j, i) for i, j in forward]
    low = lax.ppermute(high_face, "tile", forward)
    high = lax.ppermute(low_face, "tile", backward)
    return low, high


def halo(faces):
    last = FACE - COLUMN
    a, b = slab_neighbours(faces[0], faces[1])
    low = jnp.concatenate([a[:COLUMN], faces[2], b[:COLUMN]], axis=0)
    high = jnp.concatenate([a[last:], faces[3], b[last:]], axis=0)
    tile_low, tile_high = tile_neighbours(low, high)
    return a, b, tile_low, tile_high


def reduce_all(sums):
    near = lax.all_to_all(sums, ("slab_1", "slab_2"), 0, 0)
    block = call(near_kernel, jax.ShapeDtypeStruct((64, 1, 3 * CH), jnp.float32), [], 4, near)
    return lax.all_to_all(block, ("slab_0", "tile"), 0, 0)


def per_device(
    features, counts, rulebook, face_rows, conv_one, gain_one, shift_one, conv_two, gain_two, shift_two
):
    f32, bf16, i32 = jnp.float32, jnp.bfloat16, jnp.int32
    shaped = jax.ShapeDtypeStruct
    dma = pltpu.SemaphoreType.DMA
    outs = (shaped((ROWS, CH), bf16), shaped((4, FACE), i32), *(shaped((FACE, CH), bf16),) * 4)
    rows, faces, *picked = call(faces_kernel, outs, [dma((2,))], 4, features[0, 0], face_rows[0, 0], hbm=True)
    received = halo(picked)
    params = (conv_one, conv_two, gain_one[None], shift_one[None], gain_two[None], shift_two[None])
    outs = (
        shaped((32, ROWS), i32), shaped((ROWS, CH), i32), shaped((CH, ROWS), bf16), shaped((1, 1), i32),
        *(shaped(p.shape, p.dtype) for p in params),
    )
    scratch = [pltpu.VMEM((TAPS, 1, ROWS), i32), pltpu.VMEM((32, ROWS), i32), dma((7,))]
    *plan, chunks, weight_one, weight_two, gain_one, shift_one, gain_two, shift_two = call(
        plan_kernel, outs, scratch, 8, rulebook.reshape(TAPS, 1, ROWS), *params, hbm=True
    )
    big = shaped((ROWS, CH), f32)
    small = shaped((8, 1, 3 * CH), f32)
    first, sums, *send = call(
        conv_one_kernel, (big, small, *(shaped((FACE, CH), f32),) * 4), conv_scratch(), 24,
        counts, chunks, rows, *received, *plan, faces, weight_one,
    )
    received = halo(send)
    stats = reduce_all(sums)
    second, sums = call(
        conv_two_kernel, (big, small), conv_scratch(), 24,
        counts, chunks, first, *received, *plan, weight_two, stats, gain_one, shift_one,
    )
    stats = reduce_all(sums)
    out = call(
        finish_kernel, shaped((ROWS, CH), bf16), [], 4, counts, second, rows, stats, gain_two, shift_two
    )
    return out[None, None]


def solution(mesh):
    torus = Mesh(
        mesh.devices.reshape(8, 4, 2, mesh.shape["tile"]), ("slab_0", "slab_1", "slab_2", "tile")
    )
    split = P(SLAB, "tile", None, None)
    in_specs = (split, P(SLAB, "tile"), split, split, P(), P(), P(), P(), P(), P())
    return jax.shard_map(
        per_device, mesh=torus, in_specs=in_specs, out_specs=split, check_vma=False
    )
```

```python
import jax
import jax.numpy as jnp
from jax import lax
from jax.experimental import pallas as pl
from jax.experimental.pallas import tpu as pltpu
from jax.sharding import Mesh
from jax.sharding import PartitionSpec as P

ROWS = 512
CH = 128
TAPS = 27
SIDES = 26
CENTRE = 13
SLOTS = 32
TABLE = 800
FACE = 64
COLUMN = 8
SIDE_ROWS = FACE + 2 * COLUMN
HALO = 2 * FACE + 2 * SIDE_ROWS
EXT = 832
SLAB = ("slab_0", "slab_1", "slab_2")
EPSILON = 1e-05


A, B, QH, QL = ROWS, ROWS + FACE, ROWS + 2 * FACE, ROWS + 2 * FACE + SIDE_ROWS


def dot(a, b, **kw):
    return jnp.dot(a, b, preferred_element_type=jnp.float32, **kw)


def hot(index, shape, dim):
    return jnp.where(jnp.broadcast_to(index, shape) == lax.broadcasted_iota(jnp.int32, shape, dim), 1.0, 0.0).astype(
        jnp.bfloat16
    )


def fetch(pairs, sems):
    copies = [pltpu.make_async_copy(src, dst, sems.at[i]) for i, (src, dst) in enumerate(pairs)]
    for copy in copies:
        copy.start()
    return copies


def thirds(values):
    high = values.astype(jnp.bfloat16)
    rest = values - high.astype(jnp.float32)
    mid = rest.astype(jnp.bfloat16)
    return high, mid, (rest - mid.astype(jnp.float32)).astype(jnp.bfloat16)


def face_hot(faces_ref, k):
    return hot(jnp.concatenate([faces_ref[k : k + 1, :], faces_ref[k + 1 : k + 2, :]], axis=1), (ROWS, 2 * FACE), 0)


def pick(selector, rows):
    got = lax.dot_general(
        selector, jnp.concatenate(thirds(rows), axis=1), (((0,), (0,)), ((), ())), preferred_element_type=jnp.float32
    )
    return got[:, :CH] + got[:, CH : 2 * CH] + got[:, 2 * CH :]


def put(selector, values):
    return dot(jnp.concatenate([selector] * 3, axis=1), jnp.concatenate(thirds(values), axis=0))


def plan_pairs(rb_ref, work_ref, rank_ref, rank_t_ref, digits_ref, chunks_ref):
    work_ref[...] = jnp.full_like(work_ref, TABLE)
    for t in range(SIDES):
        work_ref[t : t + 1, :] = rb_ref[t + (t >= CENTRE)]
    entry = work_ref[...]
    present = entry != TABLE
    ones = jnp.where(present, 1.0, 0.0)
    before = lax.broadcasted_iota(jnp.int32, (ROWS, ROWS), 0) < lax.broadcasted_iota(jnp.int32, (ROWS, ROWS), 1)
    place = dot(ones.astype(jnp.bfloat16), jnp.where(before, 1.0, 0.0).astype(jnp.bfloat16))
    rank = jnp.where(present, place.astype(jnp.int32), -1)
    rank_ref[...] = rank
    padded = jnp.concatenate([rank, jnp.full((CH - rank.shape[0], ROWS), -1, jnp.int32)], axis=0)
    rank_t_ref[...] = padded.T
    digits_ref[...] = jnp.concatenate(
        [(entry // SLOTS).astype(jnp.float32), (entry % SLOTS).astype(jnp.float32),
         jnp.zeros((CH - 2 * entry.shape[0], ROWS), jnp.float32)], axis=0
    ).astype(jnp.bfloat16)
    most = jnp.max(jnp.sum(ones, axis=1, keepdims=True))
    chunks_ref[0, 0] = (most.astype(jnp.int32) + (SLOTS - 1)) // SLOTS


def slots_of_rows(rank_ref, base, to_slot_ref):
    slot = lax.broadcasted_iota(jnp.int32, (SLOTS, ROWS), 0) + base
    for t in range(SIDES):
        match = jnp.broadcast_to(rank_ref[t : t + 1, :], (SLOTS, ROWS)) == slot
        to_slot_ref[t * SLOTS : (t + 1) * SLOTS, :] = jnp.where(match, 1.0, 0.0).astype(jnp.bfloat16)


def rows_of_slots(rank_t_ref, base, to_row_ref):
    lanes = lax.broadcasted_iota(jnp.int32, (ROWS, CH), 1)
    wanted = jnp.bitwise_and(lanes, SLOTS - 1) + base
    for i in range(to_row_ref.shape[1] // CH):
        spread = jnp.take_along_axis(
            rank_t_ref[...], lanes // SLOTS + i * (CH // SLOTS), axis=1, mode="promise_in_bounds"
        )
        to_row_ref[:, i * CH : (i + 1) * CH] = jnp.where(spread == wanted, 1.0, 0.0).astype(jnp.bfloat16)


def multiply_slots(picked, weight_ref, tap_of, part_ref):
    for t in range(SIDES):
        at = slice(t * SLOTS, (t + 1) * SLOTS)
        part = dot(picked[at], weight_ref[tap_of(t)])
        high = part.astype(jnp.bfloat16)
        part_ref[at, :CH] = high
        part_ref[at, CH:] = (part - high.astype(jnp.float32)).astype(jnp.bfloat16)


def clear_padding(part_ref):
    part_ref[SIDES * SLOTS :, :] = jnp.zeros((part_ref.shape[0] - SIDES * SLOTS, 2 * CH), jnp.bfloat16)


def spread_kernel(count_ref, *refs):
    (rb_hbm, rows_hbm, weight_hbm, faces_hbm, *params_hbm) = refs[:9]
    out_ref, up_ref, down_ref, rank_ref, rank_t_ref, digits_ref, chunks_ref, rows_ref, faces_ref, *params = refs[9:23]
    rb_ref, weight_ref, work_ref, to_slot_ref, to_row_ref, part_ref, sems = refs[23:]
    rb_copy, rows_copy, weight_copy, *others = fetch(
        [(rb_hbm, rb_ref), (rows_hbm, rows_ref), (weight_hbm, weight_ref), (faces_hbm, faces_ref),
         *zip(params_hbm, params, strict=True)], sems,
    )
    rb_copy.wait()
    plan_pairs(rb_ref, work_ref, rank_ref, rank_t_ref, digits_ref, chunks_ref)
    clear_padding(part_ref)
    rows_copy.wait()
    weight_copy.wait()
    out_ref[:ROWS] = dot(rows_ref[...], weight_ref[CENTRE]) * live_rows(count_ref)
    out_ref[ROWS:] = jnp.zeros((EXT - ROWS, CH), jnp.float32)
    slots = part_ref.shape[0]

    def chunk(c, carry):
        slots_of_rows(rank_ref, c * SLOTS, to_slot_ref)
        picked = dot(to_slot_ref[...], rows_ref[...]).astype(jnp.bfloat16)
        multiply_slots(picked, weight_ref, lambda t: TAPS - 1 - (t + (t >= CENTRE)), part_ref)
        rows_of_slots(rank_t_ref, c * SLOTS, to_row_ref)
        found = dot(digits_ref[...], to_row_ref[...])
        digit = lax.broadcasted_iota(jnp.int32, (CH, slots), 0)
        tap = lax.broadcasted_iota(jnp.int32, (CH, slots), 1) // SLOTS
        worth = jnp.where(digit == tap, float(SLOTS), jnp.where(digit == tap + 32, 1.0, 0.0))
        target = jnp.sum(found * worth, axis=0, keepdims=True).astype(jnp.int32)
        added = dot(hot(target, (EXT, slots), 0), part_ref[...])
        out_ref[...] += added[:, :CH] + added[:, CH:]
        return carry

    lax.fori_loop(0, chunks_ref[0, 0], chunk, 0)
    for copy in others:
        copy.wait()
    picked = pick(face_hot(faces_ref, 2), out_ref[:ROWS])
    for ref, own, at, far in ((down_ref, picked[:FACE], 0, QH), (up_ref, picked[FACE:], FACE - COLUMN, QL)):
        ref[:COLUMN] = out_ref[A + at : A + at + COLUMN]
        ref[COLUMN : COLUMN + FACE] = own
        ref[COLUMN + FACE : SIDE_ROWS] = out_ref[B + at : B + at + COLUMN]
        ref[SIDE_ROWS:] = out_ref[far : far + SIDE_ROWS]


def tile_kernel(sums_ref, low_ref, high_ref, faces_ref, out_ref, left_ref, right_ref):
    out_ref[...] = sums_ref[...]
    first, last = SIDE_ROWS + COLUMN, SIDE_ROWS + COLUMN + FACE
    out_ref[QH:QL] += low_ref[:SIDE_ROWS]
    out_ref[QL : QL + SIDE_ROWS] += high_ref[:SIDE_ROWS]
    for ref, at in ((low_ref, 0), (high_ref, FACE - COLUMN)):
        out_ref[A + at : A + at + COLUMN] += ref[SIDE_ROWS:first]
        out_ref[B + at : B + at + COLUMN] += ref[last:]
    out_ref[:ROWS] += put(face_hot(faces_ref, 2), jnp.concatenate([low_ref[first:last], high_ref[first:last]], axis=0))
    picked = pick(face_hot(faces_ref, 0), out_ref[:ROWS])
    for ref, own, own_at, far, far_at in (
        (left_ref, picked[:FACE], COLUMN, A, 0),
        (right_ref, picked[FACE:], FACE, B, FACE + COLUMN),
    ):
        ref[:FACE] = own
        ref[SIDE_ROWS : SIDE_ROWS + FACE] = out_ref[far : far + FACE]
        for start, at in ((0, own_at), (SIDE_ROWS, far_at)):
            ref[start + FACE : start + FACE + COLUMN] = out_ref[QH + at : QH + at + COLUMN]
            ref[start + FACE + COLUMN : start + SIDE_ROWS] = out_ref[QL + at : QL + at + COLUMN]


def slab_kernel(count_ref, sums_ref, low_ref, high_ref, faces_ref, out_ref, stats_ref):
    out_ref[...] = sums_ref[...]
    for ref, far, far_at, own_at in ((low_ref, A, 0, COLUMN), (high_ref, B, FACE + COLUMN, FACE)):
        out_ref[far : far + FACE] += ref[:FACE]
        for start, at in ((0, far_at), (SIDE_ROWS, own_at)):
            out_ref[QH + at : QH + at + COLUMN] += ref[start + FACE : start + FACE + COLUMN]
            out_ref[QL + at : QL + at + COLUMN] += ref[start + FACE + COLUMN : start + SIDE_ROWS]
    own = slice(SIDE_ROWS, SIDE_ROWS + FACE)
    total = out_ref[:ROWS] + put(face_hot(faces_ref, 0), jnp.concatenate([low_ref[own], high_ref[own]], axis=0))
    out_ref[:ROWS] = total
    write_sums(stats_ref, sums_of(total, live_rows(count_ref), count_ref))


def gather_kernel(
    count_ref, chunks_ref, first_ref, rank_ref, rank_t_ref, digits_ref, weight_ref, stats_ref, gain_ref, shift_ref,
    out_ref, sums_ref, table_ref, to_slot_ref, to_row_ref, part_ref,
):
    norm = scale_of(total_of(stats_ref), gain_ref[...], shift_ref[...])
    live = live_rows(count_ref)

    def act(values):
        return jnp.maximum(affine(values, *norm), 0.0)

    table_ref[:, :CH] = (live * act(first_ref[:ROWS])).astype(jnp.bfloat16)
    table_ref[:HALO, CH:] = act(first_ref[ROWS : ROWS + HALO]).astype(jnp.bfloat16)
    table_ref[HALO:, CH:] = jnp.zeros((ROWS - HALO, CH), jnp.bfloat16)
    out_ref[...] = dot(table_ref[:, :CH], weight_ref[CENTRE]) * live
    clear_padding(part_ref)
    total = SIDES * SLOTS

    def chunk(c, carry):
        slots_of_rows(rank_ref, c * SLOTS, to_slot_ref)
        found = lax.dot_general(
            to_slot_ref[...], digits_ref[...], (((1,), (1,)), ((), ())), preferred_element_type=jnp.float32
        )
        tap = lax.broadcasted_iota(jnp.int32, (total, CH), 0) // SLOTS
        lane = lax.broadcasted_iota(jnp.int32, (total, CH), 1)
        worth = jnp.where(lane == tap, float(SLOTS), jnp.where(lane == tap + 32, 1.0, 0.0))
        source = jnp.sum(found * worth, axis=1, keepdims=True).astype(jnp.int32)
        both = dot(hot(jnp.bitwise_and(source, ROWS - 1), (total, ROWS), 1), table_ref[...])
        upper = jnp.broadcast_to(source, (total, CH)) >= ROWS
        picked = jnp.where(upper, both[:, CH:], both[:, :CH]).astype(jnp.bfloat16)
        multiply_slots(picked, weight_ref, lambda t: t + (t >= CENTRE), part_ref)
        rows_of_slots(rank_t_ref, c * SLOTS, to_row_ref)
        added = dot(to_row_ref[...], part_ref[...])
        out_ref[...] += added[:, :CH] + added[:, CH:]
        return carry

    lax.fori_loop(0, chunks_ref[0, 0], chunk, 0)
    write_sums(sums_ref, sums_of(out_ref[...], live, count_ref))


def live_rows(count_ref):
    return (lax.broadcasted_iota(jnp.int32, (ROWS, 1), 0) < count_ref[0, 0]).astype(jnp.float32)


def sums_of(conv_out, live, count_ref):
    kept = conv_out * live
    first = jnp.sum(kept, axis=0, keepdims=True)
    second = jnp.sum(kept * conv_out, axis=0, keepdims=True)
    count = jnp.full((1, CH), count_ref[0, 0].astype(jnp.float32), jnp.float32)
    return jnp.concatenate([first, second, count], axis=1)


def write_sums(sums_ref, sums):
    for i in range(sums_ref.shape[0]):
        sums_ref[i] = sums


def total_of(stats_ref):
    total = stats_ref[0]
    for i in range(1, stats_ref.shape[0]):
        total = total + stats_ref[i]
    return total


def near_kernel(stats_ref, out_ref):
    write_sums(out_ref, total_of(stats_ref))


def scale_of(sums, gain, shift):
    total = sums[:, 2 * CH :]
    average = sums[:, :CH] / total
    variance = sums[:, CH : 2 * CH] / total - average * average
    scale = lax.rsqrt(variance + EPSILON) * gain
    return average, scale, shift


def affine(values, average, scale, shift):
    return (values - average) * scale + shift


def finish_kernel(count_ref, second_ref, rows_ref, stats_ref, gain_ref, shift_ref, out_ref):
    stats = total_of(stats_ref)
    norm = scale_of(stats, gain_ref[...], shift_ref[...])
    summed = affine(second_ref[...], *norm) + rows_ref[...].astype(jnp.float32)
    out_ref[...] = (live_rows(count_ref) * jnp.maximum(summed, 0.0)).astype(jnp.bfloat16)


def call(kernel, outs, scratch, limit, *args, hbm=False):
    def out_spec(shape):
        return pl.BlockSpec(memory_space=pltpu.SMEM if shape == (1, 1) else pltpu.VMEM)

    def spec(shape):
        return pl.BlockSpec(memory_space=pltpu.HBM) if hbm and shape != (1, 1) else out_spec(shape)

    if hbm:
        args = [a if a.shape == (1, 1) else pltpu.with_memory_space_constraint(a, pltpu.HBM) for a in args]
    return pl.pallas_call(
        kernel,
        out_shape=outs,
        in_specs=[spec(a.shape) for a in args],
        out_specs=jax.tree.map(lambda o: out_spec(o.shape), outs),
        scratch_shapes=scratch,
        compiler_params=pltpu.CompilerParams(vmem_limit_bytes=limit << 20),
    )(*args)


def conv_scratch():
    padded = -(-SIDES * SLOTS // CH) * CH
    return [
        pltpu.VMEM((SIDES * SLOTS, ROWS), jnp.bfloat16),
        pltpu.VMEM((ROWS, padded), jnp.bfloat16),
        pltpu.VMEM((padded, 2 * CH), jnp.bfloat16),
    ]


def slab_neighbours(to_low, to_high):
    count = lax.axis_size(SLAB)
    even = lax.axis_index("slab_2") == 0
    partner = [(i, i ^ 1) for i in range(count)]
    across = [(i, i + 1) for i in range(1, count - 1, 2)] + [(i + 1, i) for i in range(1, count - 1, 2)]
    near = lax.ppermute(jnp.where(even, to_high, to_low), SLAB, partner)
    far = lax.ppermute(jnp.where(even, to_low, to_high), SLAB, across)
    return jnp.where(even, far, near), jnp.where(even, near, far)


def tile_neighbours(to_low, to_high):
    count = lax.axis_size("tile")
    forward = [(i, i + 1) for i in range(count - 1)]
    backward = [(j, i) for i, j in forward]
    return lax.ppermute(to_high, "tile", forward), lax.ppermute(to_low, "tile", backward)


def reduce_all(sums):
    near = lax.all_to_all(sums, ("slab_1", "slab_2"), 0, 0)
    far = lax.axis_size(("slab_0", "tile"))
    block = call(near_kernel, jax.ShapeDtypeStruct((far, 1, 3 * CH), jnp.float32), [], 4, near)
    return lax.all_to_all(block, ("slab_0", "tile"), 0, 0)


def per_device(
    features, counts, rulebook, face_rows, conv_one, gain_one, shift_one, conv_two, gain_two, shift_two
):
    f32, bf16, i32 = jnp.float32, jnp.bfloat16, jnp.int32
    shaped = jax.ShapeDtypeStruct
    ext, message, big = shaped((EXT, CH), f32), shaped((2 * SIDE_ROWS, CH), f32), shaped((ROWS, CH), f32)
    small = shaped((8, 1, 3 * CH), f32)
    params = (conv_two, gain_one[None], shift_one[None], gain_two[None], shift_two[None])
    outs = (
        ext, message, message,
        shaped((32, ROWS), i32), shaped((ROWS, CH), i32), shaped((CH, ROWS), bf16), shaped((1, 1), i32),
        shaped((ROWS, CH), bf16), shaped((4, FACE), i32), *(shaped(p.shape, p.dtype) for p in params),
    )
    scratch = [
        pltpu.VMEM((TAPS, 1, ROWS), i32), pltpu.VMEM((TAPS, CH, CH), bf16), pltpu.VMEM((32, ROWS), i32),
        *conv_scratch(), pltpu.SemaphoreType.DMA((9,)),
    ]
    taps = rulebook.reshape(TAPS, 1, ROWS)
    first, up, down, *plan, chunks, rows, faces, weight_two, gain_one, shift_one, gain_two, shift_two = call(
        spread_kernel, outs, scratch, 24, counts, taps, features[0, 0], conv_one, face_rows[0, 0], *params, hbm=True
    )
    received = tile_neighbours(down, up)
    first, left, right = call(tile_kernel, (ext, message, message), [], 8, first, *received, faces)
    received = slab_neighbours(left, right)
    first, sums = call(slab_kernel, (ext, small), [], 8, counts, first, *received, faces)
    stats = reduce_all(sums)
    second, sums = call(
        gather_kernel, (big, small), [pltpu.VMEM((ROWS, 2 * CH), bf16), *conv_scratch()], 24,
        counts, chunks, first, *plan, weight_two, stats, gain_one, shift_one,
    )
    stats = reduce_all(sums)
    out = call(
        finish_kernel, shaped((ROWS, CH), bf16), [], 4, counts, second, rows, stats, gain_two, shift_two
    )
    return out[None, None]


def solution(mesh):
    tiles = mesh.shape["tile"]
    torus = Mesh(
        mesh.devices.reshape(-1, 4, 2, tiles), ("slab_0", "slab_1", "slab_2", "tile")
    )
    split = P(SLAB, "tile", None, None)
    in_specs = (split, P(SLAB, "tile"), split, split, P(), P(), P(), P(), P(), P())
    return jax.shard_map(
        per_device, mesh=torus, in_specs=in_specs, out_specs=split, check_vma=False
    )
```

```python
import jax
import jax.numpy as jnp
from jax import lax
from jax.experimental import pallas as pl
from jax.experimental.pallas import tpu as pltpu
from jax.sharding import Mesh
from jax.sharding import PartitionSpec as P

ROWS = 512
CH = 128
TAPS = 27
SIDES = 26
CENTRE = 13
SLOTS = 32
TABLE = 800
FACE = 64
COLUMN = 8
SIDE_ROWS = FACE + 2 * COLUMN
HALO = 2 * FACE + 2 * SIDE_ROWS
EXT = 832
SLAB = ("slab_0", "slab_1", "slab_2")
EPSILON = 1e-05


A, B, QH, QL = ROWS, ROWS + FACE, ROWS + 2 * FACE, ROWS + 2 * FACE + SIDE_ROWS


def dot(a, b, **kw):
    return jnp.dot(a, b, preferred_element_type=jnp.float32, **kw)


def hot(index, shape, dim):
    return jnp.where(jnp.broadcast_to(index, shape) == lax.broadcasted_iota(jnp.int32, shape, dim), 1.0, 0.0).astype(
        jnp.bfloat16
    )


def fetch(pairs, sems):
    copies = [pltpu.make_async_copy(src, dst, sems.at[i]) for i, (src, dst) in enumerate(pairs)]
    for copy in copies:
        copy.start()
    return copies


def thirds(values):
    high = values.astype(jnp.bfloat16)
    rest = values - high.astype(jnp.float32)
    mid = rest.astype(jnp.bfloat16)
    return high, mid, (rest - mid.astype(jnp.float32)).astype(jnp.bfloat16)


def face_hot(faces_ref, k):
    return hot(jnp.concatenate([faces_ref[k : k + 1, :], faces_ref[k + 1 : k + 2, :]], axis=1), (ROWS, 2 * FACE), 0)


def pick(selector, rows):
    got = lax.dot_general(
        selector, jnp.concatenate(thirds(rows), axis=1), (((0,), (0,)), ((), ())), preferred_element_type=jnp.float32
    )
    return got[:, :CH] + got[:, CH : 2 * CH] + got[:, 2 * CH :]


def put(selector, values):
    return dot(jnp.concatenate([selector] * 3, axis=1), jnp.concatenate(thirds(values), axis=0))


def plan_pairs(rb_ref, work_ref, rank_ref, rank_t_ref, digits_ref):
    work_ref[...] = jnp.full_like(work_ref, TABLE)
    for t in range(SIDES):
        work_ref[t : t + 1, :] = rb_ref[t + (t >= CENTRE)]
    entry = work_ref[...]
    present = entry != TABLE
    ones = jnp.where(present, 1.0, 0.0)
    before = lax.broadcasted_iota(jnp.int32, (ROWS, ROWS), 0) < lax.broadcasted_iota(jnp.int32, (ROWS, ROWS), 1)
    place = dot(ones.astype(jnp.bfloat16), jnp.where(before, 1.0, 0.0).astype(jnp.bfloat16))
    rank = jnp.where(present, place.astype(jnp.int32), -1)
    rank_ref[...] = rank
    itself = jnp.broadcast_to(jnp.where(rb_ref[CENTRE] != TABLE, 1, -1), (8, ROWS))
    padded = jnp.concatenate([rank, itself, jnp.full((CH - 40, ROWS), -1, jnp.int32)], axis=0)
    rank_t_ref[...] = padded.T
    digits_ref[...] = jnp.concatenate(
        [(entry // SLOTS).astype(jnp.float32), (entry % SLOTS).astype(jnp.float32),
         jnp.zeros((CH - 2 * entry.shape[0], ROWS), jnp.float32)], axis=0
    ).astype(jnp.bfloat16)
    most = jnp.max(jnp.sum(ones, axis=1, keepdims=True))
    return (most.astype(jnp.int32) + (SLOTS - 1)) // SLOTS


def slots_of_rows(rank_ref, base, to_slot_ref):
    slot = lax.broadcasted_iota(jnp.int32, (SLOTS, ROWS), 0) + base
    for t in range(SIDES):
        match = jnp.broadcast_to(rank_ref[t : t + 1, :], (SLOTS, ROWS)) == slot
        to_slot_ref[t * SLOTS : (t + 1) * SLOTS, :] = jnp.where(match, 1.0, 0.0).astype(jnp.bfloat16)


def rows_of_slots(rank_t_ref, base, to_row_ref):
    lanes = lax.broadcasted_iota(jnp.int32, (ROWS, CH), 1)
    wanted = jnp.bitwise_and(lanes, SLOTS - 1) + base
    for i in range(to_row_ref.shape[1] // CH):
        spread = jnp.take_along_axis(
            rank_t_ref[...], lanes // SLOTS + i * (CH // SLOTS), axis=1, mode="promise_in_bounds"
        )
        to_row_ref[:, i * CH : (i + 1) * CH] = jnp.where(spread == wanted, 1.0, 0.0).astype(jnp.bfloat16)


def multiply_slots(picked, weight_ref, tap_of, part_ref):
    for t in range(SIDES):
        at = slice(t * SLOTS, (t + 1) * SLOTS)
        part = dot(picked[at], weight_ref[tap_of(t)])
        high = part.astype(jnp.bfloat16)
        part_ref[at, :CH] = high
        part_ref[at, CH:] = (part - high.astype(jnp.float32)).astype(jnp.bfloat16)


def clear_padding(part_ref):
    part_ref[SIDES * SLOTS :, :] = jnp.zeros((part_ref.shape[0] - SIDES * SLOTS, 2 * CH), jnp.bfloat16)


def spread_kernel(*refs):
    rb_hbm, rows_hbm, weight_hbm, faces_hbm, *params_hbm = refs[:9]
    out_ref, up_ref, down_ref, rank_ref, rank_t_ref, digits_ref, chunks_ref, rows_ref, faces_ref, *params = refs[9:23]
    rb_ref, weight_ref, work_ref, to_slot_ref, to_row_ref, part_ref, sems = refs[23:]
    rb_copy, rows_copy, weight_copy, *others = fetch(
        [(rb_hbm, rb_ref), (rows_hbm, rows_ref), (weight_hbm, weight_ref), (faces_hbm, faces_ref),
         *zip(params_hbm, params, strict=True)], sems,
    )
    rb_copy.wait()
    chunks = plan_pairs(rb_ref, work_ref, rank_ref, rank_t_ref, digits_ref)
    chunks_ref[...] = jnp.full((8, CH), chunks, jnp.int32)
    clear_padding(part_ref)
    rows_copy.wait()
    weight_copy.wait()
    itself = jnp.broadcast_to(rank_t_ref[:, 32:33], (ROWS, CH)) > 0
    out_ref[:ROWS] = jnp.where(itself, dot(rows_ref[...], weight_ref[CENTRE]), 0.0)
    out_ref[ROWS:] = jnp.zeros((EXT - ROWS, CH), jnp.float32)
    slots = part_ref.shape[0]

    def chunk(c, carry):
        slots_of_rows(rank_ref, c * SLOTS, to_slot_ref)
        picked = dot(to_slot_ref[...], rows_ref[...]).astype(jnp.bfloat16)
        multiply_slots(picked, weight_ref, lambda t: TAPS - 1 - (t + (t >= CENTRE)), part_ref)
        rows_of_slots(rank_t_ref, c * SLOTS, to_row_ref)
        found = dot(digits_ref[...], to_row_ref[...])
        digit = lax.broadcasted_iota(jnp.int32, (CH, slots), 0)
        tap = lax.broadcasted_iota(jnp.int32, (CH, slots), 1) // SLOTS
        worth = jnp.where(digit == tap, float(SLOTS), jnp.where(digit == tap + 32, 1.0, 0.0))
        target = jnp.sum(found * worth, axis=0, keepdims=True).astype(jnp.int32)
        added = dot(hot(target, (EXT, slots), 0), part_ref[...])
        out_ref[...] += added[:, :CH] + added[:, CH:]
        return carry

    lax.fori_loop(0, chunks, chunk, 0)
    for copy in others:
        copy.wait()
    picked = pick(face_hot(faces_ref, 2), out_ref[:ROWS])
    for ref, own, at, far in ((down_ref, picked[:FACE], 0, QH), (up_ref, picked[FACE:], FACE - COLUMN, QL)):
        ref[:COLUMN] = out_ref[A + at : A + at + COLUMN]
        ref[COLUMN : COLUMN + FACE] = own
        ref[COLUMN + FACE : SIDE_ROWS] = out_ref[B + at : B + at + COLUMN]
        ref[SIDE_ROWS:] = out_ref[far : far + SIDE_ROWS]


def tile_kernel(sums_ref, low_ref, high_ref, faces_ref, out_ref, left_ref, right_ref):
    out_ref[...] = sums_ref[...]
    first, last = SIDE_ROWS + COLUMN, SIDE_ROWS + COLUMN + FACE
    out_ref[QH:QL] += low_ref[:SIDE_ROWS]
    out_ref[QL : QL + SIDE_ROWS] += high_ref[:SIDE_ROWS]
    for ref, at in ((low_ref, 0), (high_ref, FACE - COLUMN)):
        out_ref[A + at : A + at + COLUMN] += ref[SIDE_ROWS:first]
        out_ref[B + at : B + at + COLUMN] += ref[last:]
    out_ref[:ROWS] += put(face_hot(faces_ref, 2), jnp.concatenate([low_ref[first:last], high_ref[first:last]], axis=0))
    picked = pick(face_hot(faces_ref, 0), out_ref[:ROWS])
    for ref, own, own_at, far, far_at in (
        (left_ref, picked[:FACE], COLUMN, A, 0),
        (right_ref, picked[FACE:], FACE, B, FACE + COLUMN),
    ):
        ref[:FACE] = own
        ref[SIDE_ROWS : SIDE_ROWS + FACE] = out_ref[far : far + FACE]
        for start, at in ((0, own_at), (SIDE_ROWS, far_at)):
            ref[start + FACE : start + FACE + COLUMN] = out_ref[QH + at : QH + at + COLUMN]
            ref[start + FACE + COLUMN : start + SIDE_ROWS] = out_ref[QL + at : QL + at + COLUMN]


def slab_kernel(count_ref, sums_ref, low_ref, high_ref, faces_ref, out_ref, stats_ref):
    out_ref[...] = sums_ref[...]
    for ref, far, far_at, own_at in ((low_ref, A, 0, COLUMN), (high_ref, B, FACE + COLUMN, FACE)):
        out_ref[far : far + FACE] += ref[:FACE]
        for start, at in ((0, far_at), (SIDE_ROWS, own_at)):
            out_ref[QH + at : QH + at + COLUMN] += ref[start + FACE : start + FACE + COLUMN]
            out_ref[QL + at : QL + at + COLUMN] += ref[start + FACE + COLUMN : start + SIDE_ROWS]
    own = slice(SIDE_ROWS, SIDE_ROWS + FACE)
    total = out_ref[:ROWS] + put(face_hot(faces_ref, 0), jnp.concatenate([low_ref[own], high_ref[own]], axis=0))
    out_ref[:ROWS] = total
    write_sums(stats_ref, sums_of(total, count_ref))


def gather_kernel(
    count_ref, chunks_ref, first_ref, rank_ref, rank_t_ref, digits_ref, weight_ref, stats_ref, gain_ref, shift_ref,
    out_ref, sums_ref, table_ref, to_slot_ref, to_row_ref, part_ref,
):
    norm = scale_of(total_of(stats_ref), gain_ref[...], shift_ref[...])
    live = live_rows(count_ref)

    def act(values):
        return jnp.maximum(affine(values, *norm), 0.0)

    table_ref[:, :CH] = (live * act(first_ref[:ROWS])).astype(jnp.bfloat16)
    table_ref[:HALO, CH:] = act(first_ref[ROWS : ROWS + HALO]).astype(jnp.bfloat16)
    table_ref[HALO:, CH:] = jnp.zeros((ROWS - HALO, CH), jnp.bfloat16)
    out_ref[...] = dot(table_ref[:, :CH], weight_ref[CENTRE]) * live
    clear_padding(part_ref)
    total = SIDES * SLOTS

    def chunk(c, carry):
        slots_of_rows(rank_ref, c * SLOTS, to_slot_ref)
        found = lax.dot_general(
            to_slot_ref[...], digits_ref[...], (((1,), (1,)), ((), ())), preferred_element_type=jnp.float32
        )
        tap = lax.broadcasted_iota(jnp.int32, (total, CH), 0) // SLOTS
        lane = lax.broadcasted_iota(jnp.int32, (total, CH), 1)
        worth = jnp.where(lane == tap, float(SLOTS), jnp.where(lane == tap + 32, 1.0, 0.0))
        source = jnp.sum(found * worth, axis=1, keepdims=True).astype(jnp.int32)
        both = dot(hot(jnp.bitwise_and(source, ROWS - 1), (total, ROWS), 1), table_ref[...])
        upper = jnp.broadcast_to(source, (total, CH)) >= ROWS
        picked = jnp.where(upper, both[:, CH:], both[:, :CH]).astype(jnp.bfloat16)
        multiply_slots(picked, weight_ref, lambda t: t + (t >= CENTRE), part_ref)
        rows_of_slots(rank_t_ref, c * SLOTS, to_row_ref)
        added = dot(to_row_ref[...], part_ref[...])
        out_ref[...] += added[:, :CH] + added[:, CH:]
        return carry

    lax.fori_loop(0, jnp.max(chunks_ref[...]), chunk, 0)
    write_sums(sums_ref, sums_of(out_ref[...], count_ref))


def live_rows(count_ref):
    rows = lax.broadcasted_iota(jnp.int32, (ROWS, CH), 0)
    return jnp.where(rows < jnp.broadcast_to(count_ref[0:1], (ROWS, CH)), 1.0, 0.0)


def sums_of(conv_out, count_ref):
    kept = conv_out * live_rows(count_ref)
    first = jnp.sum(kept, axis=0, keepdims=True)
    second = jnp.sum(kept * conv_out, axis=0, keepdims=True)
    return jnp.concatenate([first, second, count_ref[0:1].astype(jnp.float32)], axis=1)


def write_sums(sums_ref, sums):
    for i in range(sums_ref.shape[0]):
        sums_ref[i] = sums


def total_of(stats_ref):
    total = stats_ref[0]
    for i in range(1, stats_ref.shape[0]):
        total = total + stats_ref[i]
    return total


def near_kernel(stats_ref, out_ref):
    write_sums(out_ref, total_of(stats_ref))


def scale_of(sums, gain, shift):
    total = sums[:, 2 * CH :]
    average = sums[:, :CH] / total
    variance = sums[:, CH : 2 * CH] / total - average * average
    scale = lax.rsqrt(variance + EPSILON) * gain
    return average, scale, shift


def affine(values, average, scale, shift):
    return (values - average) * scale + shift


def finish_kernel(count_ref, second_ref, rows_ref, stats_ref, gain_ref, shift_ref, out_ref):
    stats = total_of(stats_ref)
    norm = scale_of(stats, gain_ref[...], shift_ref[...])
    summed = affine(second_ref[...], *norm) + rows_ref[...].astype(jnp.float32)
    out_ref[...] = (live_rows(count_ref) * jnp.maximum(summed, 0.0)).astype(jnp.bfloat16)


def call(kernel, outs, scratch, limit, *args, hbm=False):
    vmem = pl.BlockSpec(memory_space=pltpu.VMEM)
    if hbm:
        args = [pltpu.with_memory_space_constraint(a, pltpu.HBM) for a in args]
    return pl.pallas_call(
        kernel,
        out_shape=outs,
        in_specs=[pl.BlockSpec(memory_space=pltpu.HBM) if hbm else vmem] * len(args),
        out_specs=jax.tree.map(lambda _: vmem, outs),
        scratch_shapes=scratch,
        compiler_params=pltpu.CompilerParams(vmem_limit_bytes=limit << 20),
    )(*args)


def conv_scratch():
    padded = -(-SIDES * SLOTS // CH) * CH
    return [
        pltpu.VMEM((SIDES * SLOTS, ROWS), jnp.bfloat16),
        pltpu.VMEM((ROWS, padded), jnp.bfloat16),
        pltpu.VMEM((padded, 2 * CH), jnp.bfloat16),
    ]


def slab_neighbours(to_low, to_high):
    count = lax.axis_size(SLAB)
    even = lax.axis_index("slab_2") == 0
    across = [(i, i + 1) for i in range(1, count - 1, 2)] + [(i + 1, i) for i in range(1, count - 1, 2)]
    far = lax.ppermute(jnp.where(even, to_low, to_high), SLAB, across)
    both = lax.all_gather(jnp.where(even, to_high, to_low), "slab_2")
    return jnp.where(even, far, both[0]), jnp.where(even, both[1], far)


def tile_neighbours(to_low, to_high):
    count = lax.axis_size("tile")
    forward = [(i, i + 1) for i in range(count - 1)]
    backward = [(j, i) for i, j in forward]
    return lax.ppermute(to_high, "tile", forward), lax.ppermute(to_low, "tile", backward)


def reduce_all(sums):
    near = lax.all_to_all(sums, ("slab_1", "slab_2"), 0, 0)
    far = lax.axis_size(("slab_0", "tile"))
    block = call(near_kernel, jax.ShapeDtypeStruct((far, 1, 3 * CH), jnp.float32), [], 4, near)
    return lax.all_to_all(block, ("slab_0", "tile"), 0, 0)


def per_device(
    features, counts, rulebook, face_rows, conv_one, gain_one, shift_one, conv_two, gain_two, shift_two
):
    f32, bf16, i32 = jnp.float32, jnp.bfloat16, jnp.int32
    shaped = jax.ShapeDtypeStruct
    ext, message, big = shaped((EXT, CH), f32), shaped((2 * SIDE_ROWS, CH), f32), shaped((ROWS, CH), f32)
    small = shaped((8, 1, 3 * CH), f32)
    params = (conv_two, gain_one[None], shift_one[None], gain_two[None], shift_two[None])
    outs = (
        ext, message, message,
        shaped((32, ROWS), i32), shaped((ROWS, CH), i32), shaped((CH, ROWS), bf16), shaped((8, CH), i32),
        shaped((ROWS, CH), bf16), shaped((4, FACE), i32), *(shaped(p.shape, p.dtype) for p in params),
    )
    scratch = [
        pltpu.VMEM((TAPS, 1, ROWS), i32), pltpu.VMEM((TAPS, CH, CH), bf16), pltpu.VMEM((32, ROWS), i32),
        *conv_scratch(), pltpu.SemaphoreType.DMA((9,)),
    ]
    taps = rulebook.reshape(TAPS, 1, ROWS)
    first, up, down, *plan, chunks, rows, faces, weight_two, gain_one, shift_one, gain_two, shift_two = call(
        spread_kernel, outs, scratch, 24, taps, features[0, 0], conv_one, face_rows[0, 0], *params, hbm=True
    )
    count = jnp.broadcast_to(counts, (8, CH))
    received = tile_neighbours(down, up)
    first, left, right = call(tile_kernel, (ext, message, message), [], 8, first, *received, faces)
    received = slab_neighbours(left, right)
    first, sums = call(slab_kernel, (ext, small), [], 8, count, first, *received, faces)
    stats = reduce_all(sums)
    second, sums = call(
        gather_kernel, (big, small), [pltpu.VMEM((ROWS, 2 * CH), bf16), *conv_scratch()], 24,
        count, chunks, first, *plan, weight_two, stats, gain_one, shift_one,
    )
    stats = reduce_all(sums)
    out = call(
        finish_kernel, shaped((ROWS, CH), bf16), [], 4, count, second, rows, stats, gain_two, shift_two
    )
    return out[None, None]


def solution(mesh):
    tiles = mesh.shape["tile"]
    torus = Mesh(
        mesh.devices.reshape(-1, 4, 2, tiles), ("slab_0", "slab_1", "slab_2", "tile")
    )
    split = P(SLAB, "tile", None, None)
    in_specs = (split, P(SLAB, "tile"), split, split, P(), P(), P(), P(), P(), P())
    return jax.shard_map(
        per_device, mesh=torus, in_specs=in_specs, out_specs=split, check_vma=False
    )
```

```python
import jax
import jax.numpy as jnp
from jax import lax
from jax.experimental import pallas as pl
from jax.experimental.pallas import tpu as pltpu
from jax.sharding import Mesh
from jax.sharding import PartitionSpec as P

ROWS = 512
CH = 128
TAPS = 27
SIDES = 26
CENTRE = 13
SLOTS = 24
DIGIT = 32
TABLE = 800
FACE = 64
COLUMN = 8
SIDE_ROWS = FACE + 2 * COLUMN
HALO = 2 * FACE + 2 * SIDE_ROWS
EXT = 832
SLAB = ("slab_0", "slab_1", "slab_2")
EPSILON = 1e-05


A, B, QH, QL = ROWS, ROWS + FACE, ROWS + 2 * FACE, ROWS + 2 * FACE + SIDE_ROWS


def dot(a, b, **kw):
    return jnp.dot(a, b, preferred_element_type=jnp.float32, **kw)


def hot(index, shape, dim):
    return jnp.where(jnp.broadcast_to(index, shape) == lax.broadcasted_iota(jnp.int32, shape, dim), 1.0, 0.0).astype(
        jnp.bfloat16
    )


def fetch(pairs, sems):
    copies = [pltpu.make_async_copy(src, dst, sems.at[i]) for i, (src, dst) in enumerate(pairs)]
    for copy in copies:
        copy.start()
    return copies


def thirds(values):
    high = values.astype(jnp.bfloat16)
    rest = values - high.astype(jnp.float32)
    mid = rest.astype(jnp.bfloat16)
    return high, mid, (rest - mid.astype(jnp.float32)).astype(jnp.bfloat16)


def face_hot(faces_ref, k):
    return hot(jnp.concatenate([faces_ref[k : k + 1, :], faces_ref[k + 1 : k + 2, :]], axis=1), (ROWS, 2 * FACE), 0)


def pick(selector, rows):
    got = lax.dot_general(
        selector, jnp.concatenate(thirds(rows), axis=1), (((0,), (0,)), ((), ())), preferred_element_type=jnp.float32
    )
    return got[:, :CH] + got[:, CH : 2 * CH] + got[:, 2 * CH :]


def put(selector, values):
    return dot(jnp.concatenate([selector] * 3, axis=1), jnp.concatenate(thirds(values), axis=0))


def plan_pairs(rb_ref, work_ref, rank_ref, rank_t_ref, digits_ref):
    work_ref[...] = jnp.full_like(work_ref, TABLE)
    for t in range(SIDES):
        work_ref[t : t + 1, :] = rb_ref[t + (t >= CENTRE)]
    entry = work_ref[...]
    present = entry != TABLE
    ones = jnp.where(present, 1.0, 0.0)
    before = lax.broadcasted_iota(jnp.int32, (ROWS, ROWS), 0) < lax.broadcasted_iota(jnp.int32, (ROWS, ROWS), 1)
    place = dot(ones.astype(jnp.bfloat16), jnp.where(before, 1.0, 0.0).astype(jnp.bfloat16))
    rank = jnp.where(present, place.astype(jnp.int32), -1)
    rank_ref[...] = rank
    itself = jnp.broadcast_to(jnp.where(rb_ref[CENTRE] != TABLE, 1, -1), (8, ROWS))
    padded = jnp.concatenate([rank, itself, jnp.full((CH - 40, ROWS), -1, jnp.int32)], axis=0)
    rank_t_ref[...] = padded.T
    digits_ref[...] = jnp.concatenate(
        [(entry // DIGIT).astype(jnp.float32), (entry % DIGIT).astype(jnp.float32),
         jnp.zeros((CH - 2 * entry.shape[0], ROWS), jnp.float32)], axis=0
    ).astype(jnp.bfloat16)
    most = jnp.max(jnp.sum(ones, axis=1, keepdims=True))
    return (most.astype(jnp.int32) + (SLOTS - 1)) // SLOTS


def slots_of_rows(rank_ref, base, to_slot_ref):
    slot = lax.broadcasted_iota(jnp.int32, (SLOTS, ROWS), 0) + base
    blocks = []
    for t in range(SIDES):
        match = jnp.broadcast_to(rank_ref[t : t + 1, :], (SLOTS, ROWS)) == slot
        blocks.append(jnp.where(match, 1.0, 0.0))
    to_slot_ref[...] = jnp.concatenate(blocks, axis=0).astype(jnp.bfloat16)


def tap_of_slot(slot):
    return jnp.right_shift(slot * 2731, 16)


def rows_of_slots(rank_t_ref, base, to_row_ref):
    for i in range(to_row_ref.shape[1] // CH):
        slot = lax.broadcasted_iota(jnp.int32, (1, CH), 1) + i * CH
        tap = tap_of_slot(slot)
        wanted = jnp.broadcast_to(slot - tap * SLOTS + base, (ROWS, CH))
        spread = jnp.take_along_axis(
            rank_t_ref[...], jnp.broadcast_to(tap, (ROWS, CH)), axis=1, mode="promise_in_bounds"
        )
        to_row_ref[:, i * CH : (i + 1) * CH] = jnp.where(spread == wanted, 1.0, 0.0).astype(jnp.bfloat16)


def multiply_slots(picked, weight_ref, tap_of, part_ref):
    parts = [
        dot(picked[t * SLOTS : (t + 1) * SLOTS].astype(jnp.bfloat16), weight_ref[tap_of(t)]) for t in range(SIDES)
    ]
    part = jnp.concatenate(parts, axis=0)
    high = part.astype(jnp.bfloat16)
    part_ref[: SIDES * SLOTS, :CH] = high
    part_ref[: SIDES * SLOTS, CH:] = (part - high.astype(jnp.float32)).astype(jnp.bfloat16)


def clear_padding(part_ref):
    part_ref[SIDES * SLOTS :, :] = jnp.zeros((part_ref.shape[0] - SIDES * SLOTS, 2 * CH), jnp.bfloat16)


def spread_kernel(*refs):
    rb_hbm, rows_hbm, weight_hbm, faces_hbm, *params_hbm = refs[:9]
    out_ref, up_ref, down_ref, rank_ref, rank_t_ref, digits_ref, meta_ref, rows_ref, faces_ref, *params = refs[9:23]
    rb_ref, weight_ref, work_ref, to_slot_ref, to_row_ref, part_ref, sems = refs[23:]
    rb_copy, rows_copy, weight_copy, *others = fetch(
        [(rb_hbm, rb_ref), (rows_hbm, rows_ref), (weight_hbm, weight_ref), (faces_hbm, faces_ref),
         *zip(params_hbm, params, strict=True)], sems,
    )
    rb_copy.wait()
    chunks = plan_pairs(rb_ref, work_ref, rank_ref, rank_t_ref, digits_ref)
    present = jnp.where(rb_ref[CENTRE] != TABLE, 1.0, 0.0)
    meta_ref[0:1] = jnp.broadcast_to(jnp.sum(present, axis=1, keepdims=True), (1, CH)).astype(jnp.int32)
    meta_ref[1:2] = jnp.full((1, CH), chunks, jnp.int32)
    clear_padding(part_ref)
    rows_copy.wait()
    weight_copy.wait()
    itself = jnp.broadcast_to(rank_t_ref[:, 32:33], (ROWS, CH)) > 0
    out_ref[:ROWS] = jnp.where(itself, dot(rows_ref[...], weight_ref[CENTRE]), 0.0)
    out_ref[ROWS:] = jnp.zeros((EXT - ROWS, CH), jnp.float32)
    slots = part_ref.shape[0]

    def chunk(c, carry):
        slots_of_rows(rank_ref, c * SLOTS, to_slot_ref)
        picked = dot(to_slot_ref[...], rows_ref[...])
        multiply_slots(picked, weight_ref, lambda t: TAPS - 1 - (t + (t >= CENTRE)), part_ref)
        rows_of_slots(rank_t_ref, c * SLOTS, to_row_ref)
        found = dot(digits_ref[...], to_row_ref[...])
        digit = lax.broadcasted_iota(jnp.int32, (CH, slots), 0)
        tap = jnp.broadcast_to(tap_of_slot(lax.broadcasted_iota(jnp.int32, (1, slots), 1)), (CH, slots))
        worth = jnp.where(digit == tap, float(DIGIT), jnp.where(digit == tap + 32, 1.0, 0.0))
        target = jnp.sum(found * worth, axis=0, keepdims=True).astype(jnp.int32)
        added = dot(hot(target, (EXT, slots), 0), part_ref[...])
        out_ref[...] += added[:, :CH] + added[:, CH:]
        return carry

    lax.fori_loop(0, chunks, chunk, 0)
    for copy in others:
        copy.wait()
    picked = pick(face_hot(faces_ref, 2), out_ref[:ROWS])
    for ref, own, at, far in ((down_ref, picked[:FACE], 0, QH), (up_ref, picked[FACE:], FACE - COLUMN, QL)):
        ref[:COLUMN] = out_ref[A + at : A + at + COLUMN]
        ref[COLUMN : COLUMN + FACE] = own
        ref[COLUMN + FACE : SIDE_ROWS] = out_ref[B + at : B + at + COLUMN]
        ref[SIDE_ROWS:] = out_ref[far : far + SIDE_ROWS]


def tile_kernel(sums_ref, low_ref, high_ref, faces_ref, out_ref, left_ref, right_ref):
    out_ref[...] = sums_ref[...]
    first, last = SIDE_ROWS + COLUMN, SIDE_ROWS + COLUMN + FACE
    out_ref[QH:QL] += low_ref[:SIDE_ROWS]
    out_ref[QL : QL + SIDE_ROWS] += high_ref[:SIDE_ROWS]
    for ref, at in ((low_ref, 0), (high_ref, FACE - COLUMN)):
        out_ref[A + at : A + at + COLUMN] += ref[SIDE_ROWS:first]
        out_ref[B + at : B + at + COLUMN] += ref[last:]
    out_ref[:ROWS] += put(face_hot(faces_ref, 2), jnp.concatenate([low_ref[first:last], high_ref[first:last]], axis=0))
    picked = pick(face_hot(faces_ref, 0), out_ref[:ROWS])
    for ref, own, own_at, far, far_at in (
        (left_ref, picked[:FACE], COLUMN, A, 0),
        (right_ref, picked[FACE:], FACE, B, FACE + COLUMN),
    ):
        ref[:FACE] = own
        ref[SIDE_ROWS : SIDE_ROWS + FACE] = out_ref[far : far + FACE]
        for start, at in ((0, own_at), (SIDE_ROWS, far_at)):
            ref[start + FACE : start + FACE + COLUMN] = out_ref[QH + at : QH + at + COLUMN]
            ref[start + FACE + COLUMN : start + SIDE_ROWS] = out_ref[QL + at : QL + at + COLUMN]


def slab_kernel(meta_ref, sums_ref, low_ref, high_ref, faces_ref, out_ref, stats_ref):
    out_ref[...] = sums_ref[...]
    for ref, far, far_at, own_at in ((low_ref, A, 0, COLUMN), (high_ref, B, FACE + COLUMN, FACE)):
        out_ref[far : far + FACE] += ref[:FACE]
        for start, at in ((0, far_at), (SIDE_ROWS, own_at)):
            out_ref[QH + at : QH + at + COLUMN] += ref[start + FACE : start + FACE + COLUMN]
            out_ref[QL + at : QL + at + COLUMN] += ref[start + FACE + COLUMN : start + SIDE_ROWS]
    own = slice(SIDE_ROWS, SIDE_ROWS + FACE)
    total = out_ref[:ROWS] + put(face_hot(faces_ref, 0), jnp.concatenate([low_ref[own], high_ref[own]], axis=0))
    out_ref[:ROWS] = total
    write_sums(stats_ref, sums_of(total, meta_ref))


def gather_kernel(
    meta_ref, first_ref, rank_ref, rank_t_ref, digits_ref, weight_ref, stats_ref, gain_ref, shift_ref,
    out_ref, sums_ref, table_ref, to_slot_ref, to_row_ref, part_ref,
):
    norm = scale_of(total_of(stats_ref), gain_ref[...], shift_ref[...])
    live = live_rows(meta_ref)

    def act(values):
        return jnp.maximum(affine(values, *norm), 0.0)

    table_ref[:, :CH] = (live * act(first_ref[:ROWS])).astype(jnp.bfloat16)
    table_ref[:HALO, CH:] = act(first_ref[ROWS : ROWS + HALO]).astype(jnp.bfloat16)
    table_ref[HALO:, CH:] = jnp.zeros((ROWS - HALO, CH), jnp.bfloat16)
    out_ref[...] = dot(table_ref[:, :CH], weight_ref[CENTRE]) * live
    clear_padding(part_ref)
    total = SIDES * SLOTS

    def chunk(c, carry):
        slots_of_rows(rank_ref, c * SLOTS, to_slot_ref)
        found = lax.dot_general(
            to_slot_ref[...], digits_ref[...], (((1,), (1,)), ((), ())), preferred_element_type=jnp.float32
        )
        tap = tap_of_slot(lax.broadcasted_iota(jnp.int32, (total, CH), 0))
        lane = lax.broadcasted_iota(jnp.int32, (total, CH), 1)
        worth = jnp.where(lane == tap, float(DIGIT), jnp.where(lane == tap + 32, 1.0, 0.0))
        source = jnp.sum(found * worth, axis=1, keepdims=True).astype(jnp.int32)
        both = dot(hot(jnp.bitwise_and(source, ROWS - 1), (total, ROWS), 1), table_ref[...])
        upper = jnp.broadcast_to(source, (total, CH)) >= ROWS
        picked = jnp.where(upper, both[:, CH:], both[:, :CH])
        multiply_slots(picked, weight_ref, lambda t: t + (t >= CENTRE), part_ref)
        rows_of_slots(rank_t_ref, c * SLOTS, to_row_ref)
        added = dot(to_row_ref[...], part_ref[...])
        out_ref[...] += added[:, :CH] + added[:, CH:]
        return carry

    lax.fori_loop(0, jnp.max(meta_ref[1:2]), chunk, 0)
    write_sums(sums_ref, sums_of(out_ref[...], meta_ref))


def live_rows(meta_ref):
    rows = lax.broadcasted_iota(jnp.int32, (ROWS, CH), 0)
    return jnp.where(rows < jnp.broadcast_to(meta_ref[0:1], (ROWS, CH)), 1.0, 0.0)


def sums_of(conv_out, meta_ref):
    kept = conv_out * live_rows(meta_ref)
    first = jnp.sum(kept, axis=0, keepdims=True)
    second = jnp.sum(kept * conv_out, axis=0, keepdims=True)
    return jnp.concatenate([first, second, meta_ref[0:1].astype(jnp.float32)], axis=1)


def write_sums(sums_ref, sums):
    for i in range(sums_ref.shape[0]):
        sums_ref[i] = sums


def total_of(stats_ref):
    total = stats_ref[0]
    for i in range(1, stats_ref.shape[0]):
        total = total + stats_ref[i]
    return total


def near_kernel(stats_ref, out_ref):
    write_sums(out_ref, total_of(stats_ref))


def scale_of(sums, gain, shift):
    total = sums[:, 2 * CH :]
    average = sums[:, :CH] / total
    variance = sums[:, CH : 2 * CH] / total - average * average
    scale = lax.rsqrt(variance + EPSILON) * gain
    return average, scale, shift


def affine(values, average, scale, shift):
    return (values - average) * scale + shift


def finish_kernel(meta_ref, second_ref, rows_ref, stats_ref, gain_ref, shift_ref, out_ref):
    stats = total_of(stats_ref)
    norm = scale_of(stats, gain_ref[...], shift_ref[...])
    summed = affine(second_ref[...], *norm) + rows_ref[...].astype(jnp.float32)
    out_ref[...] = (live_rows(meta_ref) * jnp.maximum(summed, 0.0)).astype(jnp.bfloat16)


def call(kernel, outs, scratch, limit, *args, hbm=False):
    vmem = pl.BlockSpec(memory_space=pltpu.VMEM)
    if hbm:
        args = [pltpu.with_memory_space_constraint(a, pltpu.HBM) for a in args]
    return pl.pallas_call(
        kernel,
        out_shape=outs,
        in_specs=[pl.BlockSpec(memory_space=pltpu.HBM) if hbm else vmem] * len(args),
        out_specs=jax.tree.map(lambda _: vmem, outs),
        scratch_shapes=scratch,
        compiler_params=pltpu.CompilerParams(vmem_limit_bytes=limit << 20),
    )(*args)


def conv_scratch():
    padded = -(-SIDES * SLOTS // CH) * CH
    return [
        pltpu.VMEM((SIDES * SLOTS, ROWS), jnp.bfloat16),
        pltpu.VMEM((ROWS, padded), jnp.bfloat16),
        pltpu.VMEM((padded, 2 * CH), jnp.bfloat16),
    ]


def slab_neighbours(to_low, to_high):
    count = lax.axis_size(SLAB)
    even = lax.axis_index("slab_2") == 0
    across = [(i, i + 1) for i in range(1, count - 1, 2)] + [(i + 1, i) for i in range(1, count - 1, 2)]
    far = lax.ppermute(jnp.where(even, to_low, to_high), SLAB, across)
    both = lax.all_gather(jnp.where(even, to_high, to_low), "slab_2")
    return jnp.where(even, far, both[0]), jnp.where(even, both[1], far)


def tile_neighbours(to_low, to_high):
    count = lax.axis_size("tile")
    forward = [(i, i + 1) for i in range(count - 1)]
    backward = [(j, i) for i, j in forward]
    return lax.ppermute(to_high, "tile", forward), lax.ppermute(to_low, "tile", backward)


def reduce_all(sums):
    near = lax.all_to_all(sums, ("slab_1", "slab_2"), 0, 0)
    far = lax.axis_size(("slab_0", "tile"))
    block = call(near_kernel, jax.ShapeDtypeStruct((far, 1, 3 * CH), jnp.float32), [], 4, near)
    return lax.all_to_all(block, ("slab_0", "tile"), 0, 0)


def per_device(
    features, counts, rulebook, face_rows, conv_one, gain_one, shift_one, conv_two, gain_two, shift_two
):
    del counts
    f32, bf16, i32 = jnp.float32, jnp.bfloat16, jnp.int32
    shaped = jax.ShapeDtypeStruct
    ext, message, big = shaped((EXT, CH), f32), shaped((2 * SIDE_ROWS, CH), f32), shaped((ROWS, CH), f32)
    small = shaped((8, 1, 3 * CH), f32)
    params = (conv_two, gain_one[None], shift_one[None], gain_two[None], shift_two[None])
    outs = (
        ext, message, message,
        shaped((32, ROWS), i32), shaped((ROWS, CH), i32), shaped((CH, ROWS), bf16), shaped((8, CH), i32),
        shaped((ROWS, CH), bf16), shaped((4, FACE), i32), *(shaped(p.shape, p.dtype) for p in params),
    )
    scratch = [
        pltpu.VMEM((TAPS, 1, ROWS), i32), pltpu.VMEM((TAPS, CH, CH), bf16), pltpu.VMEM((32, ROWS), i32),
        *conv_scratch(), pltpu.SemaphoreType.DMA((9,)),
    ]
    taps = rulebook.reshape(TAPS, 1, ROWS)
    first, up, down, *plan, meta, rows, faces, weight_two, gain_one, shift_one, gain_two, shift_two = call(
        spread_kernel, outs, scratch, 24, taps, features[0, 0], conv_one, face_rows[0, 0], *params, hbm=True
    )
    received = tile_neighbours(down, up)
    first, left, right = call(tile_kernel, (ext, message, message), [], 8, first, *received, faces)
    received = slab_neighbours(left, right)
    first, sums = call(slab_kernel, (ext, small), [], 8, meta, first, *received, faces)
    stats = reduce_all(sums)
    second, sums = call(
        gather_kernel, (big, small), [pltpu.VMEM((ROWS, 2 * CH), bf16), *conv_scratch()], 24,
        meta, first, *plan, weight_two, stats, gain_one, shift_one,
    )
    stats = reduce_all(sums)
    out = call(
        finish_kernel, shaped((ROWS, CH), bf16), [], 4, meta, second, rows, stats, gain_two, shift_two
    )
    return out[None, None]


def solution(mesh):
    tiles = mesh.shape["tile"]
    torus = Mesh(
        mesh.devices.reshape(-1, 4, 2, tiles), ("slab_0", "slab_1", "slab_2", "tile")
    )
    split = P(SLAB, "tile", None, None)
    in_specs = (split, P(SLAB, "tile"), split, split, P(), P(), P(), P(), P(), P())
    return jax.shard_map(
        per_device, mesh=torus, in_specs=in_specs, out_specs=split, check_vma=False
    )
```

```python
import jax
import jax.numpy as jnp
from jax import lax
from jax.experimental import pallas as pl
from jax.experimental.pallas import tpu as pltpu
from jax.sharding import Mesh
from jax.sharding import PartitionSpec as P

ROWS = 512
CH = 128
TAPS = 27
SIDES = 26
CENTRE = 13
SLOTS = 24
DIGIT = 32
TABLE = 800
FACE = 64
COLUMN = 8
SIDE_ROWS = FACE + 2 * COLUMN
HALO = 2 * FACE + 2 * SIDE_ROWS
EXT = 832
SLAB = ("slab_0", "slab_1", "slab_2")
EPSILON = 1e-05


A, B, QH, QL = ROWS, ROWS + FACE, ROWS + 2 * FACE, ROWS + 2 * FACE + SIDE_ROWS


def dot(a, b, **kw):
    return jnp.dot(a, b, preferred_element_type=jnp.float32, **kw)


def hot(index, shape, dim):
    return jnp.where(jnp.broadcast_to(index, shape) == lax.broadcasted_iota(jnp.int32, shape, dim), 1.0, 0.0).astype(
        jnp.bfloat16
    )


def fetch(pairs, sems):
    copies = [pltpu.make_async_copy(src, dst, sems.at[i]) for i, (src, dst) in enumerate(pairs)]
    for copy in copies:
        copy.start()
    return copies


def thirds(values):
    high = values.astype(jnp.bfloat16)
    rest = values - high.astype(jnp.float32)
    mid = rest.astype(jnp.bfloat16)
    return high, mid, (rest - mid.astype(jnp.float32)).astype(jnp.bfloat16)


def face_hot(faces_ref, k):
    return hot(jnp.concatenate([faces_ref[k : k + 1, :], faces_ref[k + 1 : k + 2, :]], axis=1), (ROWS, 2 * FACE), 0)


def pick(selector, rows):
    got = lax.dot_general(
        selector, jnp.concatenate(thirds(rows), axis=1), (((0,), (0,)), ((), ())), preferred_element_type=jnp.float32
    )
    return got[:, :CH] + got[:, CH : 2 * CH] + got[:, 2 * CH :]


def put(selector, values):
    return dot(jnp.concatenate([selector] * 3, axis=1), jnp.concatenate(thirds(values), axis=0))


def plan_pairs(rb_ref, work_ref, rank_ref, rank_t_ref, digits_ref):
    work_ref[...] = jnp.full_like(work_ref, TABLE)
    for t in range(SIDES):
        work_ref[t : t + 1, :] = rb_ref[t + (t >= CENTRE)]
    entry = work_ref[...]
    present = entry != TABLE
    ones = jnp.where(present, 1.0, 0.0)
    before = lax.broadcasted_iota(jnp.int32, (ROWS, ROWS), 0) < lax.broadcasted_iota(jnp.int32, (ROWS, ROWS), 1)
    place = dot(ones.astype(jnp.bfloat16), jnp.where(before, 1.0, 0.0).astype(jnp.bfloat16))
    rank = jnp.where(present, place.astype(jnp.int32), -1)
    rank_ref[...] = rank
    itself = jnp.broadcast_to(jnp.where(rb_ref[CENTRE] != TABLE, 1, -1), (8, ROWS))
    padded = jnp.concatenate([rank, itself, jnp.full((CH - 40, ROWS), -1, jnp.int32)], axis=0)
    rank_t_ref[...] = padded.T
    digits_ref[...] = jnp.concatenate(
        [(entry // DIGIT).astype(jnp.float32), (entry % DIGIT).astype(jnp.float32),
         jnp.zeros((CH - 2 * entry.shape[0], ROWS), jnp.float32)], axis=0
    ).astype(jnp.bfloat16)
    most = jnp.max(jnp.sum(ones, axis=1, keepdims=True))
    return (most.astype(jnp.int32) + (SLOTS - 1)) // SLOTS


def slots_of_rows(rank_ref, base, to_slot_ref):
    slot = lax.broadcasted_iota(jnp.int32, (SLOTS, ROWS), 0) + base
    blocks = []
    for t in range(SIDES):
        match = jnp.broadcast_to(rank_ref[t : t + 1, :], (SLOTS, ROWS)) == slot
        blocks.append(jnp.where(match, 1.0, 0.0))
    to_slot_ref[...] = jnp.concatenate(blocks, axis=0).astype(jnp.bfloat16)


def tap_of_slot(slot):
    return jnp.right_shift(slot * 2731, 16)


def rows_of_slots(rank_t_ref, base, to_row_ref):
    for i in range(to_row_ref.shape[1] // CH):
        slot = lax.broadcasted_iota(jnp.int32, (1, CH), 1) + i * CH
        tap = tap_of_slot(slot)
        wanted = jnp.broadcast_to(slot - tap * SLOTS + base, (ROWS, CH))
        spread = jnp.take_along_axis(
            rank_t_ref[...], jnp.broadcast_to(tap, (ROWS, CH)), axis=1, mode="promise_in_bounds"
        )
        to_row_ref[:, i * CH : (i + 1) * CH] = jnp.where(spread == wanted, 1.0, 0.0).astype(jnp.bfloat16)


def multiply_slots(picked, weight_ref, tap_of, part_ref):
    parts = [
        dot(picked[t * SLOTS : (t + 1) * SLOTS].astype(jnp.bfloat16), weight_ref[tap_of(t)]) for t in range(SIDES)
    ]
    part = jnp.concatenate(parts, axis=0)
    high = part.astype(jnp.bfloat16)
    part_ref[: SIDES * SLOTS, :CH] = high
    part_ref[: SIDES * SLOTS, CH:] = (part - high.astype(jnp.float32)).astype(jnp.bfloat16)


def clear_padding(part_ref):
    part_ref[SIDES * SLOTS :, :] = jnp.zeros((part_ref.shape[0] - SIDES * SLOTS, 2 * CH), jnp.bfloat16)


def spread_kernel(*refs):
    rb_hbm, rows_hbm, weight_hbm, faces_hbm, *params_hbm = refs[:9]
    out_ref, up_ref, down_ref, rank_ref, rank_t_ref, digits_ref, meta_ref, rows_ref, faces_ref, *params = refs[9:23]
    rb_ref, weight_ref, work_ref, to_slot_ref, to_row_ref, part_ref, sems = refs[23:]
    rb_copy, rows_copy, weight_copy, *others = fetch(
        [(rb_hbm, rb_ref), (rows_hbm, rows_ref), (weight_hbm, weight_ref), (faces_hbm, faces_ref),
         *zip(params_hbm, params, strict=True)], sems,
    )
    rb_copy.wait()
    chunks = plan_pairs(rb_ref, work_ref, rank_ref, rank_t_ref, digits_ref)
    present = jnp.where(rb_ref[CENTRE] != TABLE, 1.0, 0.0)
    meta_ref[0:1] = jnp.broadcast_to(jnp.sum(present, axis=1, keepdims=True), (1, CH)).astype(jnp.int32)
    meta_ref[1:2] = jnp.full((1, CH), chunks, jnp.int32)
    clear_padding(part_ref)
    rows_copy.wait()
    weight_copy.wait()
    itself = jnp.broadcast_to(rank_t_ref[:, 32:33], (ROWS, CH)) > 0
    out_ref[:ROWS] = jnp.where(itself, dot(rows_ref[...], weight_ref[CENTRE]), 0.0)
    out_ref[ROWS:] = jnp.zeros((EXT - ROWS, CH), jnp.float32)
    slots = part_ref.shape[0]

    def chunk(c, carry):
        slots_of_rows(rank_ref, c * SLOTS, to_slot_ref)
        picked = dot(to_slot_ref[...], rows_ref[...])
        multiply_slots(picked, weight_ref, lambda t: TAPS - 1 - (t + (t >= CENTRE)), part_ref)
        rows_of_slots(rank_t_ref, c * SLOTS, to_row_ref)
        found = dot(digits_ref[...], to_row_ref[...])
        digit = lax.broadcasted_iota(jnp.int32, (CH, slots), 0)
        tap = jnp.broadcast_to(tap_of_slot(lax.broadcasted_iota(jnp.int32, (1, slots), 1)), (CH, slots))
        worth = jnp.where(digit == tap, float(DIGIT), jnp.where(digit == tap + 32, 1.0, 0.0))
        target = jnp.sum(found * worth, axis=0, keepdims=True).astype(jnp.int32)
        added = dot(hot(target, (EXT, slots), 0), part_ref[...])
        out_ref[...] += added[:, :CH] + added[:, CH:]
        return carry

    lax.fori_loop(0, chunks, chunk, 0)
    for copy in others:
        copy.wait()
    picked = pick(face_hot(faces_ref, 2), out_ref[:ROWS])
    for ref, own, at, far in ((down_ref, picked[:FACE], 0, QH), (up_ref, picked[FACE:], FACE - COLUMN, QL)):
        ref[:COLUMN] = out_ref[A + at : A + at + COLUMN]
        ref[COLUMN : COLUMN + FACE] = own
        ref[COLUMN + FACE : SIDE_ROWS] = out_ref[B + at : B + at + COLUMN]
        ref[SIDE_ROWS:] = out_ref[far : far + SIDE_ROWS]


def tile_kernel(sums_ref, low_ref, high_ref, faces_ref, out_ref, left_ref, right_ref):
    out_ref[...] = sums_ref[...]
    first, last = SIDE_ROWS + COLUMN, SIDE_ROWS + COLUMN + FACE
    out_ref[QH:QL] += low_ref[:SIDE_ROWS]
    out_ref[QL : QL + SIDE_ROWS] += high_ref[:SIDE_ROWS]
    for ref, at in ((low_ref, 0), (high_ref, FACE - COLUMN)):
        out_ref[A + at : A + at + COLUMN] += ref[SIDE_ROWS:first]
        out_ref[B + at : B + at + COLUMN] += ref[last:]
    out_ref[:ROWS] += put(face_hot(faces_ref, 2), jnp.concatenate([low_ref[first:last], high_ref[first:last]], axis=0))
    picked = pick(face_hot(faces_ref, 0), out_ref[:ROWS])
    for ref, own, own_at, far, far_at in (
        (left_ref, picked[:FACE], COLUMN, A, 0),
        (right_ref, picked[FACE:], FACE, B, FACE + COLUMN),
    ):
        ref[:FACE] = own
        ref[SIDE_ROWS : SIDE_ROWS + FACE] = out_ref[far : far + FACE]
        for start, at in ((0, own_at), (SIDE_ROWS, far_at)):
            ref[start + FACE : start + FACE + COLUMN] = out_ref[QH + at : QH + at + COLUMN]
            ref[start + FACE + COLUMN : start + SIDE_ROWS] = out_ref[QL + at : QL + at + COLUMN]


def slab_kernel(meta_ref, sums_ref, low_ref, high_ref, faces_ref, out_ref, stats_ref):
    out_ref[...] = sums_ref[...]
    for ref, far, far_at, own_at in ((low_ref, A, 0, COLUMN), (high_ref, B, FACE + COLUMN, FACE)):
        out_ref[far : far + FACE] += ref[:FACE]
        for start, at in ((0, far_at), (SIDE_ROWS, own_at)):
            out_ref[QH + at : QH + at + COLUMN] += ref[start + FACE : start + FACE + COLUMN]
            out_ref[QL + at : QL + at + COLUMN] += ref[start + FACE + COLUMN : start + SIDE_ROWS]
    own = slice(SIDE_ROWS, SIDE_ROWS + FACE)
    total = out_ref[:ROWS] + put(face_hot(faces_ref, 0), jnp.concatenate([low_ref[own], high_ref[own]], axis=0))
    out_ref[:ROWS] = total
    write_sums(stats_ref, sums_of(total, meta_ref))


def sources(c, rank_ref, digits_ref, to_slot_ref):
    total = SIDES * SLOTS
    slots_of_rows(rank_ref, c * SLOTS, to_slot_ref)
    found = lax.dot_general(
        to_slot_ref[...], digits_ref[...], (((1,), (1,)), ((), ())), preferred_element_type=jnp.float32
    )
    tap = tap_of_slot(lax.broadcasted_iota(jnp.int32, (total, CH), 0))
    lane = lax.broadcasted_iota(jnp.int32, (total, CH), 1)
    worth = jnp.where(lane == tap, float(DIGIT), jnp.where(lane == tap + 32, 1.0, 0.0))
    source = jnp.sum(found * worth, axis=1, keepdims=True).astype(jnp.int32)
    return hot(jnp.bitwise_and(source, ROWS - 1), (total, ROWS), 1), jnp.broadcast_to(source, (total, CH))


def source_kernel(rank_ref, digits_ref, hot_ref, source_ref, to_slot_ref):
    hot_ref[...], source_ref[...] = sources(0, rank_ref, digits_ref, to_slot_ref)


def gather_kernel(
    meta_ref, first_ref, rank_ref, rank_t_ref, digits_ref, hot_ref, source_ref, weight_ref, stats_ref, gain_ref, shift_ref,
    out_ref, sums_ref, table_ref, to_slot_ref, to_row_ref, part_ref,
):
    norm = scale_of(total_of(stats_ref), gain_ref[...], shift_ref[...])
    live = live_rows(meta_ref)

    def act(values):
        return jnp.maximum(affine(values, *norm), 0.0)

    table_ref[:, :CH] = (live * act(first_ref[:ROWS])).astype(jnp.bfloat16)
    table_ref[:HALO, CH:] = act(first_ref[ROWS : ROWS + HALO]).astype(jnp.bfloat16)
    table_ref[HALO:, CH:] = jnp.zeros((ROWS - HALO, CH), jnp.bfloat16)
    out_ref[...] = dot(table_ref[:, :CH], weight_ref[CENTRE]) * live
    clear_padding(part_ref)

    def add(c, selector, source):
        both = dot(selector, table_ref[...])
        picked = jnp.where(source >= ROWS, both[:, CH:], both[:, :CH])
        multiply_slots(picked, weight_ref, lambda t: t + (t >= CENTRE), part_ref)
        rows_of_slots(rank_t_ref, c * SLOTS, to_row_ref)
        added = dot(to_row_ref[...], part_ref[...])
        out_ref[...] += added[:, :CH] + added[:, CH:]

    def chunk(c, carry):
        add(c, *sources(c, rank_ref, digits_ref, to_slot_ref))
        return carry

    add(0, hot_ref[...], source_ref[...])
    lax.fori_loop(1, jnp.max(meta_ref[1:2]), chunk, 0)
    write_sums(sums_ref, sums_of(out_ref[...], meta_ref))


def live_rows(meta_ref):
    rows = lax.broadcasted_iota(jnp.int32, (ROWS, CH), 0)
    return jnp.where(rows < jnp.broadcast_to(meta_ref[0:1], (ROWS, CH)), 1.0, 0.0)


def sums_of(conv_out, meta_ref):
    kept = conv_out * live_rows(meta_ref)
    first = jnp.sum(kept, axis=0, keepdims=True)
    second = jnp.sum(kept * conv_out, axis=0, keepdims=True)
    return jnp.concatenate([first, second, meta_ref[0:1].astype(jnp.float32)], axis=1)


def write_sums(sums_ref, sums):
    for i in range(sums_ref.shape[0]):
        sums_ref[i] = sums


def total_of(stats_ref):
    total = stats_ref[0]
    for i in range(1, stats_ref.shape[0]):
        total = total + stats_ref[i]
    return total


def near_kernel(stats_ref, out_ref):
    write_sums(out_ref, total_of(stats_ref))


def scale_of(sums, gain, shift):
    total = sums[:, 2 * CH :]
    average = sums[:, :CH] / total
    variance = sums[:, CH : 2 * CH] / total - average * average
    scale = lax.rsqrt(variance + EPSILON) * gain
    return average, scale, shift


def affine(values, average, scale, shift):
    return (values - average) * scale + shift


def finish_kernel(meta_ref, second_ref, rows_ref, stats_ref, gain_ref, shift_ref, out_ref):
    stats = total_of(stats_ref)
    norm = scale_of(stats, gain_ref[...], shift_ref[...])
    summed = affine(second_ref[...], *norm) + rows_ref[...].astype(jnp.float32)
    out_ref[...] = (live_rows(meta_ref) * jnp.maximum(summed, 0.0)).astype(jnp.bfloat16)


def call(kernel, outs, scratch, limit, *args, hbm=False):
    vmem = pl.BlockSpec(memory_space=pltpu.VMEM)
    if hbm:
        args = [pltpu.with_memory_space_constraint(a, pltpu.HBM) for a in args]
    return pl.pallas_call(
        kernel,
        out_shape=outs,
        in_specs=[pl.BlockSpec(memory_space=pltpu.HBM) if hbm else vmem] * len(args),
        out_specs=jax.tree.map(lambda _: vmem, outs),
        scratch_shapes=scratch,
        compiler_params=pltpu.CompilerParams(vmem_limit_bytes=limit << 20),
    )(*args)


def conv_scratch():
    padded = -(-SIDES * SLOTS // CH) * CH
    return [
        pltpu.VMEM((SIDES * SLOTS, ROWS), jnp.bfloat16),
        pltpu.VMEM((ROWS, padded), jnp.bfloat16),
        pltpu.VMEM((padded, 2 * CH), jnp.bfloat16),
    ]


def slab_neighbours(to_low, to_high):
    count = lax.axis_size(SLAB)
    even = lax.axis_index("slab_2") == 0
    across = [(i, i + 1) for i in range(1, count - 1, 2)] + [(i + 1, i) for i in range(1, count - 1, 2)]
    far = lax.ppermute(jnp.where(even, to_low, to_high), SLAB, across)
    both = lax.all_gather(jnp.where(even, to_high, to_low), "slab_2")
    return jnp.where(even, far, both[0]), jnp.where(even, both[1], far)


def tile_neighbours(to_low, to_high):
    count = lax.axis_size("tile")
    forward = [(i, i + 1) for i in range(count - 1)]
    backward = [(j, i) for i, j in forward]
    low = lax.ppermute(to_high, "tile", forward)
    high = lax.ppermute(to_low, "tile", backward)
    return low, high


def reduce_all(sums):
    near = lax.all_to_all(sums, ("slab_1", "slab_2"), 0, 0)
    far = lax.axis_size(("slab_0", "tile"))
    block = call(near_kernel, jax.ShapeDtypeStruct((far, 1, 3 * CH), jnp.float32), [], 4, near)
    return lax.all_to_all(block, ("slab_0", "tile"), 0, 0)


def per_device(
    features, counts, rulebook, face_rows, conv_one, gain_one, shift_one, conv_two, gain_two, shift_two
):
    del counts
    f32, bf16, i32 = jnp.float32, jnp.bfloat16, jnp.int32
    shaped = jax.ShapeDtypeStruct
    ext, message, big = shaped((EXT, CH), f32), shaped((2 * SIDE_ROWS, CH), f32), shaped((ROWS, CH), f32)
    small = shaped((8, 1, 3 * CH), f32)
    params = (conv_two, gain_one[None], shift_one[None], gain_two[None], shift_two[None])
    outs = (
        ext, message, message,
        shaped((32, ROWS), i32), shaped((ROWS, CH), i32), shaped((CH, ROWS), bf16), shaped((8, CH), i32),
        shaped((ROWS, CH), bf16), shaped((4, FACE), i32), *(shaped(p.shape, p.dtype) for p in params),
    )
    scratch = [
        pltpu.VMEM((TAPS, 1, ROWS), i32), pltpu.VMEM((TAPS, CH, CH), bf16), pltpu.VMEM((32, ROWS), i32),
        *conv_scratch(), pltpu.SemaphoreType.DMA((9,)),
    ]
    taps = rulebook.reshape(TAPS, 1, ROWS)
    first, up, down, *plan, meta, rows, faces, weight_two, gain_one, shift_one, gain_two, shift_two = call(
        spread_kernel, outs, scratch, 24, taps, features[0, 0], conv_one, face_rows[0, 0], *params, hbm=True
    )
    total = SIDES * SLOTS
    outs = (shaped((total, ROWS), bf16), shaped((total, CH), i32))
    received = tile_neighbours(down, up)
    source = call(source_kernel, outs, conv_scratch()[:1], 8, plan[0], plan[2])
    first, left, right = call(tile_kernel, (ext, message, message), [], 8, first, *received, faces)
    received = slab_neighbours(left, right)
    first, sums = call(slab_kernel, (ext, small), [], 8, meta, first, *received, faces)
    stats = reduce_all(sums)
    second, sums = call(
        gather_kernel, (big, small), [pltpu.VMEM((ROWS, 2 * CH), bf16), *conv_scratch()], 24,
        meta, first, *plan, *source, weight_two, stats, gain_one, shift_one,
    )
    stats = reduce_all(sums)
    out = call(
        finish_kernel, shaped((ROWS, CH), bf16), [], 4, meta, second, rows, stats, gain_two, shift_two
    )
    return out[None, None]


def solution(mesh):
    tiles = mesh.shape["tile"]
    torus = Mesh(
        mesh.devices.reshape(-1, 4, 2, tiles), ("slab_0", "slab_1", "slab_2", "tile")
    )
    split = P(SLAB, "tile", None, None)
    in_specs = (split, P(SLAB, "tile"), split, split, P(), P(), P(), P(), P(), P())
    return jax.shard_map(
        per_device, mesh=torus, in_specs=in_specs, out_specs=split, check_vma=False
    )
```

```python
import jax
import jax.numpy as jnp
from jax import lax
from jax.experimental import pallas as pl
from jax.experimental.pallas import tpu as pltpu
from jax.sharding import Mesh
from jax.sharding import PartitionSpec as P

ROWS = 512
CH = 128
TAPS = 27
SIDES = 26
CENTRE = 13
SLOTS = 24
DIGIT = 32
TABLE = 800
FACE = 64
COLUMN = 8
SIDE_ROWS = FACE + 2 * COLUMN
HALO = 2 * FACE + 2 * SIDE_ROWS
EXT = 832
SLAB = ("slab_0", "slab_1", "slab_2")
EPSILON = 1e-05


A, B, QH, QL = ROWS, ROWS + FACE, ROWS + 2 * FACE, ROWS + 2 * FACE + SIDE_ROWS


def dot(a, b, **kw):
    return jnp.dot(a, b, preferred_element_type=jnp.float32, **kw)


def hot(index, shape, dim):
    return jnp.where(jnp.broadcast_to(index, shape) == lax.broadcasted_iota(jnp.int32, shape, dim), 1.0, 0.0).astype(
        jnp.bfloat16
    )


def fetch(pairs, sems):
    copies = [pltpu.make_async_copy(src, dst, sems.at[i]) for i, (src, dst) in enumerate(pairs)]
    for copy in copies:
        copy.start()
    return copies


def thirds(values):
    high = values.astype(jnp.bfloat16)
    rest = values - high.astype(jnp.float32)
    mid = rest.astype(jnp.bfloat16)
    return high, mid, (rest - mid.astype(jnp.float32)).astype(jnp.bfloat16)


def face_hot(faces_ref, k):
    return hot(jnp.concatenate([faces_ref[k : k + 1, :], faces_ref[k + 1 : k + 2, :]], axis=1), (ROWS, 2 * FACE), 0)


def pick(selector, rows):
    got = lax.dot_general(
        selector, jnp.concatenate(thirds(rows), axis=1), (((0,), (0,)), ((), ())), preferred_element_type=jnp.float32
    )
    return got[:, :CH] + got[:, CH : 2 * CH] + got[:, 2 * CH :]


def put(selector, values):
    return dot(selector, jnp.concatenate(values, axis=0).astype(jnp.bfloat16))


def plan_pairs(rb_ref, work_ref, rank_ref, rank_t_ref, digits_ref):
    work_ref[...] = jnp.full_like(work_ref, TABLE)
    for t in range(SIDES):
        work_ref[t : t + 1, :] = rb_ref[t + (t >= CENTRE)]
    entry = work_ref[...]
    present = entry != TABLE
    ones = jnp.where(present, 1.0, 0.0)
    before = lax.broadcasted_iota(jnp.int32, (ROWS, ROWS), 0) < lax.broadcasted_iota(jnp.int32, (ROWS, ROWS), 1)
    place = dot(ones.astype(jnp.bfloat16), jnp.where(before, 1.0, 0.0).astype(jnp.bfloat16))
    rank = jnp.where(present, place.astype(jnp.int32), -1)
    rank_ref[...] = rank
    itself = jnp.broadcast_to(jnp.where(rb_ref[CENTRE] != TABLE, 1, -1), (8, ROWS))
    padded = jnp.concatenate([rank, itself, jnp.full((CH - 40, ROWS), -1, jnp.int32)], axis=0)
    rank_t_ref[...] = padded.T
    digits_ref[...] = jnp.concatenate(
        [(entry // DIGIT).astype(jnp.float32), (entry % DIGIT).astype(jnp.float32),
         jnp.zeros((CH - 2 * entry.shape[0], ROWS), jnp.float32)], axis=0
    ).astype(jnp.bfloat16)
    most = jnp.max(jnp.sum(ones, axis=1, keepdims=True))
    return (most.astype(jnp.int32) + (SLOTS - 1)) // SLOTS


def slots_of_rows(rank_ref, base, to_slot_ref):
    slot = lax.broadcasted_iota(jnp.int32, (SLOTS, ROWS), 0) + base
    blocks = []
    for t in range(SIDES):
        match = jnp.broadcast_to(rank_ref[t : t + 1, :], (SLOTS, ROWS)) == slot
        blocks.append(jnp.where(match, 1.0, 0.0))
    to_slot_ref[...] = jnp.concatenate(blocks, axis=0).astype(jnp.bfloat16)


def tap_of_slot(slot):
    return jnp.right_shift(slot * 2731, 16)


def rows_of_slots(rank_t_ref, base, to_row_ref):
    for i in range(to_row_ref.shape[1] // CH):
        slot = lax.broadcasted_iota(jnp.int32, (1, CH), 1) + i * CH
        tap = tap_of_slot(slot)
        wanted = jnp.broadcast_to(slot - tap * SLOTS + base, (ROWS, CH))
        spread = jnp.take_along_axis(
            rank_t_ref[...], jnp.broadcast_to(tap, (ROWS, CH)), axis=1, mode="promise_in_bounds"
        )
        to_row_ref[:, i * CH : (i + 1) * CH] = jnp.where(spread == wanted, 1.0, 0.0).astype(jnp.bfloat16)


def multiply_slots(picked, weight_ref, tap_of, part_ref):
    parts = [
        dot(picked[t * SLOTS : (t + 1) * SLOTS].astype(jnp.bfloat16), weight_ref[tap_of(t)]) for t in range(SIDES)
    ]
    part = jnp.concatenate(parts, axis=0)
    high = part.astype(jnp.bfloat16)
    part_ref[: SIDES * SLOTS, :CH] = high
    part_ref[: SIDES * SLOTS, CH:] = (part - high.astype(jnp.float32)).astype(jnp.bfloat16)


def clear_padding(part_ref):
    part_ref[SIDES * SLOTS :, :] = jnp.zeros((part_ref.shape[0] - SIDES * SLOTS, 2 * CH), jnp.bfloat16)


def spread_kernel(*refs):
    rb_hbm, rows_hbm, weight_hbm, faces_hbm, *params_hbm = refs[:9]
    out_ref, up_ref, down_ref, rank_ref, rank_t_ref, digits_ref, meta_ref, rows_ref, faces_ref, *params = refs[9:23]
    rb_ref, weight_ref, work_ref, to_slot_ref, to_row_ref, part_ref, sems = refs[23:]
    rb_copy, rows_copy, weight_copy, *others = fetch(
        [(rb_hbm, rb_ref), (rows_hbm, rows_ref), (weight_hbm, weight_ref), (faces_hbm, faces_ref),
         *zip(params_hbm, params, strict=True)], sems,
    )
    rb_copy.wait()
    chunks = plan_pairs(rb_ref, work_ref, rank_ref, rank_t_ref, digits_ref)
    present = jnp.where(rb_ref[CENTRE] != TABLE, 1.0, 0.0)
    meta_ref[0:1] = jnp.broadcast_to(jnp.sum(present, axis=1, keepdims=True), (1, CH)).astype(jnp.int32)
    meta_ref[1:2] = jnp.full((1, CH), chunks, jnp.int32)
    clear_padding(part_ref)
    rows_copy.wait()
    weight_copy.wait()
    itself = jnp.broadcast_to(rank_t_ref[:, 32:33], (ROWS, CH)) > 0
    out_ref[:ROWS] = jnp.where(itself, dot(rows_ref[...], weight_ref[CENTRE]), 0.0)
    out_ref[ROWS:] = jnp.zeros((EXT - ROWS, CH), jnp.float32)
    slots = part_ref.shape[0]

    def chunk(c, carry):
        slots_of_rows(rank_ref, c * SLOTS, to_slot_ref)
        picked = dot(to_slot_ref[...], rows_ref[...])
        multiply_slots(picked, weight_ref, lambda t: TAPS - 1 - (t + (t >= CENTRE)), part_ref)
        rows_of_slots(rank_t_ref, c * SLOTS, to_row_ref)
        found = dot(digits_ref[...], to_row_ref[...])
        digit = lax.broadcasted_iota(jnp.int32, (CH, slots), 0)
        tap = jnp.broadcast_to(tap_of_slot(lax.broadcasted_iota(jnp.int32, (1, slots), 1)), (CH, slots))
        worth = jnp.where(digit == tap, float(DIGIT), jnp.where(digit == tap + 32, 1.0, 0.0))
        target = jnp.sum(found * worth, axis=0, keepdims=True).astype(jnp.int32)
        added = dot(hot(target, (EXT, slots), 0), part_ref[...])
        out_ref[...] += added[:, :CH] + added[:, CH:]
        return carry

    lax.fori_loop(0, chunks, chunk, 0)
    for copy in others:
        copy.wait()
    picked = pick(face_hot(faces_ref, 2), out_ref[:ROWS])
    for ref, own, at, far in ((down_ref, picked[:FACE], 0, QH), (up_ref, picked[FACE:], FACE - COLUMN, QL)):
        pieces = [out_ref[A + at : A + at + COLUMN], own, out_ref[B + at : B + at + COLUMN]]
        ref[...] = jnp.concatenate([*pieces, out_ref[far : far + SIDE_ROWS]], axis=0).astype(jnp.bfloat16)


def tile_kernel(sums_ref, low_ref, high_ref, faces_ref, out_ref, left_ref, right_ref):
    out_ref[...] = sums_ref[...]
    first, last = SIDE_ROWS + COLUMN, SIDE_ROWS + COLUMN + FACE
    low, high = low_ref[...].astype(jnp.float32), high_ref[...].astype(jnp.float32)
    out_ref[QH:QL] += low[:SIDE_ROWS]
    out_ref[QL : QL + SIDE_ROWS] += high[:SIDE_ROWS]
    for sent, at in ((low, 0), (high, FACE - COLUMN)):
        out_ref[A + at : A + at + COLUMN] += sent[SIDE_ROWS:first]
        out_ref[B + at : B + at + COLUMN] += sent[last:]
    out_ref[:ROWS] += put(face_hot(faces_ref, 2), [low[first:last], high[first:last]])
    picked = pick(face_hot(faces_ref, 0), out_ref[:ROWS])
    for ref, own, own_at, far, far_at in (
        (left_ref, picked[:FACE], COLUMN, A, 0),
        (right_ref, picked[FACE:], FACE, B, FACE + COLUMN),
    ):
        pieces = []
        for face, at in ((own, own_at), (out_ref[far : far + FACE], far_at)):
            pieces += [face, out_ref[QH + at : QH + at + COLUMN], out_ref[QL + at : QL + at + COLUMN]]
        ref[...] = jnp.concatenate(pieces, axis=0).astype(jnp.bfloat16)


def slab_kernel(meta_ref, sums_ref, low_ref, high_ref, faces_ref, out_ref, stats_ref):
    out_ref[...] = sums_ref[...]
    low, high = low_ref[...].astype(jnp.float32), high_ref[...].astype(jnp.float32)
    for sent, far, far_at, own_at in ((low, A, 0, COLUMN), (high, B, FACE + COLUMN, FACE)):
        out_ref[far : far + FACE] += sent[:FACE]
        for start, at in ((0, far_at), (SIDE_ROWS, own_at)):
            out_ref[QH + at : QH + at + COLUMN] += sent[start + FACE : start + FACE + COLUMN]
            out_ref[QL + at : QL + at + COLUMN] += sent[start + FACE + COLUMN : start + SIDE_ROWS]
    own = slice(SIDE_ROWS, SIDE_ROWS + FACE)
    total = out_ref[:ROWS] + put(face_hot(faces_ref, 0), [low[own], high[own]])
    out_ref[:ROWS] = total
    write_sums(stats_ref, sums_of(total, meta_ref))


def sources(c, rank_ref, digits_ref, to_slot_ref):
    total = SIDES * SLOTS
    slots_of_rows(rank_ref, c * SLOTS, to_slot_ref)
    found = lax.dot_general(
        to_slot_ref[...], digits_ref[...], (((1,), (1,)), ((), ())), preferred_element_type=jnp.float32
    )
    tap = tap_of_slot(lax.broadcasted_iota(jnp.int32, (total, CH), 0))
    lane = lax.broadcasted_iota(jnp.int32, (total, CH), 1)
    worth = jnp.where(lane == tap, float(DIGIT), jnp.where(lane == tap + 32, 1.0, 0.0))
    source = jnp.sum(found * worth, axis=1, keepdims=True).astype(jnp.int32)
    return hot(jnp.bitwise_and(source, ROWS - 1), (total, ROWS), 1), jnp.broadcast_to(source, (total, CH))


def source_kernel(rank_ref, digits_ref, hot_ref, source_ref, to_slot_ref):
    hot_ref[...], source_ref[...] = sources(0, rank_ref, digits_ref, to_slot_ref)


def gather_kernel(
    meta_ref, first_ref, rank_ref, rank_t_ref, digits_ref, hot_ref, source_ref, weight_ref, stats_ref, gain_ref, shift_ref,
    out_ref, sums_ref, table_ref, to_slot_ref, to_row_ref, part_ref,
):
    norm = scale_of(total_of(stats_ref), gain_ref[...], shift_ref[...])
    live = live_rows(meta_ref)

    def act(values):
        return jnp.maximum(affine(values, *norm), 0.0)

    table_ref[:, :CH] = (live * act(first_ref[:ROWS])).astype(jnp.bfloat16)
    table_ref[:HALO, CH:] = act(first_ref[ROWS : ROWS + HALO]).astype(jnp.bfloat16)
    table_ref[HALO:, CH:] = jnp.zeros((ROWS - HALO, CH), jnp.bfloat16)
    out_ref[...] = dot(table_ref[:, :CH], weight_ref[CENTRE]) * live
    clear_padding(part_ref)

    def add(c, selector, source):
        both = dot(selector, table_ref[...])
        picked = jnp.where(source >= ROWS, both[:, CH:], both[:, :CH])
        multiply_slots(picked, weight_ref, lambda t: t + (t >= CENTRE), part_ref)
        rows_of_slots(rank_t_ref, c * SLOTS, to_row_ref)
        added = dot(to_row_ref[...], part_ref[...])
        out_ref[...] += added[:, :CH] + added[:, CH:]

    def chunk(c, carry):
        add(c, *sources(c, rank_ref, digits_ref, to_slot_ref))
        return carry

    add(0, hot_ref[...], source_ref[...])
    lax.fori_loop(1, jnp.max(meta_ref[1:2]), chunk, 0)
    write_sums(sums_ref, sums_of(out_ref[...], meta_ref))


def live_rows(meta_ref):
    rows = lax.broadcasted_iota(jnp.int32, (ROWS, CH), 0)
    return jnp.where(rows < jnp.broadcast_to(meta_ref[0:1], (ROWS, CH)), 1.0, 0.0)


def sums_of(conv_out, meta_ref):
    kept = conv_out * live_rows(meta_ref)
    first = jnp.sum(kept, axis=0, keepdims=True)
    second = jnp.sum(kept * conv_out, axis=0, keepdims=True)
    return jnp.concatenate([first, second, meta_ref[0:1].astype(jnp.float32)], axis=1)


def write_sums(sums_ref, sums):
    for i in range(sums_ref.shape[0]):
        sums_ref[i] = sums


def total_of(stats_ref):
    total = stats_ref[0]
    for i in range(1, stats_ref.shape[0]):
        total = total + stats_ref[i]
    return total


def near_kernel(stats_ref, out_ref):
    write_sums(out_ref, total_of(stats_ref))


def scale_of(sums, gain, shift):
    total = sums[:, 2 * CH :]
    average = sums[:, :CH] / total
    variance = sums[:, CH : 2 * CH] / total - average * average
    scale = lax.rsqrt(variance + EPSILON) * gain
    return average, scale, shift


def affine(values, average, scale, shift):
    return (values - average) * scale + shift


def finish_kernel(meta_ref, second_ref, rows_ref, stats_ref, gain_ref, shift_ref, out_ref):
    stats = total_of(stats_ref)
    norm = scale_of(stats, gain_ref[...], shift_ref[...])
    summed = affine(second_ref[...], *norm) + rows_ref[...].astype(jnp.float32)
    out_ref[...] = (live_rows(meta_ref) * jnp.maximum(summed, 0.0)).astype(jnp.bfloat16)


def call(kernel, outs, scratch, limit, *args, hbm=False):
    vmem = pl.BlockSpec(memory_space=pltpu.VMEM)
    if hbm:
        args = [pltpu.with_memory_space_constraint(a, pltpu.HBM) for a in args]
    return pl.pallas_call(
        kernel,
        out_shape=outs,
        in_specs=[pl.BlockSpec(memory_space=pltpu.HBM) if hbm else vmem] * len(args),
        out_specs=jax.tree.map(lambda _: vmem, outs),
        scratch_shapes=scratch,
        compiler_params=pltpu.CompilerParams(vmem_limit_bytes=limit << 20),
    )(*args)


def conv_scratch():
    padded = -(-SIDES * SLOTS // CH) * CH
    return [
        pltpu.VMEM((SIDES * SLOTS, ROWS), jnp.bfloat16),
        pltpu.VMEM((ROWS, padded), jnp.bfloat16),
        pltpu.VMEM((padded, 2 * CH), jnp.bfloat16),
    ]


def slab_neighbours(to_low, to_high):
    count = lax.axis_size(SLAB)
    even = lax.axis_index("slab_2") == 0
    across = [(i, i + 1) for i in range(1, count - 1, 2)] + [(i + 1, i) for i in range(1, count - 1, 2)]
    far = lax.ppermute(jnp.where(even, to_low, to_high), SLAB, across)
    both = lax.all_gather(jnp.where(even, to_high, to_low), "slab_2")
    return jnp.where(even, far, both[0]), jnp.where(even, both[1], far)


def tile_neighbours(to_low, to_high):
    count = lax.axis_size("tile")
    forward = [(i, i + 1) for i in range(count - 1)]
    backward = [(j, i) for i, j in forward]
    low = lax.ppermute(to_high, "tile", forward)
    high = lax.ppermute(to_low, "tile", backward)
    return low, high


def reduce_all(sums):
    near = lax.all_to_all(sums, ("slab_1", "slab_2"), 0, 0)
    far = lax.axis_size(("slab_0", "tile"))
    block = call(near_kernel, jax.ShapeDtypeStruct((far, 1, 3 * CH), jnp.float32), [], 4, near)
    return lax.all_to_all(block, ("slab_0", "tile"), 0, 0)


def per_device(
    features, counts, rulebook, face_rows, conv_one, gain_one, shift_one, conv_two, gain_two, shift_two
):
    del counts
    f32, bf16, i32 = jnp.float32, jnp.bfloat16, jnp.int32
    shaped = jax.ShapeDtypeStruct
    ext, message, big = shaped((EXT, CH), f32), shaped((2 * SIDE_ROWS, CH), bf16), shaped((ROWS, CH), f32)
    small = shaped((8, 1, 3 * CH), f32)
    params = (conv_two, gain_one[None], shift_one[None], gain_two[None], shift_two[None])
    outs = (
        ext, message, message,
        shaped((32, ROWS), i32), shaped((ROWS, CH), i32), shaped((CH, ROWS), bf16), shaped((8, CH), i32),
        shaped((ROWS, CH), bf16), shaped((4, FACE), i32), *(shaped(p.shape, p.dtype) for p in params),
    )
    scratch = [
        pltpu.VMEM((TAPS, 1, ROWS), i32), pltpu.VMEM((TAPS, CH, CH), bf16), pltpu.VMEM((32, ROWS), i32),
        *conv_scratch(), pltpu.SemaphoreType.DMA((9,)),
    ]
    taps = rulebook.reshape(TAPS, 1, ROWS)
    first, up, down, *plan, meta, rows, faces, weight_two, gain_one, shift_one, gain_two, shift_two = call(
        spread_kernel, outs, scratch, 24, taps, features[0, 0], conv_one, face_rows[0, 0], *params, hbm=True
    )
    total = SIDES * SLOTS
    outs = (shaped((total, ROWS), bf16), shaped((total, CH), i32))
    received = tile_neighbours(down, up)
    source = call(source_kernel, outs, conv_scratch()[:1], 8, plan[0], plan[2])
    first, left, right = call(tile_kernel, (ext, message, message), [], 8, first, *received, faces)
    received = slab_neighbours(left, right)
    first, sums = call(slab_kernel, (ext, small), [], 8, meta, first, *received, faces)
    stats = reduce_all(sums)
    second, sums = call(
        gather_kernel, (big, small), [pltpu.VMEM((ROWS, 2 * CH), bf16), *conv_scratch()], 24,
        meta, first, *plan, *source, weight_two, stats, gain_one, shift_one,
    )
    stats = reduce_all(sums)
    out = call(
        finish_kernel, shaped((ROWS, CH), bf16), [], 4, meta, second, rows, stats, gain_two, shift_two
    )
    return out[None, None]


def solution(mesh):
    tiles = mesh.shape["tile"]
    torus = Mesh(
        mesh.devices.reshape(-1, 4, 2, tiles), ("slab_0", "slab_1", "slab_2", "tile")
    )
    split = P(SLAB, "tile", None, None)
    in_specs = (split, P(SLAB, "tile"), split, split, P(), P(), P(), P(), P(), P())
    return jax.shard_map(
        per_device, mesh=torus, in_specs=in_specs, out_specs=split, check_vma=False
    )
```

```python
import jax
import jax.numpy as jnp
from jax import lax
from jax.experimental import pallas as pl
from jax.experimental.pallas import tpu as pltpu
from jax.sharding import Mesh
from jax.sharding import PartitionSpec as P

ROWS = 512
CH = 128
TAPS = 27
SIDES = 26
CENTRE = 13
SLOTS = 24
DIGIT = 32
TABLE = 800
FACE = 64
COLUMN = 8
SIDE_ROWS = FACE + 2 * COLUMN
HALO = 2 * FACE + 2 * SIDE_ROWS
EXT = 832
SLAB = ("slab_0", "slab_1", "slab_2")
EPSILON = 1e-05


A, B, QH, QL = ROWS, ROWS + FACE, ROWS + 2 * FACE, ROWS + 2 * FACE + SIDE_ROWS


def dot(a, b, **kw):
    return jnp.dot(a, b, preferred_element_type=jnp.float32, **kw)


def hot(index, shape, dim):
    return jnp.where(jnp.broadcast_to(index, shape) == lax.broadcasted_iota(jnp.int32, shape, dim), 1.0, 0.0).astype(
        jnp.bfloat16
    )


def fetch(pairs, sems):
    copies = [pltpu.make_async_copy(src, dst, sems.at[i]) for i, (src, dst) in enumerate(pairs)]
    for copy in copies:
        copy.start()
    return copies


def face_hot(faces_ref, k):
    return hot(jnp.concatenate([faces_ref[k : k + 1, :], faces_ref[k + 1 : k + 2, :]], axis=1), (ROWS, 2 * FACE), 0)


def pick(selector, rows):
    return lax.dot_general(
        selector, rows.astype(jnp.bfloat16), (((0,), (0,)), ((), ())), preferred_element_type=jnp.float32
    )


def put(selector, values):
    return dot(selector, jnp.concatenate(values, axis=0).astype(jnp.bfloat16))


def plan_pairs(rb_ref, work_ref, rank_ref, rank_t_ref, digits_ref):
    work_ref[...] = jnp.full_like(work_ref, TABLE)
    for t in range(SIDES):
        work_ref[t : t + 1, :] = rb_ref[t + (t >= CENTRE)]
    entry = work_ref[...]
    present = entry != TABLE
    ones = jnp.where(present, 1.0, 0.0)
    before = lax.broadcasted_iota(jnp.int32, (ROWS, ROWS), 0) < lax.broadcasted_iota(jnp.int32, (ROWS, ROWS), 1)
    place = dot(ones.astype(jnp.bfloat16), jnp.where(before, 1.0, 0.0).astype(jnp.bfloat16))
    rank = jnp.where(present, place.astype(jnp.int32), -1)
    rank_ref[...] = rank
    itself = jnp.broadcast_to(jnp.where(rb_ref[CENTRE] != TABLE, 1, -1), (8, ROWS))
    padded = jnp.concatenate([rank, itself, jnp.full((CH - 40, ROWS), -1, jnp.int32)], axis=0)
    rank_t_ref[...] = padded.T
    digits_ref[...] = jnp.concatenate(
        [(entry // DIGIT).astype(jnp.float32), (entry % DIGIT).astype(jnp.float32),
         jnp.zeros((CH - 2 * entry.shape[0], ROWS), jnp.float32)], axis=0
    ).astype(jnp.bfloat16)
    most = jnp.max(jnp.sum(ones, axis=1, keepdims=True))
    return (most.astype(jnp.int32) + (SLOTS - 1)) // SLOTS


def slots_of_rows(rank_ref, base, to_slot_ref):
    slot = lax.broadcasted_iota(jnp.int32, (SLOTS, ROWS), 0) + base
    blocks = []
    for t in range(SIDES):
        match = jnp.broadcast_to(rank_ref[t : t + 1, :], (SLOTS, ROWS)) == slot
        blocks.append(jnp.where(match, 1.0, 0.0))
    to_slot_ref[...] = jnp.concatenate(blocks, axis=0).astype(jnp.bfloat16)


def tap_of_slot(slot):
    return jnp.right_shift(slot * 2731, 16)


def rows_of_slots(rank_t_ref, base, to_row_ref):
    for i in range(to_row_ref.shape[1] // CH):
        slot = lax.broadcasted_iota(jnp.int32, (1, CH), 1) + i * CH
        tap = tap_of_slot(slot)
        wanted = jnp.broadcast_to(slot - tap * SLOTS + base, (ROWS, CH))
        spread = jnp.take_along_axis(
            rank_t_ref[...], jnp.broadcast_to(tap, (ROWS, CH)), axis=1, mode="promise_in_bounds"
        )
        to_row_ref[:, i * CH : (i + 1) * CH] = jnp.where(spread == wanted, 1.0, 0.0).astype(jnp.bfloat16)


def multiply_slots(picked, weight_ref, tap_of, part_ref):
    parts = []
    for t in range(0, SIDES, 2):
        both = jnp.concatenate([weight_ref[tap_of(t)], weight_ref[tap_of(t + 1)]], axis=1)
        got = dot(picked[t * SLOTS : (t + 2) * SLOTS].astype(jnp.bfloat16), both)
        parts += [got[:SLOTS, :CH], got[SLOTS:, CH:]]
    part = jnp.concatenate(parts, axis=0)
    high = part.astype(jnp.bfloat16)
    part_ref[: SIDES * SLOTS, :CH] = high
    part_ref[: SIDES * SLOTS, CH:] = (part - high.astype(jnp.float32)).astype(jnp.bfloat16)


def clear_padding(part_ref):
    part_ref[SIDES * SLOTS :, :] = jnp.zeros((part_ref.shape[0] - SIDES * SLOTS, 2 * CH), jnp.bfloat16)


def spread_kernel(*refs):
    rb_hbm, rows_hbm, weight_hbm, faces_hbm, *params_hbm = refs[:9]
    out_ref, up_ref, down_ref, rank_ref, rank_t_ref, digits_ref, meta_ref, rows_ref, faces_ref, *params = refs[9:23]
    rb_ref, weight_ref, work_ref, to_slot_ref, to_row_ref, part_ref, sems = refs[23:]
    rb_copy, rows_copy, weight_copy, *others = fetch(
        [(rb_hbm, rb_ref), (rows_hbm, rows_ref), (weight_hbm, weight_ref), (faces_hbm, faces_ref),
         *zip(params_hbm, params, strict=True)], sems,
    )
    rb_copy.wait()
    chunks = plan_pairs(rb_ref, work_ref, rank_ref, rank_t_ref, digits_ref)
    present = jnp.where(rb_ref[CENTRE] != TABLE, 1.0, 0.0)
    meta_ref[0:1] = jnp.broadcast_to(jnp.sum(present, axis=1, keepdims=True), (1, CH)).astype(jnp.int32)
    meta_ref[1:2] = jnp.full((1, CH), chunks, jnp.int32)
    clear_padding(part_ref)
    rows_copy.wait()
    weight_copy.wait()
    itself = jnp.broadcast_to(rank_t_ref[:, 32:33], (ROWS, CH)) > 0
    out_ref[:ROWS] = jnp.where(itself, dot(rows_ref[...], weight_ref[CENTRE]), 0.0)
    out_ref[ROWS:] = jnp.zeros((EXT - ROWS, CH), jnp.float32)
    slots = part_ref.shape[0]

    def chunk(c, carry):
        slots_of_rows(rank_ref, c * SLOTS, to_slot_ref)
        picked = dot(to_slot_ref[...], rows_ref[...])
        multiply_slots(picked, weight_ref, lambda t: TAPS - 1 - (t + (t >= CENTRE)), part_ref)
        rows_of_slots(rank_t_ref, c * SLOTS, to_row_ref)
        found = dot(digits_ref[...], to_row_ref[...])
        digit = lax.broadcasted_iota(jnp.int32, (CH, slots), 0)
        tap = jnp.broadcast_to(tap_of_slot(lax.broadcasted_iota(jnp.int32, (1, slots), 1)), (CH, slots))
        worth = jnp.where(digit == tap, float(DIGIT), jnp.where(digit == tap + 32, 1.0, 0.0))
        target = jnp.sum(found * worth, axis=0, keepdims=True).astype(jnp.int32)
        added = dot(hot(target, (EXT, slots), 0), part_ref[...])
        out_ref[...] += added[:, :CH] + added[:, CH:]
        return carry

    lax.fori_loop(0, chunks, chunk, 0)
    for copy in others:
        copy.wait()
    picked = pick(face_hot(faces_ref, 2), out_ref[:ROWS])
    for ref, own, at, far in ((down_ref, picked[:FACE], 0, QH), (up_ref, picked[FACE:], FACE - COLUMN, QL)):
        pieces = [out_ref[A + at : A + at + COLUMN], own, out_ref[B + at : B + at + COLUMN]]
        ref[...] = jnp.concatenate([*pieces, out_ref[far : far + SIDE_ROWS]], axis=0).astype(jnp.bfloat16)


def tile_kernel(sums_ref, low_ref, high_ref, faces_ref, out_ref, left_ref, right_ref):
    out_ref[...] = sums_ref[...]
    first, last = SIDE_ROWS + COLUMN, SIDE_ROWS + COLUMN + FACE
    low, high = low_ref[...].astype(jnp.float32), high_ref[...].astype(jnp.float32)
    out_ref[QH:QL] += low[:SIDE_ROWS]
    out_ref[QL : QL + SIDE_ROWS] += high[:SIDE_ROWS]
    for sent, at in ((low, 0), (high, FACE - COLUMN)):
        out_ref[A + at : A + at + COLUMN] += sent[SIDE_ROWS:first]
        out_ref[B + at : B + at + COLUMN] += sent[last:]
    out_ref[:ROWS] += put(face_hot(faces_ref, 2), [low[first:last], high[first:last]])
    picked = pick(face_hot(faces_ref, 0), out_ref[:ROWS])
    for ref, own, own_at, far, far_at in (
        (left_ref, picked[:FACE], COLUMN, A, 0),
        (right_ref, picked[FACE:], FACE, B, FACE + COLUMN),
    ):
        pieces = []
        for face, at in ((own, own_at), (out_ref[far : far + FACE], far_at)):
            pieces += [face, out_ref[QH + at : QH + at + COLUMN], out_ref[QL + at : QL + at + COLUMN]]
        ref[...] = jnp.concatenate(pieces, axis=0).astype(jnp.bfloat16)


def slab_kernel(meta_ref, sums_ref, low_ref, high_ref, faces_ref, out_ref, stats_ref):
    out_ref[...] = sums_ref[...]
    low, high = low_ref[...].astype(jnp.float32), high_ref[...].astype(jnp.float32)
    for sent, far, far_at, own_at in ((low, A, 0, COLUMN), (high, B, FACE + COLUMN, FACE)):
        out_ref[far : far + FACE] += sent[:FACE]
        for start, at in ((0, far_at), (SIDE_ROWS, own_at)):
            out_ref[QH + at : QH + at + COLUMN] += sent[start + FACE : start + FACE + COLUMN]
            out_ref[QL + at : QL + at + COLUMN] += sent[start + FACE + COLUMN : start + SIDE_ROWS]
    own = slice(SIDE_ROWS, SIDE_ROWS + FACE)
    total = out_ref[:ROWS] + put(face_hot(faces_ref, 0), [low[own], high[own]])
    out_ref[:ROWS] = total
    write_sums(stats_ref, sums_of(total, meta_ref))


def sources(c, rank_ref, digits_ref, to_slot_ref):
    total = SIDES * SLOTS
    slots_of_rows(rank_ref, c * SLOTS, to_slot_ref)
    found = lax.dot_general(
        to_slot_ref[...], digits_ref[...], (((1,), (1,)), ((), ())), preferred_element_type=jnp.float32
    )
    tap = tap_of_slot(lax.broadcasted_iota(jnp.int32, (total, CH), 0))
    lane = lax.broadcasted_iota(jnp.int32, (total, CH), 1)
    worth = jnp.where(lane == tap, float(DIGIT), jnp.where(lane == tap + 32, 1.0, 0.0))
    source = jnp.sum(found * worth, axis=1, keepdims=True).astype(jnp.int32)
    return hot(jnp.bitwise_and(source, ROWS - 1), (total, ROWS), 1), jnp.broadcast_to(source, (total, CH))


def source_kernel(rank_ref, digits_ref, hot_ref, source_ref, to_slot_ref):
    hot_ref[...], source_ref[...] = sources(0, rank_ref, digits_ref, to_slot_ref)


def gather_kernel(
    meta_ref, first_ref, rank_ref, rank_t_ref, digits_ref, hot_ref, source_ref, weight_ref, stats_ref, gain_ref, shift_ref,
    out_ref, sums_ref, table_ref, to_slot_ref, to_row_ref, part_ref,
):
    norm = scale_of(total_of(stats_ref), gain_ref[...], shift_ref[...])
    live = live_rows(meta_ref)

    def act(values):
        return jnp.maximum(affine(values, *norm), 0.0)

    table_ref[:, :CH] = (live * act(first_ref[:ROWS])).astype(jnp.bfloat16)
    table_ref[:HALO, CH:] = act(first_ref[ROWS : ROWS + HALO]).astype(jnp.bfloat16)
    table_ref[HALO:, CH:] = jnp.zeros((ROWS - HALO, CH), jnp.bfloat16)
    out_ref[...] = dot(table_ref[:, :CH], weight_ref[CENTRE]) * live
    clear_padding(part_ref)

    def add(c, selector, source):
        both = dot(selector, table_ref[...])
        picked = jnp.where(source >= ROWS, both[:, CH:], both[:, :CH])
        multiply_slots(picked, weight_ref, lambda t: t + (t >= CENTRE), part_ref)
        rows_of_slots(rank_t_ref, c * SLOTS, to_row_ref)
        added = dot(to_row_ref[...], part_ref[...])
        out_ref[...] += added[:, :CH] + added[:, CH:]

    def chunk(c, carry):
        add(c, *sources(c, rank_ref, digits_ref, to_slot_ref))
        return carry

    add(0, hot_ref[...], source_ref[...])
    lax.fori_loop(1, jnp.max(meta_ref[1:2]), chunk, 0)
    write_sums(sums_ref, sums_of(out_ref[...], meta_ref))


def live_rows(meta_ref):
    rows = lax.broadcasted_iota(jnp.int32, (ROWS, CH), 0)
    return jnp.where(rows < jnp.broadcast_to(meta_ref[0:1], (ROWS, CH)), 1.0, 0.0)


def sums_of(conv_out, meta_ref):
    kept = conv_out * live_rows(meta_ref)
    first = jnp.sum(kept, axis=0, keepdims=True)
    second = jnp.sum(kept * conv_out, axis=0, keepdims=True)
    return jnp.concatenate([first, second, meta_ref[0:1].astype(jnp.float32)], axis=1)


def write_sums(sums_ref, sums):
    for i in range(sums_ref.shape[0]):
        sums_ref[i] = sums


def total_of(stats_ref):
    parts = [stats_ref[i] for i in range(stats_ref.shape[0])]
    while len(parts) > 1:
        parts = [a + b for a, b in zip(parts[::2], parts[1::2], strict=True)]
    return parts[0]


def near_kernel(stats_ref, out_ref):
    write_sums(out_ref, total_of(stats_ref))


def scale_of(sums, gain, shift):
    total = sums[:, 2 * CH :]
    average = sums[:, :CH] / total
    variance = sums[:, CH : 2 * CH] / total - average * average
    scale = lax.rsqrt(variance + EPSILON) * gain
    return average, scale, shift


def affine(values, average, scale, shift):
    return (values - average) * scale + shift


def finish_kernel(meta_ref, second_ref, rows_ref, stats_ref, gain_ref, shift_ref, out_ref):
    stats = total_of(stats_ref)
    norm = scale_of(stats, gain_ref[...], shift_ref[...])
    summed = affine(second_ref[...], *norm) + rows_ref[...].astype(jnp.float32)
    out_ref[...] = (live_rows(meta_ref) * jnp.maximum(summed, 0.0)).astype(jnp.bfloat16)


def call(kernel, outs, scratch, limit, *args, hbm=False):
    vmem = pl.BlockSpec(memory_space=pltpu.VMEM)
    if hbm:
        args = [pltpu.with_memory_space_constraint(a, pltpu.HBM) for a in args]
    return pl.pallas_call(
        kernel,
        out_shape=outs,
        in_specs=[pl.BlockSpec(memory_space=pltpu.HBM) if hbm else vmem] * len(args),
        out_specs=jax.tree.map(lambda _: vmem, outs),
        scratch_shapes=scratch,
        compiler_params=pltpu.CompilerParams(vmem_limit_bytes=limit << 20),
    )(*args)


def conv_scratch():
    padded = -(-SIDES * SLOTS // CH) * CH
    return [
        pltpu.VMEM((SIDES * SLOTS, ROWS), jnp.bfloat16),
        pltpu.VMEM((ROWS, padded), jnp.bfloat16),
        pltpu.VMEM((padded, 2 * CH), jnp.bfloat16),
    ]


def slab_neighbours(to_low, to_high):
    count = lax.axis_size(SLAB)
    even = lax.axis_index("slab_2") == 0
    across = [(i, i + 1) for i in range(1, count - 1, 2)] + [(i + 1, i) for i in range(1, count - 1, 2)]
    far = lax.ppermute(jnp.where(even, to_low, to_high), SLAB, across)
    both = lax.all_gather(jnp.where(even, to_high, to_low), "slab_2")
    return jnp.where(even, far, both[0]), jnp.where(even, both[1], far)


def tile_neighbours(to_low, to_high):
    count = lax.axis_size("tile")
    forward = [(i, i + 1) for i in range(count - 1)]
    backward = [(j, i) for i, j in forward]
    low = lax.ppermute(to_high, "tile", forward)
    high = lax.ppermute(to_low, "tile", backward)
    return low, high


def reduce_all(sums):
    near = lax.all_to_all(sums, ("slab_1", "slab_2"), 0, 0)
    far = lax.axis_size(("slab_0", "tile"))
    block = call(near_kernel, jax.ShapeDtypeStruct((far, 1, 3 * CH), jnp.float32), [], 4, near)
    return lax.all_to_all(block, ("slab_0", "tile"), 0, 0)


def per_device(
    features, counts, rulebook, face_rows, conv_one, gain_one, shift_one, conv_two, gain_two, shift_two
):
    del counts
    f32, bf16, i32 = jnp.float32, jnp.bfloat16, jnp.int32
    shaped = jax.ShapeDtypeStruct
    ext, message, big = shaped((EXT, CH), f32), shaped((2 * SIDE_ROWS, CH), bf16), shaped((ROWS, CH), f32)
    small = shaped((8, 1, 3 * CH), f32)
    params = (conv_two, gain_one[None], shift_one[None], gain_two[None], shift_two[None])
    outs = (
        ext, message, message,
        shaped((32, ROWS), i32), shaped((ROWS, CH), i32), shaped((CH, ROWS), bf16), shaped((8, CH), i32),
        shaped((ROWS, CH), bf16), shaped((4, FACE), i32), *(shaped(p.shape, p.dtype) for p in params),
    )
    scratch = [
        pltpu.VMEM((TAPS, 1, ROWS), i32), pltpu.VMEM((TAPS, CH, CH), bf16), pltpu.VMEM((32, ROWS), i32),
        *conv_scratch(), pltpu.SemaphoreType.DMA((9,)),
    ]
    taps = rulebook.reshape(TAPS, 1, ROWS)
    first, up, down, *plan, meta, rows, faces, weight_two, gain_one, shift_one, gain_two, shift_two = call(
        spread_kernel, outs, scratch, 24, taps, features[0, 0], conv_one, face_rows[0, 0], *params, hbm=True
    )
    total = SIDES * SLOTS
    outs = (shaped((total, ROWS), bf16), shaped((total, CH), i32))
    received = tile_neighbours(down, up)
    source = call(source_kernel, outs, conv_scratch()[:1], 8, plan[0], plan[2])
    first, left, right = call(tile_kernel, (ext, message, message), [], 8, first, *received, faces)
    received = slab_neighbours(left, right)
    first, sums = call(slab_kernel, (ext, small), [], 8, meta, first, *received, faces)
    stats = reduce_all(sums)
    second, sums = call(
        gather_kernel, (big, small), [pltpu.VMEM((ROWS, 2 * CH), bf16), *conv_scratch()], 24,
        meta, first, *plan, *source, weight_two, stats, gain_one, shift_one,
    )
    stats = reduce_all(sums)
    out = call(
        finish_kernel, shaped((ROWS, CH), bf16), [], 4, meta, second, rows, stats, gain_two, shift_two
    )
    return out[None, None]


def solution(mesh):
    tiles = mesh.shape["tile"]
    torus = Mesh(
        mesh.devices.reshape(-1, 4, 2, tiles), ("slab_0", "slab_1", "slab_2", "tile")
    )
    split = P(SLAB, "tile", None, None)
    in_specs = (split, P(SLAB, "tile"), split, split, P(), P(), P(), P(), P(), P())
    return jax.shard_map(
        per_device, mesh=torus, in_specs=in_specs, out_specs=split, check_vma=False
    )
```

```python
import jax
import jax.numpy as jnp
from jax import lax
from jax.experimental import pallas as pl
from jax.experimental.pallas import tpu as pltpu
from jax.sharding import Mesh
from jax.sharding import PartitionSpec as P

ROWS = 512
CH = 128
TAPS = 27
SIDES = 26
CENTRE = 13
SLOTS = 24
DIGIT = 32
TABLE = 800
FACE = 64
COLUMN = 8
SIDE_ROWS = FACE + 2 * COLUMN
HALO = 2 * FACE + 2 * SIDE_ROWS
EXT = 832
SLAB = ("slab_0", "slab_1", "slab_2")
EPSILON = 1e-05


A, B, QH, QL = ROWS, ROWS + FACE, ROWS + 2 * FACE, ROWS + 2 * FACE + SIDE_ROWS


def dot(a, b, **kw):
    return jnp.dot(a, b, preferred_element_type=jnp.float32, **kw)


def hot(index, shape, dim):
    return jnp.where(jnp.broadcast_to(index, shape) == lax.broadcasted_iota(jnp.int32, shape, dim), 1.0, 0.0).astype(
        jnp.bfloat16
    )


def fetch(pairs, sems):
    copies = [pltpu.make_async_copy(src, dst, sems.at[i]) for i, (src, dst) in enumerate(pairs)]
    for copy in copies:
        copy.start()
    return copies


def face_hot(faces_ref, k):
    return hot(jnp.concatenate([faces_ref[k : k + 1, :], faces_ref[k + 1 : k + 2, :]], axis=1), (ROWS, 2 * FACE), 0)


def pick(selector, rows):
    return lax.dot_general(
        selector, rows.astype(jnp.bfloat16), (((0,), (0,)), ((), ())), preferred_element_type=jnp.float32
    )


def put(selector, values):
    return dot(selector, jnp.concatenate(values, axis=0).astype(jnp.bfloat16))


def plan_pairs(rb_ref, work_ref, rank_ref, rank_t_ref, digits_ref):
    work_ref[...] = jnp.full_like(work_ref, TABLE)
    for t in range(SIDES):
        work_ref[t : t + 1, :] = rb_ref[t + (t >= CENTRE)]
    entry = work_ref[...]
    present = entry != TABLE
    ones = jnp.where(present, 1.0, 0.0)
    before = lax.broadcasted_iota(jnp.int32, (ROWS, ROWS), 0) < lax.broadcasted_iota(jnp.int32, (ROWS, ROWS), 1)
    place = dot(ones.astype(jnp.bfloat16), jnp.where(before, 1.0, 0.0).astype(jnp.bfloat16))
    rank = jnp.where(present, place.astype(jnp.int32), -1)
    rank_ref[...] = rank
    itself = jnp.broadcast_to(jnp.where(rb_ref[CENTRE] != TABLE, 1, -1), (8, ROWS))
    padded = jnp.concatenate([rank, itself, jnp.full((CH - 40, ROWS), -1, jnp.int32)], axis=0)
    rank_t_ref[...] = padded.T
    digits_ref[...] = jnp.concatenate(
        [(entry // DIGIT).astype(jnp.float32), (entry % DIGIT).astype(jnp.float32),
         jnp.zeros((CH - 2 * entry.shape[0], ROWS), jnp.float32)], axis=0
    ).astype(jnp.bfloat16)
    most = jnp.max(jnp.sum(ones, axis=1, keepdims=True))
    return (most.astype(jnp.int32) + (SLOTS - 1)) // SLOTS


def slots_of_rows(rank_ref, base, to_slot_ref):
    slot = lax.broadcasted_iota(jnp.int32, (SLOTS, ROWS), 0) + base
    blocks = []
    for t in range(SIDES):
        match = jnp.broadcast_to(rank_ref[t : t + 1, :], (SLOTS, ROWS)) == slot
        blocks.append(jnp.where(match, 1.0, 0.0))
    to_slot_ref[...] = jnp.concatenate(blocks, axis=0).astype(jnp.bfloat16)


def tap_of_slot(slot):
    return jnp.right_shift(slot * 2731, 16)


def rows_of_slots(rank_t_ref, base, to_row_ref):
    for i in range(to_row_ref.shape[1] // CH):
        slot = lax.broadcasted_iota(jnp.int32, (1, CH), 1) + i * CH
        tap = tap_of_slot(slot)
        wanted = jnp.broadcast_to(slot - tap * SLOTS + base, (ROWS, CH))
        spread = jnp.take_along_axis(
            rank_t_ref[...], jnp.broadcast_to(tap, (ROWS, CH)), axis=1, mode="promise_in_bounds"
        )
        to_row_ref[:, i * CH : (i + 1) * CH] = jnp.where(spread == wanted, 1.0, 0.0).astype(jnp.bfloat16)


def multiply_slots(picked, weight_ref, tap_of, part_ref):
    parts = []
    for t in range(0, SIDES, 2):
        both = jnp.concatenate([weight_ref[tap_of(t)], weight_ref[tap_of(t + 1)]], axis=1)
        got = dot(picked[t * SLOTS : (t + 2) * SLOTS].astype(jnp.bfloat16), both)
        parts += [got[:SLOTS, :CH], got[SLOTS:, CH:]]
    part = jnp.concatenate(parts, axis=0)
    high = part.astype(jnp.bfloat16)
    part_ref[: SIDES * SLOTS, :CH] = high
    part_ref[: SIDES * SLOTS, CH:] = (part - high.astype(jnp.float32)).astype(jnp.bfloat16)


def clear_padding(part_ref):
    part_ref[SIDES * SLOTS :, :] = jnp.zeros((part_ref.shape[0] - SIDES * SLOTS, 2 * CH), jnp.bfloat16)


def spread_kernel(*refs):
    rb_hbm, rows_hbm, weight_hbm, faces_hbm, *params_hbm = refs[:9]
    out_ref, up_ref, down_ref, rank_ref, rank_t_ref, digits_ref, meta_ref, rows_ref, faces_ref, *params = refs[9:23]
    rb_ref, weight_ref, work_ref, to_slot_ref, to_row_ref, part_ref, sems = refs[23:]
    rb_copy, rows_copy, weight_copy, *others = fetch(
        [(rb_hbm, rb_ref), (rows_hbm, rows_ref), (weight_hbm, weight_ref), (faces_hbm, faces_ref),
         *zip(params_hbm, params, strict=True)], sems,
    )
    rb_copy.wait()
    chunks = plan_pairs(rb_ref, work_ref, rank_ref, rank_t_ref, digits_ref)
    present = jnp.where(rb_ref[CENTRE] != TABLE, 1.0, 0.0)
    meta_ref[0:1] = jnp.broadcast_to(jnp.sum(present, axis=1, keepdims=True), (1, CH)).astype(jnp.int32)
    meta_ref[1:2] = jnp.full((1, CH), chunks, jnp.int32)
    clear_padding(part_ref)
    rows_copy.wait()
    weight_copy.wait()
    itself = jnp.broadcast_to(rank_t_ref[:, 32:33], (ROWS, CH)) > 0
    out_ref[:ROWS] = jnp.where(itself, dot(rows_ref[...], weight_ref[CENTRE]), 0.0)
    out_ref[ROWS:] = jnp.zeros((EXT - ROWS, CH), jnp.float32)
    slots = part_ref.shape[0]

    def chunk(c, carry):
        slots_of_rows(rank_ref, c * SLOTS, to_slot_ref)
        picked = dot(to_slot_ref[...], rows_ref[...])
        multiply_slots(picked, weight_ref, lambda t: TAPS - 1 - (t + (t >= CENTRE)), part_ref)
        rows_of_slots(rank_t_ref, c * SLOTS, to_row_ref)
        found = dot(digits_ref[...], to_row_ref[...])
        digit = lax.broadcasted_iota(jnp.int32, (CH, slots), 0)
        tap = jnp.broadcast_to(tap_of_slot(lax.broadcasted_iota(jnp.int32, (1, slots), 1)), (CH, slots))
        worth = jnp.where(digit == tap, float(DIGIT), jnp.where(digit == tap + 32, 1.0, 0.0))
        target = jnp.sum(found * worth, axis=0, keepdims=True).astype(jnp.int32)
        added = dot(hot(target, (EXT, slots), 0), part_ref[...])
        out_ref[...] += added[:, :CH] + added[:, CH:]
        return carry

    lax.fori_loop(0, chunks, chunk, 0)
    for copy in others:
        copy.wait()
    picked = pick(face_hot(faces_ref, 2), out_ref[:ROWS])
    for ref, own, at, far in ((down_ref, picked[:FACE], 0, QH), (up_ref, picked[FACE:], FACE - COLUMN, QL)):
        pieces = [out_ref[A + at : A + at + COLUMN], own, out_ref[B + at : B + at + COLUMN]]
        ref[...] = jnp.concatenate([*pieces, out_ref[far : far + SIDE_ROWS]], axis=0).astype(jnp.bfloat16)


def tile_kernel(sums_ref, low_ref, high_ref, faces_ref, out_ref, left_ref, right_ref):
    out_ref[...] = sums_ref[...]
    first, last = SIDE_ROWS + COLUMN, SIDE_ROWS + COLUMN + FACE
    low, high = low_ref[...].astype(jnp.float32), high_ref[...].astype(jnp.float32)
    out_ref[QH:QL] += low[:SIDE_ROWS]
    out_ref[QL : QL + SIDE_ROWS] += high[:SIDE_ROWS]
    for sent, at in ((low, 0), (high, FACE - COLUMN)):
        out_ref[A + at : A + at + COLUMN] += sent[SIDE_ROWS:first]
        out_ref[B + at : B + at + COLUMN] += sent[last:]
    out_ref[:ROWS] += put(face_hot(faces_ref, 2), [low[first:last], high[first:last]])
    picked = pick(face_hot(faces_ref, 0), out_ref[:ROWS])
    for ref, own, own_at, far, far_at in (
        (left_ref, picked[:FACE], COLUMN, A, 0),
        (right_ref, picked[FACE:], FACE, B, FACE + COLUMN),
    ):
        pieces = []
        for face, at in ((own, own_at), (out_ref[far : far + FACE], far_at)):
            pieces += [face, out_ref[QH + at : QH + at + COLUMN], out_ref[QL + at : QL + at + COLUMN]]
        ref[...] = jnp.concatenate(pieces, axis=0).astype(jnp.bfloat16)


def slab_kernel(meta_ref, sums_ref, low_ref, high_ref, faces_ref, out_ref, stats_ref):
    out_ref[...] = sums_ref[...]
    low, high = low_ref[...].astype(jnp.float32), high_ref[...].astype(jnp.float32)
    for sent, far, far_at, own_at in ((low, A, 0, COLUMN), (high, B, FACE + COLUMN, FACE)):
        out_ref[far : far + FACE] += sent[:FACE]
        for start, at in ((0, far_at), (SIDE_ROWS, own_at)):
            out_ref[QH + at : QH + at + COLUMN] += sent[start + FACE : start + FACE + COLUMN]
            out_ref[QL + at : QL + at + COLUMN] += sent[start + FACE + COLUMN : start + SIDE_ROWS]
    own = slice(SIDE_ROWS, SIDE_ROWS + FACE)
    total = out_ref[:ROWS] + put(face_hot(faces_ref, 0), [low[own], high[own]])
    out_ref[:ROWS] = total
    write_sums(stats_ref, sums_of(total, meta_ref))


def sources(c, rank_ref, digits_ref, to_slot_ref):
    total = SIDES * SLOTS
    slots_of_rows(rank_ref, c * SLOTS, to_slot_ref)
    found = lax.dot_general(
        to_slot_ref[...], digits_ref[...], (((1,), (1,)), ((), ())), preferred_element_type=jnp.float32
    )
    tap = tap_of_slot(lax.broadcasted_iota(jnp.int32, (total, CH), 0))
    lane = lax.broadcasted_iota(jnp.int32, (total, CH), 1)
    worth = jnp.where(lane == tap, float(DIGIT), jnp.where(lane == tap + 32, 1.0, 0.0))
    source = jnp.sum(found * worth, axis=1, keepdims=True).astype(jnp.int32)
    return hot(jnp.bitwise_and(source, ROWS - 1), (total, ROWS), 1), jnp.broadcast_to(source, (total, CH))


def source_kernel(rank_ref, digits_ref, hot_ref, source_ref, to_slot_ref):
    hot_ref[...], source_ref[...] = sources(0, rank_ref, digits_ref, to_slot_ref)


def gather_kernel(
    meta_ref, first_ref, rank_ref, rank_t_ref, digits_ref, hot_ref, source_ref, weight_ref, stats_ref, gain_ref, shift_ref,
    out_ref, sums_ref, table_ref, to_slot_ref, to_row_ref, part_ref,
):
    norm = scale_of(total_of(stats_ref), gain_ref[...], shift_ref[...])
    live = live_rows(meta_ref)

    def act(values):
        return jnp.maximum(affine(values, *norm), 0.0)

    table_ref[:, :CH] = (live * act(first_ref[:ROWS])).astype(jnp.bfloat16)
    table_ref[:HALO, CH:] = act(first_ref[ROWS : ROWS + HALO]).astype(jnp.bfloat16)
    table_ref[HALO:, CH:] = jnp.zeros((ROWS - HALO, CH), jnp.bfloat16)
    out_ref[...] = dot(table_ref[:, :CH], weight_ref[CENTRE]) * live
    clear_padding(part_ref)

    def add(c, selector, source):
        both = dot(selector, table_ref[...])
        picked = jnp.where(source >= ROWS, both[:, CH:], both[:, :CH])
        multiply_slots(picked, weight_ref, lambda t: t + (t >= CENTRE), part_ref)
        rows_of_slots(rank_t_ref, c * SLOTS, to_row_ref)
        added = dot(to_row_ref[...], part_ref[...])
        out_ref[...] += added[:, :CH] + added[:, CH:]

    def chunk(c, carry):
        add(c, *sources(c, rank_ref, digits_ref, to_slot_ref))
        return carry

    add(0, hot_ref[...], source_ref[...])
    lax.fori_loop(1, jnp.max(meta_ref[1:2]), chunk, 0)
    write_sums(sums_ref, sums_of(out_ref[...], meta_ref))


def live_rows(meta_ref):
    rows = lax.broadcasted_iota(jnp.int32, (ROWS, CH), 0)
    return jnp.where(rows < jnp.broadcast_to(meta_ref[0:1], (ROWS, CH)), 1.0, 0.0)


def sums_of(conv_out, meta_ref):
    kept = conv_out * live_rows(meta_ref)
    first = jnp.sum(kept, axis=0, keepdims=True)
    second = jnp.sum(kept * conv_out, axis=0, keepdims=True)
    return jnp.concatenate([first, second, meta_ref[0:1].astype(jnp.float32)], axis=1)


def write_sums(sums_ref, sums):
    for i in range(sums_ref.shape[0]):
        sums_ref[i] = sums


def total_of(stats_ref):
    parts = [stats_ref[i] for i in range(stats_ref.shape[0])]
    while len(parts) > 1:
        parts = [a + b for a, b in zip(parts[::2], parts[1::2], strict=True)]
    return parts[0]


def near_kernel(stats_ref, out_ref):
    write_sums(out_ref, total_of(stats_ref))


def scale_of(sums, gain, shift):
    total = sums[:, 2 * CH :]
    average = sums[:, :CH] / total
    variance = sums[:, CH : 2 * CH] / total - average * average
    scale = lax.rsqrt(variance + EPSILON) * gain
    return average, scale, shift


def affine(values, average, scale, shift):
    return (values - average) * scale + shift


def finish_kernel(meta_ref, second_ref, rows_ref, stats_ref, gain_ref, shift_ref, out_ref):
    stats = total_of(stats_ref)
    norm = scale_of(stats, gain_ref[...], shift_ref[...])
    summed = affine(second_ref[...], *norm) + rows_ref[...].astype(jnp.float32)
    out_ref[...] = (live_rows(meta_ref) * jnp.maximum(summed, 0.0)).astype(jnp.bfloat16)


def call(kernel, outs, scratch, limit, *args, hbm=False):
    vmem = pl.BlockSpec(memory_space=pltpu.VMEM)
    if hbm:
        args = [pltpu.with_memory_space_constraint(a, pltpu.HBM) for a in args]
    return pl.pallas_call(
        kernel,
        out_shape=outs,
        in_specs=[pl.BlockSpec(memory_space=pltpu.HBM) if hbm else vmem] * len(args),
        out_specs=jax.tree.map(lambda _: vmem, outs),
        scratch_shapes=scratch,
        compiler_params=pltpu.CompilerParams(vmem_limit_bytes=limit << 20),
    )(*args)


def conv_scratch():
    padded = -(-SIDES * SLOTS // CH) * CH
    return [
        pltpu.VMEM((SIDES * SLOTS, ROWS), jnp.bfloat16),
        pltpu.VMEM((ROWS, padded), jnp.bfloat16),
        pltpu.VMEM((padded, 2 * CH), jnp.bfloat16),
    ]


def slab_neighbours(to_low, to_high):
    count = lax.axis_size(SLAB)
    even = lax.axis_index("slab_2") == 0
    across = [(i, i + 1) for i in range(1, count - 1, 2)] + [(i + 1, i) for i in range(1, count - 1, 2)]
    far = lax.ppermute(jnp.where(even, to_low, to_high), SLAB, across)
    both = lax.all_gather(jnp.where(even, to_high, to_low), "slab_2")
    return jnp.where(even, far, both[0]), jnp.where(even, both[1], far)


def tile_neighbours(to_low, to_high):
    count = lax.axis_size("tile")
    even = lax.axis_index("tile") % 2 == 0
    inner = [(i, i ^ 1) for i in range(count)]
    outer = [(i, i + 1) for i in range(1, count - 1, 2)] + [(i + 1, i) for i in range(1, count - 1, 2)]
    one = lax.ppermute(jnp.where(even, to_high, to_low), "tile", inner)
    two = lax.ppermute(jnp.where(even, to_low, to_high), "tile", outer)
    return jnp.where(even, two, one), jnp.where(even, one, two)


def reduce_all(sums):
    near = lax.all_to_all(sums, ("slab_1", "slab_2"), 0, 0)
    far = lax.axis_size(("slab_0", "tile"))
    block = call(near_kernel, jax.ShapeDtypeStruct((far, 1, 3 * CH), jnp.float32), [], 4, near)
    return lax.all_to_all(block, ("slab_0", "tile"), 0, 0)


def per_device(
    features, counts, rulebook, face_rows, conv_one, gain_one, shift_one, conv_two, gain_two, shift_two
):
    del counts
    f32, bf16, i32 = jnp.float32, jnp.bfloat16, jnp.int32
    shaped = jax.ShapeDtypeStruct
    ext, message, big = shaped((EXT, CH), f32), shaped((2 * SIDE_ROWS, CH), bf16), shaped((ROWS, CH), f32)
    small = shaped((8, 1, 3 * CH), f32)
    params = (conv_two, gain_one[None], shift_one[None], gain_two[None], shift_two[None])
    outs = (
        ext, message, message,
        shaped((32, ROWS), i32), shaped((ROWS, CH), i32), shaped((CH, ROWS), bf16), shaped((8, CH), i32),
        shaped((ROWS, CH), bf16), shaped((4, FACE), i32), *(shaped(p.shape, p.dtype) for p in params),
    )
    scratch = [
        pltpu.VMEM((TAPS, 1, ROWS), i32), pltpu.VMEM((TAPS, CH, CH), bf16), pltpu.VMEM((32, ROWS), i32),
        *conv_scratch(), pltpu.SemaphoreType.DMA((9,)),
    ]
    taps = rulebook.reshape(TAPS, 1, ROWS)
    first, up, down, *plan, meta, rows, faces, weight_two, gain_one, shift_one, gain_two, shift_two = call(
        spread_kernel, outs, scratch, 24, taps, features[0, 0], conv_one, face_rows[0, 0], *params, hbm=True
    )
    total = SIDES * SLOTS
    outs = (shaped((total, ROWS), bf16), shaped((total, CH), i32))
    received = tile_neighbours(down, up)
    source = call(source_kernel, outs, conv_scratch()[:1], 8, plan[0], plan[2])
    first, left, right = call(tile_kernel, (ext, message, message), [], 8, first, *received, faces)
    received = slab_neighbours(left, right)
    first, sums = call(slab_kernel, (ext, small), [], 8, meta, first, *received, faces)
    stats = reduce_all(sums)
    second, sums = call(
        gather_kernel, (big, small), [pltpu.VMEM((ROWS, 2 * CH), bf16), *conv_scratch()], 24,
        meta, first, *plan, *source, weight_two, stats, gain_one, shift_one,
    )
    stats = reduce_all(sums)
    out = call(
        finish_kernel, shaped((ROWS, CH), bf16), [], 4, meta, second, rows, stats, gain_two, shift_two
    )
    return out[None, None]


def solution(mesh):
    tiles = mesh.shape["tile"]
    torus = Mesh(
        mesh.devices.reshape(-1, 4, 2, tiles), ("slab_0", "slab_1", "slab_2", "tile")
    )
    split = P(SLAB, "tile", None, None)
    in_specs = (split, P(SLAB, "tile"), split, split, P(), P(), P(), P(), P(), P())
    return jax.shard_map(
        per_device, mesh=torus, in_specs=in_specs, out_specs=split, check_vma=False
    )
```

```python
import jax
import jax.numpy as jnp
from jax import lax
from jax.experimental import pallas as pl
from jax.experimental.pallas import tpu as pltpu
from jax.sharding import Mesh
from jax.sharding import PartitionSpec as P

ROWS = 512
CH = 128
TAPS = 27
SIDES = 26
CENTRE = 13
SLOTS = 24
DIGIT = 32
TABLE = 800
FACE = 64
COLUMN = 8
SIDE_ROWS = FACE + 2 * COLUMN
HALO = 2 * FACE + 2 * SIDE_ROWS
EXT = 832
SLAB = ("slab_0", "slab_1", "slab_2")
EPSILON = 1e-05


A, B, QH, QL = ROWS, ROWS + FACE, ROWS + 2 * FACE, ROWS + 2 * FACE + SIDE_ROWS


def dot(a, b, **kw):
    return jnp.dot(a, b, preferred_element_type=jnp.float32, **kw)


def hot(index, shape, dim):
    return jnp.where(jnp.broadcast_to(index, shape) == lax.broadcasted_iota(jnp.int32, shape, dim), 1.0, 0.0).astype(
        jnp.bfloat16
    )


def fetch(pairs, sems):
    copies = [pltpu.make_async_copy(src, dst, sems.at[i]) for i, (src, dst) in enumerate(pairs)]
    for copy in copies:
        copy.start()
    return copies


def face_hot(faces_ref, k):
    return hot(jnp.concatenate([faces_ref[k : k + 1, :], faces_ref[k + 1 : k + 2, :]], axis=1), (ROWS, 2 * FACE), 0)


def pick(selector, rows):
    return lax.dot_general(
        selector, rows.astype(jnp.bfloat16), (((0,), (0,)), ((), ())), preferred_element_type=jnp.float32
    )


def put(selector, values):
    return dot(selector, jnp.concatenate(values, axis=0).astype(jnp.bfloat16))


def plan_pairs(rb_ref, work_ref, rank_ref, rank_t_ref, digits_ref):
    work_ref[...] = jnp.full_like(work_ref, TABLE)
    for t in range(SIDES):
        work_ref[t : t + 1, :] = rb_ref[t + (t >= CENTRE)]
    entry = work_ref[...]
    present = entry != TABLE
    ones = jnp.where(present, 1.0, 0.0)
    before = lax.broadcasted_iota(jnp.int32, (ROWS, ROWS), 0) < lax.broadcasted_iota(jnp.int32, (ROWS, ROWS), 1)
    place = dot(ones.astype(jnp.bfloat16), jnp.where(before, 1.0, 0.0).astype(jnp.bfloat16))
    rank = jnp.where(present, place.astype(jnp.int32), -1)
    rank_ref[...] = rank
    itself = jnp.broadcast_to(jnp.where(rb_ref[CENTRE] != TABLE, 1, -1), (8, ROWS))
    padded = jnp.concatenate([rank, itself, jnp.full((CH - 40, ROWS), -1, jnp.int32)], axis=0)
    rank_t_ref[...] = padded.T
    digits_ref[...] = jnp.concatenate(
        [(entry // DIGIT).astype(jnp.float32), (entry % DIGIT).astype(jnp.float32),
         jnp.zeros((CH - 2 * entry.shape[0], ROWS), jnp.float32)], axis=0
    ).astype(jnp.bfloat16)
    most = jnp.max(jnp.sum(ones, axis=1, keepdims=True))
    return (most.astype(jnp.int32) + (SLOTS - 1)) // SLOTS


def slots_of_rows(rank_ref, base, to_slot_ref):
    slot = lax.broadcasted_iota(jnp.int32, (SLOTS, ROWS), 0) + base
    blocks = []
    for t in range(SIDES):
        match = jnp.broadcast_to(rank_ref[t : t + 1, :], (SLOTS, ROWS)) == slot
        blocks.append(jnp.where(match, 1.0, 0.0))
    to_slot_ref[...] = jnp.concatenate(blocks, axis=0).astype(jnp.bfloat16)


def tap_of_slot(slot):
    return jnp.right_shift(slot * 2731, 16)


def rows_of_slots(rank_t_ref, base, to_row_ref):
    for i in range(to_row_ref.shape[1] // CH):
        slot = lax.broadcasted_iota(jnp.int32, (1, CH), 1) + i * CH
        tap = tap_of_slot(slot)
        wanted = jnp.broadcast_to(slot - tap * SLOTS + base, (ROWS, CH))
        spread = jnp.take_along_axis(
            rank_t_ref[...], jnp.broadcast_to(tap, (ROWS, CH)), axis=1, mode="promise_in_bounds"
        )
        to_row_ref[:, i * CH : (i + 1) * CH] = jnp.where(spread == wanted, 1.0, 0.0).astype(jnp.bfloat16)


def multiply_slots(picked, weight_ref, tap_of, part_ref):
    parts = []
    for t in range(0, SIDES, 2):
        both = jnp.concatenate([weight_ref[tap_of(t)], weight_ref[tap_of(t + 1)]], axis=1)
        got = dot(picked[t * SLOTS : (t + 2) * SLOTS].astype(jnp.bfloat16), both)
        parts += [got[:SLOTS, :CH], got[SLOTS:, CH:]]
    part = jnp.concatenate(parts, axis=0)
    high = part.astype(jnp.bfloat16)
    part_ref[: SIDES * SLOTS, :CH] = high
    part_ref[: SIDES * SLOTS, CH:] = (part - high.astype(jnp.float32)).astype(jnp.bfloat16)


def clear_padding(part_ref):
    part_ref[SIDES * SLOTS :, :] = jnp.zeros((part_ref.shape[0] - SIDES * SLOTS, 2 * CH), jnp.bfloat16)


def spread_kernel(*refs):
    rb_hbm, rows_hbm, weight_hbm, faces_hbm, *params_hbm = refs[:9]
    out_ref, up_ref, down_ref, rank_ref, rank_t_ref, digits_ref, meta_ref, rows_ref, faces_ref, *params = refs[9:23]
    rb_ref, weight_ref, work_ref, to_slot_ref, to_row_ref, part_ref, sems = refs[23:]
    rb_copy, rows_copy, weight_copy, *others = fetch(
        [(rb_hbm, rb_ref), (rows_hbm, rows_ref), (weight_hbm, weight_ref), (faces_hbm, faces_ref),
         *zip(params_hbm, params, strict=True)], sems,
    )
    rb_copy.wait()
    chunks = plan_pairs(rb_ref, work_ref, rank_ref, rank_t_ref, digits_ref)
    present = jnp.where(rb_ref[CENTRE] != TABLE, 1.0, 0.0)
    meta_ref[0:1] = jnp.broadcast_to(jnp.sum(present, axis=1, keepdims=True), (1, CH)).astype(jnp.int32)
    meta_ref[1:2] = jnp.full((1, CH), chunks, jnp.int32)
    clear_padding(part_ref)
    rows_copy.wait()
    weight_copy.wait()
    itself = jnp.broadcast_to(rank_t_ref[:, 32:33], (ROWS, CH)) > 0
    out_ref[:ROWS] = jnp.where(itself, dot(rows_ref[...], weight_ref[CENTRE]), 0.0)
    out_ref[ROWS:] = jnp.zeros((EXT - ROWS, CH), jnp.float32)
    slots = part_ref.shape[0]

    def chunk(c, carry):
        slots_of_rows(rank_ref, c * SLOTS, to_slot_ref)
        picked = dot(to_slot_ref[...], rows_ref[...])
        multiply_slots(picked, weight_ref, lambda t: TAPS - 1 - (t + (t >= CENTRE)), part_ref)
        rows_of_slots(rank_t_ref, c * SLOTS, to_row_ref)
        found = dot(digits_ref[...], to_row_ref[...])
        digit = lax.broadcasted_iota(jnp.int32, (CH, slots), 0)
        tap = jnp.broadcast_to(tap_of_slot(lax.broadcasted_iota(jnp.int32, (1, slots), 1)), (CH, slots))
        worth = jnp.where(digit == tap, float(DIGIT), jnp.where(digit == tap + 32, 1.0, 0.0))
        target = jnp.sum(found * worth, axis=0, keepdims=True).astype(jnp.int32)
        added = dot(hot(target, (EXT, slots), 0), part_ref[...])
        out_ref[...] += added[:, :CH] + added[:, CH:]
        return carry

    lax.fori_loop(0, chunks, chunk, 0)
    for copy in others:
        copy.wait()
    picked = pick(face_hot(faces_ref, 2), out_ref[:ROWS])
    for ref, own, at, far in ((down_ref, picked[:FACE], 0, QH), (up_ref, picked[FACE:], FACE - COLUMN, QL)):
        pieces = [out_ref[A + at : A + at + COLUMN], own, out_ref[B + at : B + at + COLUMN]]
        ref[...] = jnp.concatenate([*pieces, out_ref[far : far + SIDE_ROWS]], axis=0).astype(jnp.bfloat16)


def tile_kernel(sums_ref, low_ref, high_ref, slab_ref, tile_ref, out_ref, left_ref, right_ref):
    out_ref[...] = sums_ref[...]
    first, last = SIDE_ROWS + COLUMN, SIDE_ROWS + COLUMN + FACE
    low, high = low_ref[...].astype(jnp.float32), high_ref[...].astype(jnp.float32)
    out_ref[QH:QL] += low[:SIDE_ROWS]
    out_ref[QL : QL + SIDE_ROWS] += high[:SIDE_ROWS]
    for sent, at in ((low, 0), (high, FACE - COLUMN)):
        out_ref[A + at : A + at + COLUMN] += sent[SIDE_ROWS:first]
        out_ref[B + at : B + at + COLUMN] += sent[last:]
    out_ref[:ROWS] += put(tile_ref[...], [low[first:last], high[first:last]])
    picked = pick(slab_ref[...], out_ref[:ROWS])
    for ref, own, own_at, far, far_at in (
        (left_ref, picked[:FACE], COLUMN, A, 0),
        (right_ref, picked[FACE:], FACE, B, FACE + COLUMN),
    ):
        pieces = []
        for face, at in ((own, own_at), (out_ref[far : far + FACE], far_at)):
            pieces += [face, out_ref[QH + at : QH + at + COLUMN], out_ref[QL + at : QL + at + COLUMN]]
        ref[...] = jnp.concatenate(pieces, axis=0).astype(jnp.bfloat16)


def slab_kernel(meta_ref, sums_ref, low_ref, high_ref, slab_ref, out_ref, stats_ref):
    out_ref[...] = sums_ref[...]
    low, high = low_ref[...].astype(jnp.float32), high_ref[...].astype(jnp.float32)
    for sent, far, far_at, own_at in ((low, A, 0, COLUMN), (high, B, FACE + COLUMN, FACE)):
        out_ref[far : far + FACE] += sent[:FACE]
        for start, at in ((0, far_at), (SIDE_ROWS, own_at)):
            out_ref[QH + at : QH + at + COLUMN] += sent[start + FACE : start + FACE + COLUMN]
            out_ref[QL + at : QL + at + COLUMN] += sent[start + FACE + COLUMN : start + SIDE_ROWS]
    own = slice(SIDE_ROWS, SIDE_ROWS + FACE)
    total = out_ref[:ROWS] + put(slab_ref[...], [low[own], high[own]])
    out_ref[:ROWS] = total
    write_sums(stats_ref, sums_of(total, meta_ref))


def sources(c, rank_ref, digits_ref, to_slot_ref):
    total = SIDES * SLOTS
    slots_of_rows(rank_ref, c * SLOTS, to_slot_ref)
    found = lax.dot_general(
        to_slot_ref[...], digits_ref[...], (((1,), (1,)), ((), ())), preferred_element_type=jnp.float32
    )
    tap = tap_of_slot(lax.broadcasted_iota(jnp.int32, (total, CH), 0))
    lane = lax.broadcasted_iota(jnp.int32, (total, CH), 1)
    worth = jnp.where(lane == tap, float(DIGIT), jnp.where(lane == tap + 32, 1.0, 0.0))
    source = jnp.sum(found * worth, axis=1, keepdims=True).astype(jnp.int32)
    return hot(jnp.bitwise_and(source, ROWS - 1), (total, ROWS), 1), jnp.broadcast_to(source, (total, CH))


def source_kernel(rank_ref, digits_ref, faces_ref, hot_ref, source_ref, slab_ref, tile_ref, to_slot_ref):
    hot_ref[...], source_ref[...] = sources(0, rank_ref, digits_ref, to_slot_ref)
    slab_ref[...], tile_ref[...] = face_hot(faces_ref, 0), face_hot(faces_ref, 2)


def gather_kernel(
    meta_ref, first_ref, rank_ref, rank_t_ref, digits_ref, hot_ref, source_ref, weight_ref, stats_ref, gain_ref, shift_ref,
    out_ref, sums_ref, table_ref, to_slot_ref, to_row_ref, part_ref,
):
    norm = scale_of(total_of(stats_ref), gain_ref[...], shift_ref[...])
    live = live_rows(meta_ref)

    def act(values):
        return jnp.maximum(affine(values, *norm), 0.0)

    table_ref[:, :CH] = (live * act(first_ref[:ROWS])).astype(jnp.bfloat16)
    table_ref[:HALO, CH:] = act(first_ref[ROWS : ROWS + HALO]).astype(jnp.bfloat16)
    table_ref[HALO:, CH:] = jnp.zeros((ROWS - HALO, CH), jnp.bfloat16)
    out_ref[...] = dot(table_ref[:, :CH], weight_ref[CENTRE]) * live
    clear_padding(part_ref)

    def add(c, selector, source):
        both = dot(selector, table_ref[...])
        picked = jnp.where(source >= ROWS, both[:, CH:], both[:, :CH])
        multiply_slots(picked, weight_ref, lambda t: t + (t >= CENTRE), part_ref)
        rows_of_slots(rank_t_ref, c * SLOTS, to_row_ref)
        added = dot(to_row_ref[...], part_ref[...])
        out_ref[...] += added[:, :CH] + added[:, CH:]

    def chunk(c, carry):
        add(c, *sources(c, rank_ref, digits_ref, to_slot_ref))
        return carry

    add(0, hot_ref[...], source_ref[...])
    lax.fori_loop(1, jnp.max(meta_ref[1:2]), chunk, 0)
    write_sums(sums_ref, sums_of(out_ref[...], meta_ref))


def live_rows(meta_ref):
    rows = lax.broadcasted_iota(jnp.int32, (ROWS, CH), 0)
    return jnp.where(rows < jnp.broadcast_to(meta_ref[0:1], (ROWS, CH)), 1.0, 0.0)


def sums_of(conv_out, meta_ref):
    kept = conv_out * live_rows(meta_ref)
    first = jnp.sum(kept, axis=0, keepdims=True)
    second = jnp.sum(kept * conv_out, axis=0, keepdims=True)
    return jnp.concatenate([first, second, meta_ref[0:1].astype(jnp.float32)], axis=1)


def write_sums(sums_ref, sums):
    for i in range(sums_ref.shape[0]):
        sums_ref[i] = sums


def total_of(stats_ref):
    parts = [stats_ref[i] for i in range(stats_ref.shape[0])]
    while len(parts) > 1:
        parts = [a + b for a, b in zip(parts[::2], parts[1::2], strict=True)]
    return parts[0]


def near_kernel(stats_ref, out_ref):
    write_sums(out_ref, total_of(stats_ref))


def scale_of(sums, gain, shift):
    total = sums[:, 2 * CH :]
    average = sums[:, :CH] / total
    variance = sums[:, CH : 2 * CH] / total - average * average
    scale = lax.rsqrt(variance + EPSILON) * gain
    return average, scale, shift


def affine(values, average, scale, shift):
    return (values - average) * scale + shift


def finish_kernel(meta_ref, second_ref, rows_ref, stats_ref, gain_ref, shift_ref, out_ref):
    stats = total_of(stats_ref)
    norm = scale_of(stats, gain_ref[...], shift_ref[...])
    summed = affine(second_ref[...], *norm) + rows_ref[...].astype(jnp.float32)
    out_ref[...] = (live_rows(meta_ref) * jnp.maximum(summed, 0.0)).astype(jnp.bfloat16)


def call(kernel, outs, scratch, limit, *args, hbm=False):
    vmem = pl.BlockSpec(memory_space=pltpu.VMEM)
    if hbm:
        args = [pltpu.with_memory_space_constraint(a, pltpu.HBM) for a in args]
    return pl.pallas_call(
        kernel,
        out_shape=outs,
        in_specs=[pl.BlockSpec(memory_space=pltpu.HBM) if hbm else vmem] * len(args),
        out_specs=jax.tree.map(lambda _: vmem, outs),
        scratch_shapes=scratch,
        compiler_params=pltpu.CompilerParams(vmem_limit_bytes=limit << 20),
    )(*args)


def conv_scratch():
    padded = -(-SIDES * SLOTS // CH) * CH
    return [
        pltpu.VMEM((SIDES * SLOTS, ROWS), jnp.bfloat16),
        pltpu.VMEM((ROWS, padded), jnp.bfloat16),
        pltpu.VMEM((padded, 2 * CH), jnp.bfloat16),
    ]


def slab_neighbours(to_low, to_high):
    count = lax.axis_size(SLAB)
    even = lax.axis_index("slab_2") == 0
    across = [(i, i + 1) for i in range(1, count - 1, 2)] + [(i + 1, i) for i in range(1, count - 1, 2)]
    far = lax.ppermute(jnp.where(even, to_low, to_high), SLAB, across)
    both = lax.all_gather(jnp.where(even, to_high, to_low), "slab_2")
    return jnp.where(even, far, both[0]), jnp.where(even, both[1], far)


def tile_neighbours(to_low, to_high):
    count = lax.axis_size("tile")
    even = lax.axis_index("tile") % 2 == 0
    inner = [(i, i ^ 1) for i in range(count)]
    outer = [(i, i + 1) for i in range(1, count - 1, 2)] + [(i + 1, i) for i in range(1, count - 1, 2)]
    one = lax.ppermute(jnp.where(even, to_high, to_low), "tile", inner)
    two = lax.ppermute(jnp.where(even, to_low, to_high), "tile", outer)
    return jnp.where(even, two, one), jnp.where(even, one, two)


def reduce_all(sums):
    near = lax.all_to_all(sums, ("slab_1", "slab_2"), 0, 0)
    far = lax.axis_size(("slab_0", "tile"))
    block = call(near_kernel, jax.ShapeDtypeStruct((far, 1, 3 * CH), jnp.float32), [], 4, near)
    return lax.all_to_all(block, ("slab_0", "tile"), 0, 0)


def per_device(
    features, counts, rulebook, face_rows, conv_one, gain_one, shift_one, conv_two, gain_two, shift_two
):
    del counts
    f32, bf16, i32 = jnp.float32, jnp.bfloat16, jnp.int32
    shaped = jax.ShapeDtypeStruct
    ext, message, big = shaped((EXT, CH), f32), shaped((2 * SIDE_ROWS, CH), bf16), shaped((ROWS, CH), f32)
    small = shaped((8, 1, 3 * CH), f32)
    params = (conv_two, gain_one[None], shift_one[None], gain_two[None], shift_two[None])
    outs = (
        ext, message, message,
        shaped((32, ROWS), i32), shaped((ROWS, CH), i32), shaped((CH, ROWS), bf16), shaped((8, CH), i32),
        shaped((ROWS, CH), bf16), shaped((4, FACE), i32), *(shaped(p.shape, p.dtype) for p in params),
    )
    scratch = [
        pltpu.VMEM((TAPS, 1, ROWS), i32), pltpu.VMEM((TAPS, CH, CH), bf16), pltpu.VMEM((32, ROWS), i32),
        *conv_scratch(), pltpu.SemaphoreType.DMA((9,)),
    ]
    taps = rulebook.reshape(TAPS, 1, ROWS)
    first, up, down, *plan, meta, rows, faces, weight_two, gain_one, shift_one, gain_two, shift_two = call(
        spread_kernel, outs, scratch, 24, taps, features[0, 0], conv_one, face_rows[0, 0], *params, hbm=True
    )
    total = SIDES * SLOTS
    outs = (shaped((total, ROWS), bf16), shaped((total, CH), i32), *(shaped((ROWS, 2 * FACE), bf16),) * 2)
    received = tile_neighbours(down, up)
    *source, at_slab, at_tile = call(
        source_kernel, outs, conv_scratch()[:1], 8, plan[0], plan[2], faces
    )
    first, left, right = call(tile_kernel, (ext, message, message), [], 8, first, *received, at_slab, at_tile)
    received = slab_neighbours(left, right)
    first, sums = call(slab_kernel, (ext, small), [], 8, meta, first, *received, at_slab)
    stats = reduce_all(sums)
    second, sums = call(
        gather_kernel, (big, small), [pltpu.VMEM((ROWS, 2 * CH), bf16), *conv_scratch()], 24,
        meta, first, *plan, *source, weight_two, stats, gain_one, shift_one,
    )
    stats = reduce_all(sums)
    out = call(
        finish_kernel, shaped((ROWS, CH), bf16), [], 4, meta, second, rows, stats, gain_two, shift_two
    )
    return out[None, None]


def solution(mesh):
    tiles = mesh.shape["tile"]
    torus = Mesh(
        mesh.devices.reshape(-1, 4, 2, tiles), ("slab_0", "slab_1", "slab_2", "tile")
    )
    split = P(SLAB, "tile", None, None)
    in_specs = (split, P(SLAB, "tile"), split, split, P(), P(), P(), P(), P(), P())
    return jax.shard_map(
        per_device, mesh=torus, in_specs=in_specs, out_specs=split, check_vma=False
    )
```

```python
import jax
import jax.numpy as jnp
from jax import lax
from jax.experimental import pallas as pl
from jax.experimental.pallas import tpu as pltpu
from jax.sharding import Mesh
from jax.sharding import PartitionSpec as P

ROWS = 512
CH = 128
TAPS = 27
SIDES = 26
CENTRE = 13
SLOTS = 24
DIGIT = 32
TABLE = 800
FACE = 64
COLUMN = 8
SIDE_ROWS = FACE + 2 * COLUMN
HALO = 2 * FACE + 2 * SIDE_ROWS
EXT = 832
SLAB = ("slab_0", "slab_1", "slab_2")
EPSILON = 1e-05


A, B, QH, QL = ROWS, ROWS + FACE, ROWS + 2 * FACE, ROWS + 2 * FACE + SIDE_ROWS


def dot(a, b, **kw):
    return jnp.dot(a, b, preferred_element_type=jnp.float32, **kw)


def hot(index, shape, dim):
    return jnp.where(jnp.broadcast_to(index, shape) == lax.broadcasted_iota(jnp.int32, shape, dim), 1.0, 0.0).astype(
        jnp.bfloat16
    )


def fetch(pairs, sems):
    copies = [pltpu.make_async_copy(src, dst, sems.at[i]) for i, (src, dst) in enumerate(pairs)]
    for copy in copies:
        copy.start()
    return copies


def face_hot(faces_ref, k):
    return hot(jnp.concatenate([faces_ref[k : k + 1, :], faces_ref[k + 1 : k + 2, :]], axis=1), (ROWS, 2 * FACE), 0)


def pick(selector, rows):
    return lax.dot_general(
        selector, rows.astype(jnp.bfloat16), (((0,), (0,)), ((), ())), preferred_element_type=jnp.float32
    )


def put(selector, values):
    return dot(selector, jnp.concatenate(values, axis=0).astype(jnp.bfloat16))


def plan_pairs(rb_ref, work_ref, rank_ref, rank_t_ref, digits_ref):
    work_ref[...] = jnp.full_like(work_ref, TABLE)
    for t in range(SIDES):
        work_ref[t : t + 1, :] = rb_ref[t + (t >= CENTRE)]
    entry = work_ref[...]
    present = entry != TABLE
    ones = jnp.where(present, 1.0, 0.0)
    before = lax.broadcasted_iota(jnp.int32, (ROWS, ROWS), 0) < lax.broadcasted_iota(jnp.int32, (ROWS, ROWS), 1)
    place = dot(ones.astype(jnp.bfloat16), jnp.where(before, 1.0, 0.0).astype(jnp.bfloat16))
    rank = jnp.where(present, place.astype(jnp.int32), -1)
    rank_ref[...] = rank
    itself = jnp.broadcast_to(jnp.where(rb_ref[CENTRE] != TABLE, 1, -1), (8, ROWS))
    padded = jnp.concatenate([rank, itself, jnp.full((CH - 40, ROWS), -1, jnp.int32)], axis=0)
    rank_t_ref[...] = padded.T
    digits_ref[...] = jnp.concatenate(
        [(entry // DIGIT).astype(jnp.float32), (entry % DIGIT).astype(jnp.float32),
         jnp.zeros((CH - 2 * entry.shape[0], ROWS), jnp.float32)], axis=0
    ).astype(jnp.bfloat16)
    most = jnp.max(jnp.sum(ones, axis=1, keepdims=True))
    return (most.astype(jnp.int32) + (SLOTS - 1)) // SLOTS


def slots_of_rows(rank_ref, base, to_slot_ref):
    slot = lax.broadcasted_iota(jnp.int32, (SLOTS, ROWS), 0) + base
    blocks = []
    for t in range(SIDES):
        match = jnp.broadcast_to(rank_ref[t : t + 1, :], (SLOTS, ROWS)) == slot
        blocks.append(jnp.where(match, 1.0, 0.0))
    to_slot_ref[...] = jnp.concatenate(blocks, axis=0).astype(jnp.bfloat16)


def tap_of_slot(slot):
    return jnp.right_shift(slot * 2731, 16)


def rows_of_slots(rank_t_ref, base, to_row_ref):
    for i in range(to_row_ref.shape[1] // CH):
        slot = lax.broadcasted_iota(jnp.int32, (1, CH), 1) + i * CH
        tap = tap_of_slot(slot)
        wanted = jnp.broadcast_to(slot - tap * SLOTS + base, (ROWS, CH))
        spread = jnp.take_along_axis(
            rank_t_ref[...], jnp.broadcast_to(tap, (ROWS, CH)), axis=1, mode="promise_in_bounds"
        )
        to_row_ref[:, i * CH : (i + 1) * CH] = jnp.where(spread == wanted, 1.0, 0.0).astype(jnp.bfloat16)


def multiply_slots(picked, weight_ref, tap_of, part_ref):
    parts = []
    for t in range(0, SIDES, 2):
        both = jnp.concatenate([weight_ref[tap_of(t)], weight_ref[tap_of(t + 1)]], axis=1)
        got = dot(picked[t * SLOTS : (t + 2) * SLOTS].astype(jnp.bfloat16), both)
        parts += [got[:SLOTS, :CH], got[SLOTS:, CH:]]
    part = jnp.concatenate(parts, axis=0)
    high = part.astype(jnp.bfloat16)
    part_ref[: SIDES * SLOTS, :CH] = high
    part_ref[: SIDES * SLOTS, CH:] = (part - high.astype(jnp.float32)).astype(jnp.bfloat16)


def clear_padding(part_ref):
    part_ref[SIDES * SLOTS :, :] = jnp.zeros((part_ref.shape[0] - SIDES * SLOTS, 2 * CH), jnp.bfloat16)


def spread_kernel(*refs):
    rb_hbm, rows_hbm, weight_hbm, faces_hbm, *params_hbm = refs[:9]
    out_ref, up_ref, down_ref, rank_ref, rank_t_ref, digits_ref, meta_ref, rows_ref, faces_ref, *params = refs[9:23]
    rb_ref, weight_ref, work_ref, to_slot_ref, to_row_ref, part_ref, sems = refs[23:]
    rb_copy, rows_copy, weight_copy, *others = fetch(
        [(rb_hbm, rb_ref), (rows_hbm, rows_ref), (weight_hbm, weight_ref), (faces_hbm, faces_ref),
         *zip(params_hbm, params, strict=True)], sems,
    )
    rb_copy.wait()
    chunks = plan_pairs(rb_ref, work_ref, rank_ref, rank_t_ref, digits_ref)
    present = jnp.where(rb_ref[CENTRE] != TABLE, 1.0, 0.0)
    meta_ref[0:1] = jnp.broadcast_to(jnp.sum(present, axis=1, keepdims=True), (1, CH)).astype(jnp.int32)
    meta_ref[1:2] = jnp.full((1, CH), chunks, jnp.int32)
    clear_padding(part_ref)
    rows_copy.wait()
    weight_copy.wait()
    itself = jnp.broadcast_to(rank_t_ref[:, 32:33], (ROWS, CH)) > 0
    out_ref[:ROWS] = jnp.where(itself, dot(rows_ref[...], weight_ref[CENTRE]), 0.0)
    out_ref[ROWS:] = jnp.zeros((EXT - ROWS, CH), jnp.float32)
    slots = part_ref.shape[0]

    def chunk(c, carry):
        slots_of_rows(rank_ref, c * SLOTS, to_slot_ref)
        picked = dot(to_slot_ref[...], rows_ref[...])
        multiply_slots(picked, weight_ref, lambda t: TAPS - 1 - (t + (t >= CENTRE)), part_ref)
        rows_of_slots(rank_t_ref, c * SLOTS, to_row_ref)
        found = dot(digits_ref[...], to_row_ref[...])
        digit = lax.broadcasted_iota(jnp.int32, (CH, slots), 0)
        tap = jnp.broadcast_to(tap_of_slot(lax.broadcasted_iota(jnp.int32, (1, slots), 1)), (CH, slots))
        worth = jnp.where(digit == tap, float(DIGIT), jnp.where(digit == tap + 32, 1.0, 0.0))
        target = jnp.sum(found * worth, axis=0, keepdims=True).astype(jnp.int32)
        added = dot(hot(target, (EXT, slots), 0), part_ref[...])
        out_ref[...] += added[:, :CH] + added[:, CH:]
        return carry

    lax.fori_loop(0, chunks, chunk, 0)
    for copy in others:
        copy.wait()
    picked = pick(face_hot(faces_ref, 2), out_ref[:ROWS])
    for ref, own, at, far in ((down_ref, picked[:FACE], 0, QH), (up_ref, picked[FACE:], FACE - COLUMN, QL)):
        pieces = [out_ref[A + at : A + at + COLUMN], own, out_ref[B + at : B + at + COLUMN]]
        ref[...] = jnp.concatenate([*pieces, out_ref[far : far + SIDE_ROWS]], axis=0).astype(jnp.bfloat16)


def tile_kernel(sums_ref, low_ref, high_ref, slab_ref, tile_ref, out_ref, left_ref, right_ref):
    out_ref[...] = sums_ref[...]
    first, last = SIDE_ROWS + COLUMN, SIDE_ROWS + COLUMN + FACE
    low, high = low_ref[...].astype(jnp.float32), high_ref[...].astype(jnp.float32)
    out_ref[QH:QL] += low[:SIDE_ROWS]
    out_ref[QL : QL + SIDE_ROWS] += high[:SIDE_ROWS]
    for sent, at in ((low, 0), (high, FACE - COLUMN)):
        out_ref[A + at : A + at + COLUMN] += sent[SIDE_ROWS:first]
        out_ref[B + at : B + at + COLUMN] += sent[last:]
    out_ref[:ROWS] += put(tile_ref[...], [low[first:last], high[first:last]])
    picked = pick(slab_ref[...], out_ref[:ROWS])
    for ref, own, own_at, far, far_at in (
        (left_ref, picked[:FACE], COLUMN, A, 0),
        (right_ref, picked[FACE:], FACE, B, FACE + COLUMN),
    ):
        pieces = []
        for face, at in ((own, own_at), (out_ref[far : far + FACE], far_at)):
            pieces += [face, out_ref[QH + at : QH + at + COLUMN], out_ref[QL + at : QL + at + COLUMN]]
        ref[...] = jnp.concatenate(pieces, axis=0).astype(jnp.bfloat16)


def slab_kernel(meta_ref, sums_ref, low_ref, high_ref, slab_ref, out_ref, stats_ref):
    out_ref[...] = sums_ref[...]
    low, high = low_ref[...].astype(jnp.float32), high_ref[...].astype(jnp.float32)
    for sent, far, far_at, own_at in ((low, A, 0, COLUMN), (high, B, FACE + COLUMN, FACE)):
        out_ref[far : far + FACE] += sent[:FACE]
        for start, at in ((0, far_at), (SIDE_ROWS, own_at)):
            out_ref[QH + at : QH + at + COLUMN] += sent[start + FACE : start + FACE + COLUMN]
            out_ref[QL + at : QL + at + COLUMN] += sent[start + FACE + COLUMN : start + SIDE_ROWS]
    own = slice(SIDE_ROWS, SIDE_ROWS + FACE)
    total = out_ref[:ROWS] + put(slab_ref[...], [low[own], high[own]])
    out_ref[:ROWS] = total
    write_sums(stats_ref, sums_of(total, meta_ref))


def sources(c, rank_ref, digits_ref, to_slot_ref):
    total = SIDES * SLOTS
    slots_of_rows(rank_ref, c * SLOTS, to_slot_ref)
    found = lax.dot_general(
        to_slot_ref[...], digits_ref[...], (((1,), (1,)), ((), ())), preferred_element_type=jnp.float32
    )
    tap = tap_of_slot(lax.broadcasted_iota(jnp.int32, (total, CH), 0))
    lane = lax.broadcasted_iota(jnp.int32, (total, CH), 1)
    worth = jnp.where(lane == tap, float(DIGIT), jnp.where(lane == tap + 32, 1.0, 0.0))
    source = jnp.sum(found * worth, axis=1, keepdims=True).astype(jnp.int32)
    return hot(jnp.bitwise_and(source, ROWS - 1), (total, ROWS), 1), jnp.broadcast_to(source, (total, CH))


def source_kernel(rank_ref, digits_ref, faces_ref, hot_ref, source_ref, slab_ref, tile_ref, to_slot_ref):
    hot_ref[...], source_ref[...] = sources(0, rank_ref, digits_ref, to_slot_ref)
    slab_ref[...], tile_ref[...] = face_hot(faces_ref, 0), face_hot(faces_ref, 2)


def gather_kernel(
    meta_ref, first_ref, rank_ref, rank_t_ref, digits_ref, hot_ref, source_ref, weight_ref, stats_ref, gain_ref, shift_ref,
    out_ref, sums_ref, table_ref, to_slot_ref, to_row_ref, part_ref,
):
    norm = scale_of(total_of(stats_ref), gain_ref[...], shift_ref[...])
    live = live_rows(meta_ref)

    def act(values):
        return jnp.maximum(affine(values, *norm), 0.0)

    table_ref[:, :CH] = (live * act(first_ref[:ROWS])).astype(jnp.bfloat16)
    table_ref[:HALO, CH:] = act(first_ref[ROWS : ROWS + HALO]).astype(jnp.bfloat16)
    table_ref[HALO:, CH:] = jnp.zeros((ROWS - HALO, CH), jnp.bfloat16)
    out_ref[...] = dot(table_ref[:, :CH], weight_ref[CENTRE]) * live
    clear_padding(part_ref)

    def add(c, selector, source):
        both = dot(selector, table_ref[...])
        picked = jnp.where(source >= ROWS, both[:, CH:], both[:, :CH])
        multiply_slots(picked, weight_ref, lambda t: t + (t >= CENTRE), part_ref)
        rows_of_slots(rank_t_ref, c * SLOTS, to_row_ref)
        added = dot(to_row_ref[...], part_ref[...])
        out_ref[...] += added[:, :CH] + added[:, CH:]

    def chunk(c, carry):
        add(c, *sources(c, rank_ref, digits_ref, to_slot_ref))
        return carry

    add(0, hot_ref[...], source_ref[...])
    lax.fori_loop(1, jnp.max(meta_ref[1:2]), chunk, 0)
    write_sums(sums_ref, sums_of(out_ref[...], meta_ref))


def live_rows(meta_ref):
    rows = lax.broadcasted_iota(jnp.int32, (ROWS, CH), 0)
    return jnp.where(rows < jnp.broadcast_to(meta_ref[0:1], (ROWS, CH)), 1.0, 0.0)


def sums_of(conv_out, meta_ref):
    kept = conv_out * live_rows(meta_ref)
    first = jnp.sum(kept, axis=0, keepdims=True)
    second = jnp.sum(kept * conv_out, axis=0, keepdims=True)
    return jnp.concatenate([first, second, meta_ref[0:1].astype(jnp.float32)], axis=1)


def write_sums(sums_ref, sums):
    for i in range(sums_ref.shape[0]):
        sums_ref[i] = sums


def total_of(stats_ref):
    parts = [stats_ref[i] for i in range(stats_ref.shape[0])]
    while len(parts) > 1:
        parts = [a + b for a, b in zip(parts[::2], parts[1::2], strict=True)]
    return parts[0]


def near_kernel(stats_ref, out_ref):
    write_sums(out_ref, total_of(stats_ref))


def scale_of(sums, gain, shift):
    total = sums[:, 2 * CH :]
    average = sums[:, :CH] / total
    variance = sums[:, CH : 2 * CH] / total - average * average
    scale = lax.rsqrt(variance + EPSILON) * gain
    return average, scale, shift


def affine(values, average, scale, shift):
    return (values - average) * scale + shift


def finish_kernel(meta_ref, second_ref, rows_ref, stats_ref, gain_ref, shift_ref, out_hbm, out_ref, sems):
    norm = scale_of(total_of(stats_ref), gain_ref[...], shift_ref[...])
    live = live_rows(meta_ref)
    size = ROWS // 4
    copies = []
    for i in range(4):
        at = slice(i * size, (i + 1) * size)
        summed = affine(second_ref[at], *norm) + rows_ref[at].astype(jnp.float32)
        out_ref[at] = (live[at] * jnp.maximum(summed, 0.0)).astype(jnp.bfloat16)
        copies += [pltpu.make_async_copy(out_ref.at[pl.ds(i * size, size)], out_hbm.at[pl.ds(i * size, size)], sems.at[i])]
        copies[-1].start()
    for copy in copies:
        copy.wait()


def call(kernel, outs, scratch, limit, *args, hbm=False, out_hbm=False):
    vmem = pl.BlockSpec(memory_space=pltpu.VMEM)
    if hbm:
        args = [pltpu.with_memory_space_constraint(a, pltpu.HBM) for a in args]
    return pl.pallas_call(
        kernel,
        out_shape=outs,
        in_specs=[pl.BlockSpec(memory_space=pltpu.HBM) if hbm else vmem] * len(args),
        out_specs=jax.tree.map(lambda _: pl.BlockSpec(memory_space=pltpu.HBM) if out_hbm else vmem, outs),
        scratch_shapes=scratch,
        compiler_params=pltpu.CompilerParams(vmem_limit_bytes=limit << 20),
    )(*args)


def conv_scratch():
    padded = -(-SIDES * SLOTS // CH) * CH
    return [
        pltpu.VMEM((SIDES * SLOTS, ROWS), jnp.bfloat16),
        pltpu.VMEM((ROWS, padded), jnp.bfloat16),
        pltpu.VMEM((padded, 2 * CH), jnp.bfloat16),
    ]


def slab_neighbours(to_low, to_high):
    count = lax.axis_size(SLAB)
    even = lax.axis_index("slab_2") == 0
    across = [(i, i + 1) for i in range(1, count - 1, 2)] + [(i + 1, i) for i in range(1, count - 1, 2)]
    far = lax.ppermute(jnp.where(even, to_low, to_high), SLAB, across)
    both = lax.all_gather(jnp.where(even, to_high, to_low), "slab_2")
    return jnp.where(even, far, both[0]), jnp.where(even, both[1], far)


def tile_neighbours(to_low, to_high):
    count = lax.axis_size("tile")
    even = lax.axis_index("tile") % 2 == 0
    inner = [(i, i ^ 1) for i in range(count)]
    outer = [(i, i + 1) for i in range(1, count - 1, 2)] + [(i + 1, i) for i in range(1, count - 1, 2)]
    one = lax.ppermute(jnp.where(even, to_high, to_low), "tile", inner)
    two = lax.ppermute(jnp.where(even, to_low, to_high), "tile", outer)
    return jnp.where(even, two, one), jnp.where(even, one, two)


def reduce_all(sums):
    near = lax.all_to_all(sums, ("slab_1", "slab_2"), 0, 0)
    far = lax.axis_size(("slab_0", "tile"))
    block = call(near_kernel, jax.ShapeDtypeStruct((far, 1, 3 * CH), jnp.float32), [], 4, near)
    return lax.all_to_all(block, ("slab_0", "tile"), 0, 0)


def per_device(
    features, counts, rulebook, face_rows, conv_one, gain_one, shift_one, conv_two, gain_two, shift_two
):
    del counts
    f32, bf16, i32 = jnp.float32, jnp.bfloat16, jnp.int32
    shaped = jax.ShapeDtypeStruct
    ext, message, big = shaped((EXT, CH), f32), shaped((2 * SIDE_ROWS, CH), bf16), shaped((ROWS, CH), f32)
    small = shaped((8, 1, 3 * CH), f32)
    params = (conv_two, gain_one[None], shift_one[None], gain_two[None], shift_two[None])
    outs = (
        ext, message, message,
        shaped((32, ROWS), i32), shaped((ROWS, CH), i32), shaped((CH, ROWS), bf16), shaped((8, CH), i32),
        shaped((ROWS, CH), bf16), shaped((4, FACE), i32), *(shaped(p.shape, p.dtype) for p in params),
    )
    scratch = [
        pltpu.VMEM((TAPS, 1, ROWS), i32), pltpu.VMEM((TAPS, CH, CH), bf16), pltpu.VMEM((32, ROWS), i32),
        *conv_scratch(), pltpu.SemaphoreType.DMA((9,)),
    ]
    taps = rulebook.reshape(TAPS, 1, ROWS)
    first, up, down, *plan, meta, rows, faces, weight_two, gain_one, shift_one, gain_two, shift_two = call(
        spread_kernel, outs, scratch, 24, taps, features[0, 0], conv_one, face_rows[0, 0], *params, hbm=True
    )
    total = SIDES * SLOTS
    outs = (shaped((total, ROWS), bf16), shaped((total, CH), i32), *(shaped((ROWS, 2 * FACE), bf16),) * 2)
    received = tile_neighbours(down, up)
    *source, at_slab, at_tile = call(
        source_kernel, outs, conv_scratch()[:1], 8, plan[0], plan[2], faces
    )
    first, left, right = call(tile_kernel, (ext, message, message), [], 8, first, *received, at_slab, at_tile)
    received = slab_neighbours(left, right)
    first, sums = call(slab_kernel, (ext, small), [], 8, meta, first, *received, at_slab)
    stats = reduce_all(sums)
    second, sums = call(
        gather_kernel, (big, small), [pltpu.VMEM((ROWS, 2 * CH), bf16), *conv_scratch()], 24,
        meta, first, *plan, *source, weight_two, stats, gain_one, shift_one,
    )
    stats = reduce_all(sums)
    out = call(
        finish_kernel, shaped((ROWS, CH), bf16),
        [pltpu.VMEM((ROWS, CH), bf16), pltpu.SemaphoreType.DMA((4,))], 4,
        meta, second, rows, stats, gain_two, shift_two, out_hbm=True,
    )
    return out[None, None]


def solution(mesh):
    tiles = mesh.shape["tile"]
    torus = Mesh(
        mesh.devices.reshape(-1, 4, 2, tiles), ("slab_0", "slab_1", "slab_2", "tile")
    )
    split = P(SLAB, "tile", None, None)
    in_specs = (split, P(SLAB, "tile"), split, split, P(), P(), P(), P(), P(), P())
    return jax.shard_map(
        per_device, mesh=torus, in_specs=in_specs, out_specs=split, check_vma=False
    )
```
